128 devices in a mesh: ctx: 16 (over z_hi, y, core), tp: 8 (over x, z_lo).
Axes of the slice: x: 4, y: 4, z: 4 (z_hi: 2, z_lo: 2; z = z_hi * 2 + z_lo), core: 2. Of those that a mesh axis runs over, the one named last changes fastest.
Arguments:
- hidden: bfloat16 [16384, 4096], P('ctx'), may hold values from -6 to 6
- norm_gain: float32 [4096], replicated, may hold values from 0.25 to 1.75
- w_query: bfloat16 [4096, 4096], P(None, 'tp')
- w_key: bfloat16 [4096, 1024], P(None, 'tp')
- w_value: bfloat16 [4096, 1024], P(None, 'tp'), may hold values from -0.09375 to 0.09375
- w_output: bfloat16 [4096, 4096], P('tp'), may hold values from -0.09375 to 0.09375
- positions: int32 [8192], P('ctx'), may hold values from -1 to 16383, as said below
- counts: int32 [64], P('ctx'), may hold values from 1 to 128, as said below
- router_weight: float32 [16384], P('ctx'), may hold values from 0.25 to 2
Outputs:
- mixed: bfloat16 [16384, 4096], P('ctx', 'tp')
The draws below stay inside these ranges and needn't reach their ends.
Inputs may be any that keep to these rules, and one draw needn't show every extreme that they name: Slots of ctx index s are those from s * 512 to (s + 1) * 512 - 1; their live slots hold distinct positions from s * 1024 to (s + 1) * 1024 - 1, increasing in slot order; other slots hold -1. `counts`: blocks of ctx index s are those from s * 4 to (s + 1) * 4 - 1; one block among all 64 is full.
All inputs are finite; a program needn't handle non-finite values.
Results may differ from the reference program's by a relative error of at most 0.0089.
Values may be sent and summed in bfloat16 or wider, within the bound.
A program may use at most 128 MiB of HBM per device.

```python
import math
import jax
import jax.numpy as jnp
from jax import lax

D = 4096
HEADS = 32
KV_HEADS = 8
HEAD_DIM = 128
BLOCK = 128
SEQ_DEV = 1024
CAP = 512
LENGTH = 16384
N_CTX = 16
N_TP = 8


def routed_layout(key):
    base = jax.random.fold_in(key, 31)
    blocks = CAP // BLOCK
    level = jax.random.randint(jax.random.fold_in(base, 1), (N_CTX, 1), 1, 5)
    lowest = jnp.maximum(1, BLOCK * level // 8)
    highest = BLOCK * level // 4 + 1
    raw = jax.random.randint(jax.random.fold_in(base, 2), (N_CTX, blocks), 0, 2 ** 20)
    counts = lowest + raw % (highest - lowest)
    full_shard = jax.random.randint(jax.random.fold_in(base, 4), (), 0, N_CTX)
    full_block = jax.random.randint(jax.random.fold_in(base, 5), (), 0, blocks)
    pick = (jnp.arange(N_CTX)[:, None] == full_shard) & (jnp.arange(blocks)[None, :] == full_block)
    counts = jnp.where(pick, BLOCK, counts).astype(jnp.int32)
    totals = jnp.sum(counts, axis=1)
    shard_keys = jax.random.split(jax.random.fold_in(base, 3), N_CTX)
    orders = jax.vmap(lambda item: jax.random.permutation(item, SEQ_DEV))(shard_keys)[:, :CAP]
    chosen = jnp.where(jnp.arange(CAP)[None, :] < totals[:, None], orders, SEQ_DEV)
    ordered = jnp.sort(chosen, axis=1)
    starts = jnp.cumsum(counts, axis=1) - counts
    inner = jnp.arange(BLOCK)
    wanted = (starts[:, :, None] + inner[None, None, :]).reshape(N_CTX, CAP)
    taken = jnp.take_along_axis(ordered, jnp.minimum(wanted, CAP - 1), axis=1)
    live = (inner[None, None, :] < counts[:, :, None]).reshape(N_CTX, CAP)
    placed = taken + jnp.arange(N_CTX)[:, None] * SEQ_DEV
    positions = jnp.where(live, placed, -1).astype(jnp.int32)
    return (counts.reshape(-1), positions.reshape(-1))


def query_weights(key):
    return jax.random.normal(jax.random.fold_in(key, 11), (D, HEADS * HEAD_DIM), jnp.float32) * D ** (-0.5)


def draw_positions(key, part):
    return routed_layout(key)[1]


def draw_counts(key, part):
    return routed_layout(key)[0]


def draw_w_query(key, part):
    return query_weights(key).astype(jnp.bfloat16)


def draw_w_key(key, part):
    noise = jax.random.normal(jax.random.fold_in(key, 12), (D, KV_HEADS * HEAD_DIM), jnp.float32) * D ** (-0.5)
    return noise.astype(jnp.bfloat16)


def shard_levels(rng, extent, shards, least, top_value):
    gain, own = 1.0, jax.random.fold_in(rng, 6)
    for axis_at, shards_of in shards:
        steps = jnp.exp(jax.random.uniform(jax.random.fold_in(own, axis_at), (shards_of,), jnp.float32, least / len(shards), top_value / len(shards)))
        gain = gain * jnp.repeat(steps, extent[axis_at] // shards_of).reshape([-1 if axis == axis_at else 1 for axis in range(len(extent))])
    return gain


def gaussian(own_key, shape, spread, bound, cuts=(), held_as=jnp.bfloat16):
    values = jax.random.normal(own_key, shape, jnp.float32) * spread
    if len(cuts) > 0:
        values = shard_levels(own_key, shape, cuts, -0.22, 0.18) * values
    return jnp.clip(values, min=-bound, max=bound).astype(held_as)


def setup_inputs(seed: int = 0) -> dict:
    seeds = jax.random.split(jax.random.key(seed), 10)
    hidden = gaussian(seeds[0], (LENGTH, D), 1.0, 6.0, ((0, 16),))
    norm_gain = jnp.clip(1.0 + 0.15 * jax.random.normal(seeds[1], (D,), jnp.float32), 0.25, 1.75)
    w_query = draw_w_query(jax.random.fold_in(seeds[9], 71), 0)
    w_key = draw_w_key(jax.random.fold_in(seeds[9], 71), 0)
    w_value = gaussian(seeds[4], (D, KV_HEADS * HEAD_DIM), D ** -0.5, 0.09375, ((1, 8),))
    w_output = gaussian(seeds[5], (HEADS * HEAD_DIM, D), (HEADS * HEAD_DIM) ** -0.5, 0.09375, ((0, 8),))
    positions = draw_positions(jax.random.fold_in(seeds[9], 71), 0)
    counts = draw_counts(jax.random.fold_in(seeds[9], 71), 0)
    router_weight = jnp.clip(jnp.exp(math.log(2.0) - 2.0794415 * jax.random.uniform(seeds[8], (LENGTH,), jnp.float32) ** shard_levels(seeds[8], (LENGTH,), ((0, 16),), -0.2, 0.2)), 0.25, 2.0)
    return {"hidden": hidden, "norm_gain": norm_gain, "w_query": w_query, "w_key": w_key, "w_value": w_value, "w_output": w_output, "positions": positions, "counts": counts, "router_weight": router_weight}


def rotate(field, angle_pos):
    half = field.shape[-1] // 2
    freq = 500000.0 ** (-2.0 * jnp.arange(half, dtype=jnp.float32) / field.shape[-1])
    angle = angle_pos[:, None] * freq[None, :]
    cosine = jnp.cos(angle)[:, None, :]
    sine = jnp.sin(angle)[:, None, :]
    first = field[..., :half]
    second = field[..., half:]
    return jnp.concatenate([first * cosine - second * sine, second * cosine + first * sine], axis=-1)

def reference(hidden, norm_gain, w_query, w_key, w_value, w_output, positions, counts, router_weight):
    slot_count = positions.shape[0]
    within = jnp.arange(slot_count, dtype=jnp.int32)
    block_of = (within // BLOCK).astype(jnp.int32)
    live = within % BLOCK < counts[block_of]
    index = jnp.where(live, positions, 0).astype(jnp.int32)
    rows = hidden[index].astype(jnp.float32) * live[:, None].astype(jnp.float32)
    scale_rows = lax.rsqrt(lax.optimization_barrier(jnp.mean(rows * rows, axis=-1, keepdims=True)) + 1e-05)
    normed = (rows * scale_rows * norm_gain[None, :]).astype(jnp.bfloat16)
    queries = jnp.dot(normed, w_query, preferred_element_type=jnp.float32)
    key_rows = jnp.dot(normed, w_key, preferred_element_type=jnp.float32)
    value_rows = jnp.dot(normed, w_value, preferred_element_type=jnp.float32).astype(jnp.bfloat16)
    angle_pos = index.astype(jnp.float32)
    queries = rotate(queries.reshape(slot_count, HEADS, HEAD_DIM), angle_pos).astype(jnp.bfloat16)
    key_rows = rotate(key_rows.reshape(slot_count, KV_HEADS, HEAD_DIM), angle_pos).astype(jnp.bfloat16)
    value_rows = value_rows.reshape(slot_count, KV_HEADS, HEAD_DIM)
    query_pos = jnp.where(live, positions, -1)
    key_pos = jnp.where(live, positions, 2 ** 30)
    allowed = key_pos[None, :] <= query_pos[:, None]
    group = HEADS // KV_HEADS

    def one_head(head):
        query_head = queries[:, head, :]
        key_head = key_rows[:, head // group, :]
        value_head = value_rows[:, head // group, :]
        score = jnp.dot(query_head, key_head.T, preferred_element_type=jnp.float32) * HEAD_DIM ** (-0.5)
        masked = jnp.where(allowed, score, -1e+30)
        largest = lax.optimization_barrier(jnp.max(masked, axis=-1, keepdims=True))
        weight = jnp.where(allowed, jnp.exp(masked - largest), 0.0)
        total = lax.optimization_barrier(jnp.sum(weight, axis=-1, keepdims=True))
        total = jnp.where(total > 0, total, 1.0)
        product = jnp.dot(weight.astype(jnp.bfloat16), value_head, preferred_element_type=jnp.float32)
        return (product / total).astype(jnp.bfloat16)
    heads_out = lax.map(one_head, jnp.arange(HEADS, dtype=jnp.int32))
    attn = jnp.transpose(heads_out, (1, 0, 2)).reshape(slot_count, HEADS * HEAD_DIM)
    width = HEADS * HEAD_DIM // N_TP
    attn_groups = attn.reshape(slot_count, N_TP, width)
    output_groups = w_output.reshape(N_TP, width, w_output.shape[1])

    def add_group(carry, member):
        product = jnp.dot(attn_groups[:, member, :], output_groups[member], preferred_element_type=jnp.float32)
        return (carry + product.astype(jnp.bfloat16).astype(jnp.float32), None)
    proj, unused = lax.scan(add_group, jnp.zeros((slot_count, w_output.shape[1]), jnp.float32), jnp.arange(N_TP, dtype=jnp.int32))
    target = jnp.where(live, positions, hidden.shape[0]).astype(jnp.int32)
    update = router_weight[index][:, None] * proj
    mixed = hidden.astype(jnp.float32).at[target].add(update, mode='drop')
    return mixed.astype(jnp.bfloat16)
```

```python
import functools

import jax
import jax.numpy as jnp
import numpy as np
from jax import lax
from jax.experimental import pallas as pl
from jax.experimental.pallas import tpu as pltpu
from jax.sharding import Mesh
from jax.sharding import PartitionSpec as P

HEAD_DIM = 128
BLOCK = 128
CTX = ("zh", "y", "core")
TP = ("x", "zl")
CHUNK = 512
KEY_CHUNK = 512
STEP = 32
F32 = jnp.float32
BF16 = jnp.bfloat16
VMEM_LIMIT = 60 * 1024 * 1024


def freq_table():
    half = HEAD_DIM // 2
    one = 500000.0 ** (-2.0 * np.arange(half, dtype=np.float64) / HEAD_DIM)
    return np.concatenate([one, one])


def angle_tables(seq, shards):
    freq = freq_table()
    sign = np.concatenate([-np.ones(HEAD_DIM // 2), np.ones(HEAD_DIM // 2)])
    coarse = np.arange(0, seq * shards, STEP, dtype=np.float64)[:, None] * freq[None, :]
    fine = np.arange(STEP, dtype=np.float64)[:, None] * freq[None, :]
    big = np.stack([np.cos(coarse), np.sin(coarse)]).astype(np.float32)
    small = np.stack([np.cos(fine), np.sin(fine), np.tile(sign, (STEP, 1))]).astype(np.float32)
    return big.reshape(2, shards, seq // STEP, HEAD_DIM).transpose(1, 0, 2, 3), small


def live_rows(counts_ref, blocks):
    total = counts_ref[0]
    for block in range(1, blocks):
        total = total + counts_ref[block]
    return total


def compact_positions(counts_ref, pos_ref, base, slots):
    lane = lax.broadcasted_iota(jnp.int32, (1, BLOCK), 1)
    row = lax.broadcasted_iota(jnp.int32, (slots, BLOCK), 0)
    start = jnp.int32(0)
    total = jnp.zeros((slots, BLOCK), F32)
    for block in range(slots // BLOCK):
        count = counts_ref[block]
        place = jnp.where(lane < count, lane + start, -1)
        value = (pos_ref[:, block * BLOCK : (block + 1) * BLOCK] - (base - 1)).astype(F32)
        total = total + jnp.where(place == row, value, 0.0)
        start = start + count
    return jnp.sum(total, axis=1, keepdims=True).astype(jnp.int32) - 1


def select_matrix(counts_ref, pos_ref, base, slots, seq):
    column = compact_positions(counts_ref, pos_ref, base, slots)
    place = lax.broadcasted_iota(jnp.int32, (slots, seq), 1)
    return jnp.where(place == column, 1.0, 0.0).astype(BF16)


def rotated(field, cos, sin):
    return field * cos + pltpu.roll(field, HEAD_DIM // 2, 1) * sin


def front_kernel(
    shard_ref, counts_ref, pos_ref, gain_ref, big_ref, small_ref, hidden, wq, wk, wv,
    q_out, kv_out,
    hbuf, wkv, wqv, xg, acc_kv, acc_q, ssq, cos, sin, sel, hsem, wsem,
):
    seq, width = hidden.shape
    slots = pos_ref.shape[1]
    chunks = width // CHUNK
    rows = 256
    blocks = seq // rows
    copies_w = [
        pltpu.make_async_copy(wk, wkv.at[:, :HEAD_DIM], wsem.at[0]),
        pltpu.make_async_copy(wv, wkv.at[:, HEAD_DIM:], wsem.at[1]),
        pltpu.make_async_copy(wq, wqv, wsem.at[2]),
    ]

    def fetch(chunk):
        columns = pl.ds(pl.multiple_of(chunk * CHUNK, CHUNK), CHUNK)
        slot = lax.rem(chunk, 3)
        return pltpu.make_async_copy(hidden.at[:, columns], hbuf.at[slot], hsem.at[slot])

    copies_w[0].start()
    copies_w[1].start()
    fetch(0).start()
    fetch(1).start()
    copies_w[2].start()

    base = shard_ref[0] * seq
    for step in range(seq // STEP):
        part = slice(step * STEP, (step + 1) * STEP)
        cb, sb = big_ref[0, step : step + 1, :], big_ref[1, step : step + 1, :]
        cf, sf, sign = small_ref[0], small_ref[1], small_ref[2]
        cos[part, :] = cb * cf - sb * sf
        sin[part, :] = (sb * cf + cb * sf) * sign
    sel[...] = select_matrix(counts_ref, pos_ref, base, slots, seq)
    acc_kv[...] = jnp.zeros_like(acc_kv)
    ssq[...] = jnp.zeros_like(ssq)
    copies_w[0].wait()
    copies_w[1].wait()

    @pl.loop(0, chunks)
    def _(chunk):
        fetch(chunk).wait()

        @pl.when(chunk + 2 < chunks)
        def _():
            fetch(chunk + 2).start()

        slot = lax.rem(chunk, 3)
        columns = pl.ds(pl.multiple_of(chunk * CHUNK, CHUNK), CHUNK)
        gain = gain_ref[:, columns]
        weight = wkv[columns, :]
        for block in range(blocks):
            part = slice(block * rows, (block + 1) * rows)
            value = hbuf[slot, part, :].astype(F32)
            square = value * value
            partial = square[:, :128]
            for lane in range(1, CHUNK // 128):
                partial = partial + square[:, lane * 128 : (lane + 1) * 128]
            ssq[part, :] += partial
            scaled = (value * gain).astype(BF16)
            xg[part, columns] = scaled
            acc_kv[part, :] += jnp.dot(scaled, weight, preferred_element_type=F32)

    def scale_of(part):
        mean = jnp.sum(ssq[part, :], axis=1, keepdims=True) * (1.0 / width)
        return lax.rsqrt(mean + 1e-05)

    pieces = []
    for block in range(blocks):
        part = slice(block * rows, (block + 1) * rows)
        scale = scale_of(part)
        keys = rotated(acc_kv[part, :HEAD_DIM] * scale, cos[part, :], sin[part, :])
        values = acc_kv[part, HEAD_DIM:] * scale
        pieces.append(jnp.concatenate([keys.astype(BF16), values.astype(BF16)], axis=1))
    both = jnp.dot(sel[...], jnp.concatenate(pieces, axis=0), preferred_element_type=F32)
    kv_out[0] = both[:, :HEAD_DIM].astype(BF16)
    kv_out[1] = both[:, HEAD_DIM:].astype(BF16)

    copies_w[2].wait()
    heads = wq.shape[1] // HEAD_DIM
    factor = HEAD_DIM ** (-0.5) * 1.4426950408889634

    @pl.loop(0, blocks)
    def _(block):
        part = pl.ds(pl.multiple_of(block * rows, rows), rows)
        product = jnp.dot(xg[part, :], wqv[...], preferred_element_type=F32)
        scale = scale_of(part) * factor
        for head in range(heads):
            lanes = slice(head * HEAD_DIM, (head + 1) * HEAD_DIM)
            turned = rotated(product[:, lanes] * scale, cos[part, :], sin[part, :])
            acc_q[part, lanes] = turned.astype(BF16)

    picked = jnp.dot(sel[...], acc_q[...], preferred_element_type=F32)
    for head in range(heads):
        q_out[head] = picked[:, head * HEAD_DIM : (head + 1) * HEAD_DIM].astype(BF16)


def smem():
    return pl.BlockSpec(memory_space=pltpu.SMEM)


def vmem():
    return pl.BlockSpec(memory_space=pltpu.VMEM)


def hbm():
    return pl.BlockSpec(memory_space=pl.ANY)


def front(shard, counts, pos, gain, big, small, hidden, wq, wk, wv):
    seq, width = hidden.shape
    slots = pos.shape[1]
    heads = wq.shape[1] // HEAD_DIM
    return pl.pallas_call(
        front_kernel,
        out_shape=(
            jax.ShapeDtypeStruct((heads, slots, HEAD_DIM), BF16),
            jax.ShapeDtypeStruct((2, slots, HEAD_DIM), BF16),
        ),
        in_specs=[smem(), smem(), vmem(), vmem(), vmem(), vmem(), hbm(), hbm(), hbm(), hbm()],
        out_specs=(vmem(), vmem()),
        scratch_shapes=[
            pltpu.VMEM((3, seq, CHUNK), BF16),
            pltpu.VMEM((width, 2 * HEAD_DIM), BF16),
            pltpu.VMEM(wq.shape, BF16),
            pltpu.VMEM((seq, width), BF16),
            pltpu.VMEM((seq, 2 * HEAD_DIM), F32),
            pltpu.VMEM((seq, heads * HEAD_DIM), BF16),
            pltpu.VMEM((seq, 128), F32),
            pltpu.VMEM((seq, HEAD_DIM), F32),
            pltpu.VMEM((seq, HEAD_DIM), F32),
            pltpu.VMEM((slots, seq), BF16),
            pltpu.SemaphoreType.DMA((3,)),
            pltpu.SemaphoreType.DMA((3,)),
        ],
        compiler_params=pltpu.CompilerParams(vmem_limit_bytes=VMEM_LIMIT),
        name="front",
    )(shard, counts, pos, gain, big, small, hidden, wq, wk, wv)


def attend_kernel(shard_ref, live_ref, q_ref, kv_ref, out_ref, keys, values, best, acc):
    shards, _, slots, dim = kv_ref.shape
    heads = q_ref.shape[0]
    me = shard_ref[0]
    lane = lax.broadcasted_iota(jnp.int32, (slots, dim), 1)
    row = lax.broadcasted_iota(jnp.int32, (slots, dim), 0)

    def place(shard, start):
        live = live_ref[shard]
        part = pl.ds(pl.multiple_of(start, 16), slots)
        keys[part, :dim] = kv_ref[shard, 0]
        keys[part, dim:] = jnp.where((lane == 0) & (row >= live), -1e30, 0.0).astype(BF16)
        values[part, :] = kv_ref[shard, 1]
        return start + (live + 15) // 16 * 16

    own = lax.fori_loop(0, me, place, jnp.int32(0))
    place(me, own)
    full = own // KEY_CHUNK
    tile = 128
    ones = jnp.where(lane == 0, 1.0, 0.0).astype(BF16)
    lane_q = lax.broadcasted_iota(jnp.int32, (heads * tile, dim), 1)
    ones_q = jnp.where(lane_q == 0, 1.0, 0.0).astype(BF16)
    tail = pl.ds(pl.multiple_of(own + slots, 16), KEY_CHUNK)
    keys[tail, :dim] = jnp.zeros((KEY_CHUNK, dim), BF16)
    keys[tail, dim:] = jnp.where(lane == 0, -1e30, 0.0).astype(BF16)
    values[tail, :] = jnp.zeros((KEY_CHUNK, dim), BF16)

    @pl.loop(0, (live_ref[me] + tile - 1) // tile)
    def _(block):
        rows = pl.ds(pl.multiple_of(block * tile, tile), tile)
        query = jnp.concatenate([q_ref[head, rows, :] for head in range(heads)], axis=0)
        query = jnp.concatenate([query, ones_q], axis=1)
        best[...] = jnp.full_like(best, -3e38)
        acc[...] = jnp.zeros_like(acc)

        def step(chunk, masked):
            part = pl.ds(pl.multiple_of(chunk * KEY_CHUNK, KEY_CHUNK), KEY_CHUNK)
            score = lax.dot_general(
                query, keys[part, :], (((1,), (1,)), ((), ())), preferred_element_type=F32
            )
            if masked:
                key_at = lax.broadcasted_iota(jnp.int32, score.shape, 1) + chunk * KEY_CHUNK
                query_at = lax.broadcasted_iota(jnp.int32, score.shape, 0)
                limit = jnp.bitwise_and(query_at, tile - 1) + (own + block * tile)
                score = jnp.where(key_at <= limit, score, -1e30)
            old = best[...]
            new = jnp.maximum(old, jnp.max(score, axis=1, keepdims=True))
            weight = jnp.exp2(score - new[:, :1]).astype(BF16)
            both = jnp.concatenate([values[part, :], ones], axis=1)
            product = jnp.dot(weight, both, preferred_element_type=F32)
            factor = jnp.exp2(old - new)
            acc[:, :dim] = acc[:, :dim] * factor + product[:, :dim]
            acc[:, dim:] = acc[:, dim:] * factor + product[:, dim:]
            best[...] = new

        @pl.loop(0, full)
        def _(chunk):
            step(chunk, False)

        last = (own + (block + 1) * tile + KEY_CHUNK - 1) // KEY_CHUNK

        @pl.loop(full, last)
        def _(chunk):
            step(chunk, True)

        total = acc[:, dim : dim + 1]
        result = acc[:, :dim] / total
        for head in range(heads):
            out_ref[rows, head * dim : (head + 1) * dim] = result[
                head * tile : (head + 1) * tile, :
            ].astype(BF16)


def attend(shard, live, q, kv):
    heads, slots, dim = q.shape
    shards = kv.shape[0]
    length = shards * slots + KEY_CHUNK + 512
    return pl.pallas_call(
        attend_kernel,
        out_shape=jax.ShapeDtypeStruct((slots, heads * dim), BF16),
        in_specs=[smem(), smem(), vmem(), vmem()],
        out_specs=vmem(),
        scratch_shapes=[
            pltpu.VMEM((length, 2 * dim), BF16),
            pltpu.VMEM((length, dim), BF16),
            pltpu.VMEM((heads * 128, 128), F32),
            pltpu.VMEM((heads * 128, 2 * dim), F32),
        ],
        compiler_params=pltpu.CompilerParams(vmem_limit_bytes=VMEM_LIMIT),
        name="attend",
    )(shard, live, q, kv)


def merge_kernel(shard_ref, counts_ref, pos_ref, router_ref, parts_ref, own_ref, out_ref, sel):
    seq, width = own_ref.shape
    members, slots, _ = parts_ref.shape
    sel[...] = select_matrix(counts_ref, pos_ref, shard_ref[0] * seq, slots, seq)
    total = parts_ref[0].astype(F32)
    for member in range(1, members):
        total = total + parts_ref[member].astype(F32)
    live = lax.broadcasted_iota(jnp.int32, (slots, width), 0) < live_rows(
        counts_ref, slots // BLOCK
    )
    total = jnp.where(live, total, 0.0)
    high = total.astype(BF16)
    low = (total - high.astype(F32)).astype(BF16)
    dims = (((0,), (0,)), ((), ()))
    update = lax.dot_general(sel[...], high, dims, preferred_element_type=F32)
    update = update + lax.dot_general(sel[...], low, dims, preferred_element_type=F32)
    router = jnp.transpose(jnp.broadcast_to(router_ref[...], (128, seq)))[:, :1]
    out_ref[...] = (own_ref[...].astype(F32) + router * update).astype(BF16)


def merge(shard, counts, pos, router, parts, own):
    return pl.pallas_call(
        merge_kernel,
        out_shape=jax.ShapeDtypeStruct(own.shape, BF16),
        in_specs=[smem(), smem(), vmem(), vmem(), vmem(), vmem()],
        out_specs=vmem(),
        scratch_shapes=[pltpu.VMEM((pos.shape[1], own.shape[0]), BF16)],
        compiler_params=pltpu.CompilerParams(vmem_limit_bytes=VMEM_LIMIT),
        name="merge",
    )(shard, counts, pos, router, parts, own)


def per_device(
    hidden, norm_gain, w_query, w_key, w_value, w_output, positions, counts, router_weight
):
    seq = hidden.shape[0]
    slots = positions.shape[0]
    shards = lax.axis_size(CTX)
    shard = lax.axis_index(CTX).astype(jnp.int32)
    big, small = angle_tables(seq, shards)
    big = lax.dynamic_index_in_dim(jnp.asarray(big), shard, 0, keepdims=False)
    shard = shard.reshape(1)
    pos = positions.reshape(1, slots)
    q, kv = front(
        shard, counts, pos, norm_gain.reshape(1, -1), big, jnp.asarray(small),
        hidden, w_query, w_key, w_value,
    )
    live = lax.all_gather(jnp.sum(counts), CTX, axis=0)
    gathered = lax.all_gather(kv, CTX, axis=0)
    attn = attend(shard, live, q, gathered)
    product = jnp.dot(attn, w_output, preferred_element_type=F32).astype(BF16)
    members = lax.axis_size(TP)
    width = product.shape[1] // members
    parts = jnp.moveaxis(product.reshape(slots, members, width), 1, 0)
    arrived = lax.all_to_all(parts, TP, split_axis=0, concat_axis=0, tiled=True)
    own = lax.dynamic_slice_in_dim(hidden, lax.axis_index(TP) * width, width, 1)
    return merge(shard, counts, pos, router_weight.reshape(1, seq), arrived, own)


def solution(mesh):
    finer = Mesh(mesh.devices.reshape(2, 4, 2, 4, 2), CTX + TP)
    return jax.shard_map(
        per_device,
        mesh=finer,
        in_specs=(
            P(CTX, None), P(), P(None, TP), P(None, TP), P(None, TP), P(TP, None),
            P(CTX), P(CTX), P(CTX),
        ),
        out_specs=P(CTX, TP),
        check_vma=False,
    )
```

```python
import functools

import jax
import jax.numpy as jnp
import numpy as np
from jax import lax
from jax.experimental import pallas as pl
from jax.experimental.pallas import tpu as pltpu
from jax.sharding import Mesh
from jax.sharding import PartitionSpec as P

HEAD_DIM = 128
BLOCK = 128
CTX = ("zh", "y", "core")
TP = ("x", "zl")
CHUNK = 512
KEY_CHUNK = 512
STEP = 32
F32 = jnp.float32
BF16 = jnp.bfloat16
VMEM_LIMIT = 60 * 1024 * 1024
MESH = pl.DeviceIdType.MESH


def freq_table():
    half = HEAD_DIM // 2
    one = 500000.0 ** (-2.0 * np.arange(half, dtype=np.float64) / HEAD_DIM)
    return np.concatenate([one, one])


def angle_tables(seq, shards):
    freq = freq_table()
    sign = np.concatenate([-np.ones(HEAD_DIM // 2), np.ones(HEAD_DIM // 2)])
    coarse = np.arange(0, seq * shards, STEP, dtype=np.float64)[:, None] * freq[None, :]
    fine = np.arange(STEP, dtype=np.float64)[:, None] * freq[None, :]
    big = np.stack([np.cos(coarse), np.sin(coarse)]).astype(np.float32)
    small = np.stack([np.cos(fine), np.sin(fine), np.tile(sign, (STEP, 1))]).astype(np.float32)
    return big.reshape(2, shards, seq // STEP, HEAD_DIM).transpose(1, 0, 2, 3), small


def live_rows(counts_ref, blocks):
    total = counts_ref[0]
    for block in range(1, blocks):
        total = total + counts_ref[block]
    return total


def compact_positions(counts_ref, pos_ref, base, slots):
    lane = lax.broadcasted_iota(jnp.int32, (1, BLOCK), 1)
    row = lax.broadcasted_iota(jnp.int32, (slots, BLOCK), 0)
    start = jnp.int32(0)
    total = jnp.zeros((slots, BLOCK), F32)
    for block in range(slots // BLOCK):
        count = counts_ref[block]
        place = jnp.where(lane < count, lane + start, -1)
        value = (pos_ref[:, block * BLOCK : (block + 1) * BLOCK] - (base - 1)).astype(F32)
        total = total + jnp.where(place == row, value, 0.0)
        start = start + count
    return jnp.sum(total, axis=1, keepdims=True).astype(jnp.int32) - 1


def select_matrix(counts_ref, pos_ref, base, slots, seq):
    column = compact_positions(counts_ref, pos_ref, base, slots)
    place = lax.broadcasted_iota(jnp.int32, (slots, seq), 1)
    return jnp.where(place == column, 1.0, 0.0).astype(BF16)


def rotated(field, cos, sin):
    return field * cos + pltpu.roll(field, HEAD_DIM // 2, 1) * sin


def greet(peers):
    barrier = pltpu.get_barrier_semaphore()
    for peer in peers:
        pl.semaphore_signal(barrier, inc=1, device_id=peer, device_id_type=MESH)

    def wait():
        pl.semaphore_wait(barrier, len(peers))

    return wait


def front_kernel(
    counts_ref, pos_ref, gain_ref, small_ref, big, hidden, wq, wk, wv, wo,
    q_out, live_out, kv_hbm, w_out,
    hbuf, wkv, wqv, xg, acc_kv, acc_q, ssq, cos, sin, sel, bigv, kvbuf, relay,
    hsem, wsem, kv_send, kv_recv, w_send, w_recv, out_sem,
):
    zh, y, core = lax.axis_index("zh"), lax.axis_index("y"), lax.axis_index("core")
    x = lax.axis_index("x")
    y_next, y_prev, y_far = lax.rem(y + 1, 4), lax.rem(y + 3, 4), lax.rem(y + 2, 4)
    x_next, x_prev, x_far = lax.rem(x + 1, 4), lax.rem(x + 3, 4), lax.rem(x + 2, 4)
    mate, up, down = {"core": 1 - core}, {"y": y_next}, {"y": y_prev}
    across, right, left = {"zh": 1 - zh}, {"x": x_next}, {"x": x_prev}

    def shard_at(plane, row, side):
        return (plane * 4 + row) * 2 + side

    shard = shard_at(zh, y, core)
    seq, width = hidden.shape
    slots = pos_ref.shape[1]
    chunks = width // CHUNK
    rows = 256
    blocks = seq // rows
    copies_w = [
        pltpu.make_async_copy(wk, wkv.at[:, :HEAD_DIM], wsem.at[0]),
        pltpu.make_async_copy(wv, wkv.at[:, HEAD_DIM:], wsem.at[1]),
        pltpu.make_async_copy(wq, wqv, wsem.at[2]),
    ]
    copy_big = pltpu.make_async_copy(big.at[shard], bigv, wsem.at[3])

    def fetch(chunk):
        columns = pl.ds(pl.multiple_of(chunk * CHUNK, CHUNK), CHUNK)
        slot = lax.rem(chunk, 3)
        return pltpu.make_async_copy(hidden.at[:, columns], hbuf.at[slot], hsem.at[slot])

    copy_big.start()
    copies_w[0].start()
    copies_w[1].start()
    fetch(0).start()
    fetch(1).start()
    copies_w[2].start()
    greeted = greet([mate, up, down, across, right, left])

    base = shard * seq
    sel[...] = select_matrix(counts_ref, pos_ref, base, slots, seq)
    copy_big.wait()
    for step in range(seq // STEP):
        part = slice(step * STEP, (step + 1) * STEP)
        cb, sb = bigv[0, step : step + 1, :], bigv[1, step : step + 1, :]
        cf, sf, sign = small_ref[0], small_ref[1], small_ref[2]
        cos[part, :] = cb * cf - sb * sf
        sin[part, :] = (sb * cf + cb * sf) * sign

    sends = []

    def push(src, dst, send, recv, peer):
        copy = pltpu.make_async_remote_copy(
            src_ref=src, dst_ref=dst, send_sem=send, recv_sem=recv,
            device_id=peer, device_id_type=MESH,
        )
        copy.start()
        sends.append(copy)

    def landed(dst, recv):
        pltpu.make_async_remote_copy(
            src_ref=dst, dst_ref=dst, send_sem=w_send.at[0], recv_sem=recv,
            device_id=mate, device_id_type=MESH,
        ).wait_recv()

    half_rows = wo.shape[0] // 2
    quarter = half_rows // 2
    own_row = core * half_rows
    wide = wo.shape[1] // 4

    def wo_part(row, count, column):
        return wo.at[
            pl.ds(pl.multiple_of(row, quarter), count),
            pl.ds(pl.multiple_of(column * wide, wide), wide),
        ]

    def slot_part(source, row, count):
        return w_out.at[source, pl.ds(pl.multiple_of(row, quarter), count), :]

    greeted()
    push(wo_part(own_row, quarter, x_far), relay.at[0], w_send.at[0], w_recv.at[2], right)
    push(
        wo_part(own_row + quarter, quarter, x_far), relay.at[1], w_send.at[1], w_recv.at[3], left
    )
    push(
        wo_part(own_row, half_rows, x_next), slot_part(x, own_row, half_rows),
        w_send.at[2], w_recv.at[0], right,
    )
    push(
        wo_part(own_row, half_rows, x_prev), slot_part(x, own_row, half_rows),
        w_send.at[3], w_recv.at[1], left,
    )

    acc_kv[...] = jnp.zeros_like(acc_kv)
    ssq[...] = jnp.zeros_like(ssq)
    copies_w[0].wait()
    copies_w[1].wait()

    @pl.loop(0, chunks)
    def _(chunk):
        fetch(chunk).wait()

        @pl.when(chunk + 2 < chunks)
        def _():
            fetch(chunk + 2).start()

        slot = lax.rem(chunk, 3)
        columns = pl.ds(pl.multiple_of(chunk * CHUNK, CHUNK), CHUNK)
        gain = gain_ref[:, columns]
        weight = wkv[columns, :]
        for block in range(blocks):
            part = slice(block * rows, (block + 1) * rows)
            value = hbuf[slot, part, :].astype(F32)
            square = value * value
            partial = square[:, :128]
            for lane in range(1, CHUNK // 128):
                partial = partial + square[:, lane * 128 : (lane + 1) * 128]
            ssq[part, :] += partial
            scaled = (value * gain).astype(BF16)
            xg[part, columns] = scaled
            acc_kv[part, :] += jnp.dot(scaled, weight, preferred_element_type=F32)

    def scale_of(part):
        mean = jnp.sum(ssq[part, :], axis=1, keepdims=True) * (1.0 / width)
        return lax.rsqrt(mean + 1e-05)

    pieces = []
    for block in range(blocks):
        part = slice(block * rows, (block + 1) * rows)
        scale = scale_of(part)
        keys = rotated(acc_kv[part, :HEAD_DIM] * scale, cos[part, :], sin[part, :])
        values = acc_kv[part, HEAD_DIM:] * scale
        pieces.append(jnp.concatenate([keys.astype(BF16), values.astype(BF16)], axis=1))
    both = jnp.dot(sel[...], jnp.concatenate(pieces, axis=0), preferred_element_type=F32)
    live = live_rows(counts_ref, slots // BLOCK)
    low = jnp.minimum(live, 256)
    lane = lax.broadcasted_iota(jnp.int32, (16, HEAD_DIM), 1)
    first = lax.broadcasted_iota(jnp.int32, (16, HEAD_DIM), 0) == 0
    tag = jnp.where(lane == 0, low, jnp.where(lane == 1, live - low, 0))
    kvbuf[shard, 0, :slots] = both[:, :HEAD_DIM].astype(BF16)
    kvbuf[shard, 0, slots:] = jnp.where(first, tag, 0).astype(F32).astype(BF16)
    kvbuf[shard, 1, :slots] = both[:, HEAD_DIM:].astype(BF16)

    def kv_part(source, part):
        return kvbuf.at[source, 0] if part == 0 else kvbuf.at[source, 1, :slots]

    outs = []

    def send_kv(source, part, peer):
        ref = kv_part(source, part)
        push(ref, ref, kv_send.at[len(sends)], kv_recv.at[source, part], peer)

    def keep(source, part):
        ref = kv_part(source, part)
        to = kv_hbm.at[source, part]
        copy = pltpu.make_async_copy(ref.at[:slots] if part == 0 else ref, to, out_sem.at[source, part])
        copy.start()
        outs.append(copy)

    def receive_kv(source, part, peers):
        landed(kv_part(source, part), kv_recv.at[source, part])
        for peer in peers:
            send_kv(source, part, peer)
        keep(source, part)

    for part in range(2):
        send_kv(shard, part, across)
        send_kv(shard, part, up)
        send_kv(shard, part, down)
        send_kv(shard, part, mate)
        keep(shard, part)

    copies_w[2].wait()
    heads = wq.shape[1] // HEAD_DIM
    factor = HEAD_DIM ** (-0.5) * 1.4426950408889634

    @pl.loop(0, blocks)
    def _(block):
        part = pl.ds(pl.multiple_of(block * rows, rows), rows)
        product = jnp.dot(xg[part, :], wqv[...], preferred_element_type=F32)
        scale = scale_of(part) * factor
        for head in range(heads):
            lanes = slice(head * HEAD_DIM, (head + 1) * HEAD_DIM)
            turned = rotated(product[:, lanes] * scale, cos[part, :], sin[part, :])
            acc_q[part, lanes] = turned.astype(BF16)

    picked = jnp.dot(sel[...], acc_q[...], preferred_element_type=F32)
    for head in range(heads):
        q_out[head] = picked[:, head * HEAD_DIM : (head + 1) * HEAD_DIM].astype(BF16)

    landed(relay.at[0], w_recv.at[2])
    push(relay.at[0], slot_part(x_prev, own_row, quarter), w_send.at[4], w_recv.at[4], right)
    landed(relay.at[1], w_recv.at[3])
    push(
        relay.at[1], slot_part(x_next, own_row + quarter, quarter), w_send.at[5], w_recv.at[5], left
    )

    def ring(plane):
        prev, following = shard_at(plane, y_prev, core), shard_at(plane, y_next, core)
        receive_kv(prev, 0, [up, mate])
        receive_kv(following, 0, [mate])
        receive_kv(following, 1, [down, mate])
        receive_kv(prev, 1, [mate])

    ring(zh)
    other = 1 - zh
    for part in range(2):
        receive_kv(shard_at(other, y, core), part, [up, down, mate])
    for part in range(2):
        receive_kv(shard_at(zh, y_far, core), part, [mate])
    ring(other)

    def pass_on(source, row, count, received, index):
        ref = slot_part(source, row, count)
        landed(ref, w_recv.at[received])
        push(ref, ref, w_send.at[index], w_recv.at[index], mate)

    pass_on(x_prev, own_row, half_rows, 0, 6)
    pass_on(x_next, own_row, half_rows, 1, 7)
    for part in range(2):
        receive_kv(shard_at(other, y_far, core), part, [mate])
    pass_on(x_far, own_row, quarter, 4, 8)
    pass_on(x_far, own_row + quarter, quarter, 5, 9)

    for plane in range(2):
        for row in range(4):
            for part in range(2):
                receive_kv(shard_at(plane, row, 1 - core), part, [])
    mate_row = (1 - core) * half_rows
    landed(slot_part(x_prev, mate_row, half_rows), w_recv.at[6])
    landed(slot_part(x_next, mate_row, half_rows), w_recv.at[7])
    landed(slot_part(x_far, mate_row, quarter), w_recv.at[8])
    landed(slot_part(x_far, mate_row + quarter, quarter), w_recv.at[9])
    for source in range(kvbuf.shape[0]):
        tag = jnp.sum(kvbuf[source, 0, slots:].astype(F32))
        live_out[source] = tag.astype(jnp.int32)
    for copy in sends:
        copy.wait_send()
    for copy in outs:
        copy.wait()


def smem():
    return pl.BlockSpec(memory_space=pltpu.SMEM)


def vmem():
    return pl.BlockSpec(memory_space=pltpu.VMEM)


def hbm():
    return pl.BlockSpec(memory_space=pl.ANY)


def front(counts, pos, gain, small, big, hidden, wq, wk, wv, wo):
    seq, width = hidden.shape
    slots = pos.shape[1]
    heads = wq.shape[1] // HEAD_DIM
    shards = big.shape[0]
    wide = wo.shape[1] // 4
    return pl.pallas_call(
        front_kernel,
        out_shape=(
            jax.ShapeDtypeStruct((heads, slots, HEAD_DIM), BF16),
            jax.ShapeDtypeStruct((shards,), jnp.int32),
            jax.ShapeDtypeStruct((shards, 2, slots, HEAD_DIM), BF16),
            jax.ShapeDtypeStruct((4, wo.shape[0], wide), BF16),
        ),
        in_specs=[smem(), vmem(), vmem(), vmem(), hbm(), hbm(), hbm(), hbm(), hbm(), hbm()],
        out_specs=(vmem(), smem(), hbm(), hbm()),
        scratch_shapes=[
            pltpu.VMEM((3, seq, CHUNK), BF16),
            pltpu.VMEM((width, 2 * HEAD_DIM), BF16),
            pltpu.VMEM(wq.shape, BF16),
            pltpu.VMEM((seq, width), BF16),
            pltpu.VMEM((seq, 2 * HEAD_DIM), F32),
            pltpu.VMEM((seq, heads * HEAD_DIM), BF16),
            pltpu.VMEM((seq, 128), F32),
            pltpu.VMEM((seq, HEAD_DIM), F32),
            pltpu.VMEM((seq, HEAD_DIM), F32),
            pltpu.VMEM((slots, seq), BF16),
            pltpu.VMEM(big.shape[1:], F32),
            pltpu.VMEM((shards, 2, slots + 16, HEAD_DIM), BF16),
            pltpu.VMEM((2, wo.shape[0] // 4, wide), BF16),
            pltpu.SemaphoreType.DMA((3,)),
            pltpu.SemaphoreType.DMA((4,)),
            pltpu.SemaphoreType.DMA((48,)),
            pltpu.SemaphoreType.DMA((shards, 2)),
            pltpu.SemaphoreType.DMA((10,)),
            pltpu.SemaphoreType.DMA((10,)),
            pltpu.SemaphoreType.DMA((shards, 2)),
        ],
        compiler_params=pltpu.CompilerParams(
            vmem_limit_bytes=VMEM_LIMIT, collective_id=0, has_side_effects=True
        ),
        name="front",
    )(counts, pos, gain, small, big, hidden, wq, wk, wv, wo)


def attend_kernel(live_ref, q_ref, kv, out_ref, keys, values, best, acc, kv_ref, sem):
    shards, _, slots, dim = kv.shape
    heads = q_ref.shape[0]
    me = lax.axis_index(CTX)

    def fetch(shard):
        return pltpu.make_async_copy(kv.at[shard], kv_ref.at[shard], sem.at[shard])

    @pl.loop(0, me + 1)
    def _(shard):
        fetch(shard).start()

    lane = lax.broadcasted_iota(jnp.int32, (slots, dim), 1)
    row = lax.broadcasted_iota(jnp.int32, (slots, dim), 0)

    def place(shard, start):
        live = live_ref[shard]
        fetch(shard).wait()
        part = pl.ds(pl.multiple_of(start, 16), slots)
        keys[part, :dim] = kv_ref[shard, 0]
        keys[part, dim:] = jnp.where((lane == 0) & (row >= live), -1e30, 0.0).astype(BF16)
        values[part, :] = kv_ref[shard, 1]
        return start + (live + 15) // 16 * 16

    own = lax.fori_loop(0, me, place, jnp.int32(0))
    place(me, own)
    full = own // KEY_CHUNK
    tile = 128
    ones = jnp.where(lane == 0, 1.0, 0.0).astype(BF16)
    lane_q = lax.broadcasted_iota(jnp.int32, (heads * tile, dim), 1)
    ones_q = jnp.where(lane_q == 0, 1.0, 0.0).astype(BF16)
    tail = pl.ds(pl.multiple_of(own + slots, 16), KEY_CHUNK)
    keys[tail, :dim] = jnp.zeros((KEY_CHUNK, dim), BF16)
    keys[tail, dim:] = jnp.where(lane == 0, -1e30, 0.0).astype(BF16)
    values[tail, :] = jnp.zeros((KEY_CHUNK, dim), BF16)

    used = (live_ref[me] + tile - 1) // tile

    @pl.loop(used, slots // tile)
    def _(block):
        rows = pl.ds(pl.multiple_of(block * tile, tile), tile)
        out_ref[rows, :] = jnp.zeros((tile, heads * dim), BF16)

    @pl.loop(0, used)
    def _(block):
        rows = pl.ds(pl.multiple_of(block * tile, tile), tile)
        query = jnp.concatenate([q_ref[head, rows, :] for head in range(heads)], axis=0)
        query = jnp.concatenate([query, ones_q], axis=1)
        best[...] = jnp.full_like(best, -3e38)
        acc[...] = jnp.zeros_like(acc)

        def step(chunk, masked):
            part = pl.ds(pl.multiple_of(chunk * KEY_CHUNK, KEY_CHUNK), KEY_CHUNK)
            score = lax.dot_general(
                query, keys[part, :], (((1,), (1,)), ((), ())), preferred_element_type=F32
            )
            if masked:
                key_at = lax.broadcasted_iota(jnp.int32, score.shape, 1) + chunk * KEY_CHUNK
                query_at = lax.broadcasted_iota(jnp.int32, score.shape, 0)
                limit = jnp.bitwise_and(query_at, tile - 1) + (own + block * tile)
                score = jnp.where(key_at <= limit, score, -1e30)
            old = best[...]
            new = jnp.maximum(old, jnp.max(score, axis=1, keepdims=True))
            weight = jnp.exp2(score - new[:, :1]).astype(BF16)
            both = jnp.concatenate([values[part, :], ones], axis=1)
            product = jnp.dot(weight, both, preferred_element_type=F32)
            factor = jnp.exp2(old - new)
            acc[:, :dim] = acc[:, :dim] * factor + product[:, :dim]
            acc[:, dim:] = acc[:, dim:] * factor + product[:, dim:]
            best[...] = new

        @pl.loop(0, full)
        def _(chunk):
            step(chunk, False)

        last = (own + (block + 1) * tile + KEY_CHUNK - 1) // KEY_CHUNK

        @pl.loop(full, last)
        def _(chunk):
            step(chunk, True)

        total = acc[:, dim : dim + 1]
        result = acc[:, :dim] / total
        for head in range(heads):
            out_ref[rows, head * dim : (head + 1) * dim] = result[
                head * tile : (head + 1) * tile, :
            ].astype(BF16)


def attend(live, q, kv):
    heads, slots, dim = q.shape
    shards = kv.shape[0]
    length = shards * slots + KEY_CHUNK + 512
    return pl.pallas_call(
        attend_kernel,
        out_shape=jax.ShapeDtypeStruct((slots, heads * dim), BF16),
        in_specs=[smem(), vmem(), hbm()],
        out_specs=vmem(),
        scratch_shapes=[
            pltpu.VMEM((length, 2 * dim), BF16),
            pltpu.VMEM((length, dim), BF16),
            pltpu.VMEM((heads * 128, 128), F32),
            pltpu.VMEM((heads * 128, 2 * dim), F32),
            pltpu.VMEM(kv.shape, BF16),
            pltpu.SemaphoreType.DMA((shards,)),
        ],
        compiler_params=pltpu.CompilerParams(vmem_limit_bytes=VMEM_LIMIT),
        name="attend",
    )(live, q, kv)


def merge_kernel(shard_ref, counts_ref, pos_ref, router_ref, parts_ref, own_ref, out_ref, sel):
    seq, width = own_ref.shape
    members, slots, _ = parts_ref.shape
    sel[...] = select_matrix(counts_ref, pos_ref, shard_ref[0] * seq, slots, seq)
    total = parts_ref[0].astype(F32)
    for member in range(1, members):
        total = total + parts_ref[member].astype(F32)
    live = lax.broadcasted_iota(jnp.int32, (slots, width), 0) < live_rows(
        counts_ref, slots // BLOCK
    )
    total = jnp.where(live, total, 0.0)
    high = total.astype(BF16)
    low = (total - high.astype(F32)).astype(BF16)
    dims = (((0,), (0,)), ((), ()))
    update = lax.dot_general(sel[...], high, dims, preferred_element_type=F32)
    update = update + lax.dot_general(sel[...], low, dims, preferred_element_type=F32)
    router = jnp.transpose(jnp.broadcast_to(router_ref[...], (128, seq)))[:, :1]
    out_ref[...] = (own_ref[...].astype(F32) + router * update).astype(BF16)


def merge(shard, counts, pos, router, parts, own):
    return pl.pallas_call(
        merge_kernel,
        out_shape=jax.ShapeDtypeStruct(own.shape, BF16),
        in_specs=[smem(), smem(), vmem(), vmem(), vmem(), vmem()],
        out_specs=vmem(),
        scratch_shapes=[pltpu.VMEM((pos.shape[1], own.shape[0]), BF16)],
        compiler_params=pltpu.CompilerParams(vmem_limit_bytes=VMEM_LIMIT),
        name="merge",
    )(shard, counts, pos, router, parts, own)


def per_device(
    hidden, norm_gain, w_query, w_key, w_value, w_output, positions, counts, router_weight
):
    seq = hidden.shape[0]
    slots = positions.shape[0]
    shards = lax.axis_size(CTX)
    shard = lax.axis_index(CTX).astype(jnp.int32).reshape(1)
    big, small = angle_tables(seq, shards)
    pos = positions.reshape(1, slots)
    q, live, gathered, weights = front(
        counts, pos, norm_gain.reshape(1, -1), jnp.asarray(small), jnp.asarray(big),
        hidden, w_query, w_key, w_value, w_output,
    )
    attn = attend(live, q, gathered)
    product = jnp.dot(attn, w_output, preferred_element_type=F32).astype(BF16)
    members = lax.axis_size(TP)
    width = product.shape[1] // members
    parts = jnp.moveaxis(product.reshape(slots, members, width), 1, 0)
    arrived = lax.all_to_all(parts, TP, split_axis=0, concat_axis=0, tiled=True)
    own = lax.dynamic_slice_in_dim(hidden, lax.axis_index(TP) * width, width, 1)
    return merge(shard, counts, pos, router_weight.reshape(1, seq), arrived, own)


def solution(mesh):
    finer = Mesh(mesh.devices.reshape(2, 4, 2, 4, 2), CTX + TP)
    return jax.shard_map(
        per_device,
        mesh=finer,
        in_specs=(
            P(CTX, None), P(), P(None, TP), P(None, TP), P(None, TP), P(TP, None),
            P(CTX), P(CTX), P(CTX),
        ),
        out_specs=P(CTX, TP),
        check_vma=False,
    )
```

```python
import jax
import jax.numpy as jnp
import numpy as np
from jax import lax
from jax.experimental import pallas as pl
from jax.experimental.pallas import tpu as pltpu
from jax.sharding import Mesh
from jax.sharding import PartitionSpec as P

HEAD_DIM = 128
BLOCK = 128
CTX = ("zh", "y", "core")
TP = ("x", "zl")
CHUNK = 512
KEY_CHUNK = 512
STEP = 32
F32 = jnp.float32
BF16 = jnp.bfloat16
VMEM_LIMIT = 60 * 1024 * 1024
MESH = pl.DeviceIdType.MESH


def freq_table():
    half = HEAD_DIM // 2
    one = 500000.0 ** (-2.0 * np.arange(half, dtype=np.float64) / HEAD_DIM)
    return np.concatenate([one, one])


def angle_tables(seq, shards):
    freq = freq_table()
    sign = np.concatenate([-np.ones(HEAD_DIM // 2), np.ones(HEAD_DIM // 2)])
    coarse = np.arange(0, seq * shards, STEP, dtype=np.float64)[:, None] * freq[None, :]
    fine = np.arange(STEP, dtype=np.float64)[:, None] * freq[None, :]
    big = np.stack([np.cos(coarse), np.sin(coarse)]).astype(np.float32)
    small = np.stack([np.cos(fine), np.sin(fine), np.tile(sign, (STEP, 1))]).astype(np.float32)
    return big.reshape(2, shards, seq // STEP, HEAD_DIM).transpose(1, 0, 2, 3), small


def live_rows(counts_ref, blocks):
    total = counts_ref[0]
    for block in range(1, blocks):
        total = total + counts_ref[block]
    return total


def compact_positions(counts_ref, pos_ref, base, slots):
    lane = lax.broadcasted_iota(jnp.int32, (1, BLOCK), 1)
    row = lax.broadcasted_iota(jnp.int32, (slots, BLOCK), 0)
    start = jnp.int32(0)
    total = jnp.zeros((slots, BLOCK), F32)
    for block in range(slots // BLOCK):
        count = counts_ref[block]
        place = jnp.where(lane < count, lane + start, -1)
        value = (pos_ref[:, block * BLOCK : (block + 1) * BLOCK] - (base - 1)).astype(F32)
        total = total + jnp.where(place == row, value, 0.0)
        start = start + count
    return jnp.sum(total, axis=1, keepdims=True).astype(jnp.int32) - 1


def select_matrix(counts_ref, pos_ref, base, slots, seq):
    column = compact_positions(counts_ref, pos_ref, base, slots)
    place = lax.broadcasted_iota(jnp.int32, (slots, seq), 1)
    return jnp.where(place == column, 1.0, 0.0).astype(BF16)


def rotated(field, cos, sin):
    return field * cos + pltpu.roll(field, HEAD_DIM // 2, 1) * sin


def greet(peers):
    barrier = pltpu.get_barrier_semaphore()
    for peer in peers:
        pl.semaphore_signal(barrier, inc=1, device_id=peer, device_id_type=MESH)

    def wait():
        pl.semaphore_wait(barrier, len(peers))

    return wait


def front_kernel(
    counts_ref, pos_ref, gain_ref, small_ref, big, hidden, wq, wk, wv, wo,
    q_out, live_out, kv_hbm, w_out,
    hbuf, wkv, wqv, xg, acc_kv, acc_q, ssq, cos, sin, sel, bigv, kvbuf, relay,
    hsem, wsem, kv_send, kv_recv, w_send, w_recv, out_sem,
):
    zh, y, core = lax.axis_index("zh"), lax.axis_index("y"), lax.axis_index("core")
    x = lax.axis_index("x")
    y_next, y_prev, y_far = lax.rem(y + 1, 4), lax.rem(y + 3, 4), lax.rem(y + 2, 4)
    x_next, x_prev, x_far = lax.rem(x + 1, 4), lax.rem(x + 3, 4), lax.rem(x + 2, 4)
    mate, up, down = {"core": 1 - core}, {"y": y_next}, {"y": y_prev}
    across, right, left = {"zh": 1 - zh}, {"x": x_next}, {"x": x_prev}

    def shard_at(plane, row, side):
        return (plane * 4 + row) * 2 + side

    shard = shard_at(zh, y, core)
    seq, width = hidden.shape
    slots = pos_ref.shape[1]
    chunks = width // CHUNK
    rows = 256
    blocks = seq // rows
    copies_w = [
        pltpu.make_async_copy(wk, wkv.at[:, :HEAD_DIM], wsem.at[0]),
        pltpu.make_async_copy(wv, wkv.at[:, HEAD_DIM:], wsem.at[1]),
        pltpu.make_async_copy(wq, wqv, wsem.at[2]),
    ]
    copy_big = pltpu.make_async_copy(big.at[shard], bigv, wsem.at[3])

    def fetch(chunk):
        columns = pl.ds(pl.multiple_of(chunk * CHUNK, CHUNK), CHUNK)
        slot = lax.rem(chunk, 3)
        return pltpu.make_async_copy(hidden.at[:, columns], hbuf.at[slot], hsem.at[slot])

    copy_big.start()
    copies_w[0].start()
    copies_w[1].start()
    fetch(0).start()
    fetch(1).start()
    copies_w[2].start()
    greeted = greet([mate, up, down, across, right, left])

    base = shard * seq
    sel[...] = select_matrix(counts_ref, pos_ref, base, slots, seq)
    copy_big.wait()
    for step in range(seq // STEP):
        part = slice(step * STEP, (step + 1) * STEP)
        cb, sb = bigv[0, step : step + 1, :], bigv[1, step : step + 1, :]
        cf, sf, sign = small_ref[0], small_ref[1], small_ref[2]
        cos[part, :] = cb * cf - sb * sf
        sin[part, :] = (sb * cf + cb * sf) * sign

    sends = []

    def push(src, dst, send, recv, peer):
        copy = pltpu.make_async_remote_copy(
            src_ref=src, dst_ref=dst, send_sem=send, recv_sem=recv,
            device_id=peer, device_id_type=MESH,
        )
        copy.start()
        sends.append(copy)

    def landed(dst, recv):
        pltpu.make_async_remote_copy(
            src_ref=dst, dst_ref=dst, send_sem=w_send.at[0], recv_sem=recv,
            device_id=mate, device_id_type=MESH,
        ).wait_recv()

    half_rows = wo.shape[0] // 2
    quarter = half_rows // 2
    own_row = core * half_rows
    wide = wo.shape[1] // 4

    def wo_part(row, count, column):
        return wo.at[
            pl.ds(pl.multiple_of(row, quarter), count),
            pl.ds(pl.multiple_of(column * wide, wide), wide),
        ]

    def slot_part(source, row, count):
        return w_out.at[source, pl.ds(pl.multiple_of(row, quarter), count), :]

    greeted()
    push(wo_part(own_row, quarter, x_far), relay.at[0], w_send.at[0], w_recv.at[2], right)
    push(
        wo_part(own_row + quarter, quarter, x_far), relay.at[1], w_send.at[1], w_recv.at[3], left
    )
    push(
        wo_part(own_row, half_rows, x_next), slot_part(x, own_row, half_rows),
        w_send.at[2], w_recv.at[0], right,
    )
    push(
        wo_part(own_row, half_rows, x_prev), slot_part(x, own_row, half_rows),
        w_send.at[3], w_recv.at[1], left,
    )

    acc_kv[...] = jnp.zeros_like(acc_kv)
    ssq[...] = jnp.zeros_like(ssq)
    copies_w[0].wait()
    copies_w[1].wait()

    @pl.loop(0, chunks)
    def _(chunk):
        fetch(chunk).wait()

        @pl.when(chunk + 2 < chunks)
        def _():
            fetch(chunk + 2).start()

        slot = lax.rem(chunk, 3)
        columns = pl.ds(pl.multiple_of(chunk * CHUNK, CHUNK), CHUNK)
        gain = gain_ref[:, columns]
        weight = wkv[columns, :]
        for block in range(blocks):
            part = slice(block * rows, (block + 1) * rows)
            value = hbuf[slot, part, :].astype(F32)
            square = value * value
            partial = square[:, :128]
            for lane in range(1, CHUNK // 128):
                partial = partial + square[:, lane * 128 : (lane + 1) * 128]
            ssq[part, :] += partial
            scaled = (value * gain).astype(BF16)
            xg[part, columns] = scaled
            acc_kv[part, :] += jnp.dot(scaled, weight, preferred_element_type=F32)

    def scale_of(part):
        mean = jnp.sum(ssq[part, :], axis=1, keepdims=True) * (1.0 / width)
        return lax.rsqrt(mean + 1e-05)

    pieces = []
    for block in range(blocks):
        part = slice(block * rows, (block + 1) * rows)
        scale = scale_of(part)
        keys = rotated(acc_kv[part, :HEAD_DIM] * scale, cos[part, :], sin[part, :])
        values = acc_kv[part, HEAD_DIM:] * scale
        pieces.append(jnp.concatenate([keys.astype(BF16), values.astype(BF16)], axis=1))
    both = jnp.dot(sel[...], jnp.concatenate(pieces, axis=0), preferred_element_type=F32)
    live = live_rows(counts_ref, slots // BLOCK)
    low = jnp.minimum(live, 256)
    lane = lax.broadcasted_iota(jnp.int32, (16, HEAD_DIM), 1)
    first = lax.broadcasted_iota(jnp.int32, (16, HEAD_DIM), 0) == 0
    tag = jnp.where(lane == 0, low, jnp.where(lane == 1, live - low, 0))
    kvbuf[shard, 0, :slots] = both[:, :HEAD_DIM].astype(BF16)
    kvbuf[shard, 0, slots:] = jnp.where(first, tag, 0).astype(F32).astype(BF16)
    kvbuf[shard, 1, :slots] = both[:, HEAD_DIM:].astype(BF16)

    def kv_part(source, part):
        return kvbuf.at[source, 0] if part == 0 else kvbuf.at[source, 1, :slots]

    outs = []

    def send_kv(source, part, peer):
        ref = kv_part(source, part)
        push(ref, ref, kv_send.at[len(sends)], kv_recv.at[source, part], peer)

    def keep(source, part):
        ref = kv_part(source, part)
        to = kv_hbm.at[source, part]
        copy = pltpu.make_async_copy(ref.at[:slots] if part == 0 else ref, to, out_sem.at[source, part])
        copy.start()
        outs.append(copy)

    def receive_kv(source, part, peers):
        landed(kv_part(source, part), kv_recv.at[source, part])
        for peer in peers:
            send_kv(source, part, peer)
        keep(source, part)

    for part in range(2):
        send_kv(shard, part, across)
        send_kv(shard, part, up)
        send_kv(shard, part, down)
        send_kv(shard, part, mate)
        keep(shard, part)

    copies_w[2].wait()
    heads = wq.shape[1] // HEAD_DIM
    factor = HEAD_DIM ** (-0.5) * 1.4426950408889634

    @pl.loop(0, blocks)
    def _(block):
        part = pl.ds(pl.multiple_of(block * rows, rows), rows)
        product = jnp.dot(xg[part, :], wqv[...], preferred_element_type=F32)
        scale = scale_of(part) * factor
        for head in range(heads):
            lanes = slice(head * HEAD_DIM, (head + 1) * HEAD_DIM)
            turned = rotated(product[:, lanes] * scale, cos[part, :], sin[part, :])
            acc_q[part, lanes] = turned.astype(BF16)

    picked = jnp.dot(sel[...], acc_q[...], preferred_element_type=F32)
    for head in range(heads):
        q_out[head] = picked[:, head * HEAD_DIM : (head + 1) * HEAD_DIM].astype(BF16)

    landed(relay.at[0], w_recv.at[2])
    push(relay.at[0], slot_part(x_prev, own_row, quarter), w_send.at[4], w_recv.at[4], right)
    landed(relay.at[1], w_recv.at[3])
    push(
        relay.at[1], slot_part(x_next, own_row + quarter, quarter), w_send.at[5], w_recv.at[5], left
    )

    def ring(plane):
        prev, following = shard_at(plane, y_prev, core), shard_at(plane, y_next, core)
        receive_kv(prev, 0, [up, mate])
        receive_kv(following, 0, [mate])
        receive_kv(following, 1, [down, mate])
        receive_kv(prev, 1, [mate])

    ring(zh)
    other = 1 - zh
    for part in range(2):
        receive_kv(shard_at(other, y, core), part, [up, down, mate])
    for part in range(2):
        receive_kv(shard_at(zh, y_far, core), part, [mate])
    ring(other)

    def pass_on(source, row, count, received, index):
        ref = slot_part(source, row, count)
        landed(ref, w_recv.at[received])
        push(ref, ref, w_send.at[index], w_recv.at[index], mate)

    pass_on(x_prev, own_row, half_rows, 0, 6)
    pass_on(x_next, own_row, half_rows, 1, 7)
    for part in range(2):
        receive_kv(shard_at(other, y_far, core), part, [mate])
    pass_on(x_far, own_row, quarter, 4, 8)
    pass_on(x_far, own_row + quarter, quarter, 5, 9)

    for plane in range(2):
        for row in range(4):
            for part in range(2):
                receive_kv(shard_at(plane, row, 1 - core), part, [])
    mate_row = (1 - core) * half_rows
    landed(slot_part(x_prev, mate_row, half_rows), w_recv.at[6])
    landed(slot_part(x_next, mate_row, half_rows), w_recv.at[7])
    landed(slot_part(x_far, mate_row, quarter), w_recv.at[8])
    landed(slot_part(x_far, mate_row + quarter, quarter), w_recv.at[9])
    for source in range(kvbuf.shape[0]):
        tag = jnp.sum(kvbuf[source, 0, slots:].astype(F32))
        live_out[source] = tag.astype(jnp.int32)
    for copy in sends:
        copy.wait_send()
    for copy in outs:
        copy.wait()


def smem():
    return pl.BlockSpec(memory_space=pltpu.SMEM)


def vmem():
    return pl.BlockSpec(memory_space=pltpu.VMEM)


def hbm():
    return pl.BlockSpec(memory_space=pl.ANY)


def front(counts, pos, gain, small, big, hidden, wq, wk, wv, wo):
    seq, width = hidden.shape
    slots = pos.shape[1]
    heads = wq.shape[1] // HEAD_DIM
    shards = big.shape[0]
    wide = wo.shape[1] // 4
    return pl.pallas_call(
        front_kernel,
        out_shape=(
            jax.ShapeDtypeStruct((heads, slots, HEAD_DIM), BF16),
            jax.ShapeDtypeStruct((shards,), jnp.int32),
            jax.ShapeDtypeStruct((shards, 2, slots, HEAD_DIM), BF16),
            jax.ShapeDtypeStruct((4, wo.shape[0], wide), BF16),
        ),
        in_specs=[smem(), vmem(), vmem(), vmem(), hbm(), hbm(), hbm(), hbm(), hbm(), hbm()],
        out_specs=(vmem(), smem(), hbm(), hbm()),
        scratch_shapes=[
            pltpu.VMEM((3, seq, CHUNK), BF16),
            pltpu.VMEM((width, 2 * HEAD_DIM), BF16),
            pltpu.VMEM(wq.shape, BF16),
            pltpu.VMEM((seq, width), BF16),
            pltpu.VMEM((seq, 2 * HEAD_DIM), F32),
            pltpu.VMEM((seq, heads * HEAD_DIM), BF16),
            pltpu.VMEM((seq, 128), F32),
            pltpu.VMEM((seq, HEAD_DIM), F32),
            pltpu.VMEM((seq, HEAD_DIM), F32),
            pltpu.VMEM((slots, seq), BF16),
            pltpu.VMEM(big.shape[1:], F32),
            pltpu.VMEM((shards, 2, slots + 16, HEAD_DIM), BF16),
            pltpu.VMEM((2, wo.shape[0] // 4, wide), BF16),
            pltpu.SemaphoreType.DMA((3,)),
            pltpu.SemaphoreType.DMA((4,)),
            pltpu.SemaphoreType.DMA((48,)),
            pltpu.SemaphoreType.DMA((shards, 2)),
            pltpu.SemaphoreType.DMA((10,)),
            pltpu.SemaphoreType.DMA((10,)),
            pltpu.SemaphoreType.DMA((shards, 2)),
        ],
        compiler_params=pltpu.CompilerParams(
            vmem_limit_bytes=VMEM_LIMIT, collective_id=0, has_side_effects=True
        ),
        name="front",
    )(counts, pos, gain, small, big, hidden, wq, wk, wv, wo)


def attend_kernel(live_ref, q_ref, kv, out_ref, keys, values, best, acc, kv_ref, sem):
    shards, _, slots, dim = kv.shape
    heads = q_ref.shape[0]
    me = lax.axis_index(CTX)

    def fetch(shard):
        return pltpu.make_async_copy(kv.at[shard], kv_ref.at[shard], sem.at[shard])

    @pl.loop(0, me + 1)
    def _(shard):
        fetch(shard).start()

    lane = lax.broadcasted_iota(jnp.int32, (slots, dim), 1)
    row = lax.broadcasted_iota(jnp.int32, (slots, dim), 0)

    def place(shard, start):
        live = live_ref[shard]
        fetch(shard).wait()
        part = pl.ds(pl.multiple_of(start, 16), slots)
        keys[part, :dim] = kv_ref[shard, 0]
        keys[part, dim:] = jnp.where((lane == 0) & (row >= live), -1e30, 0.0).astype(BF16)
        values[part, :] = kv_ref[shard, 1]
        return start + (live + 15) // 16 * 16

    own = lax.fori_loop(0, me, place, jnp.int32(0))
    place(me, own)
    full = own // KEY_CHUNK
    tile = 128
    ones = jnp.where(lane == 0, 1.0, 0.0).astype(BF16)
    lane_q = lax.broadcasted_iota(jnp.int32, (heads * tile, dim), 1)
    ones_q = jnp.where(lane_q == 0, 1.0, 0.0).astype(BF16)
    tail = pl.ds(pl.multiple_of(own + slots, 16), KEY_CHUNK)
    keys[tail, :dim] = jnp.zeros((KEY_CHUNK, dim), BF16)
    keys[tail, dim:] = jnp.where(lane == 0, -1e30, 0.0).astype(BF16)
    values[tail, :] = jnp.zeros((KEY_CHUNK, dim), BF16)

    used = (live_ref[me] + tile - 1) // tile

    @pl.loop(used, slots // tile)
    def _(block):
        rows = pl.ds(pl.multiple_of(block * tile, tile), tile)
        out_ref[rows, :] = jnp.zeros((tile, heads * dim), BF16)

    @pl.loop(0, used)
    def _(block):
        rows = pl.ds(pl.multiple_of(block * tile, tile), tile)
        query = jnp.concatenate([q_ref[head, rows, :] for head in range(heads)], axis=0)
        query = jnp.concatenate([query, ones_q], axis=1)
        best[...] = jnp.full_like(best, -3e38)
        acc[...] = jnp.zeros_like(acc)

        def step(chunk, masked):
            part = pl.ds(pl.multiple_of(chunk * KEY_CHUNK, KEY_CHUNK), KEY_CHUNK)
            score = lax.dot_general(
                query, keys[part, :], (((1,), (1,)), ((), ())), preferred_element_type=F32
            )
            if masked:
                key_at = lax.broadcasted_iota(jnp.int32, score.shape, 1) + chunk * KEY_CHUNK
                query_at = lax.broadcasted_iota(jnp.int32, score.shape, 0)
                limit = jnp.bitwise_and(query_at, tile - 1) + (own + block * tile)
                score = jnp.where(key_at <= limit, score, -1e30)
            old = best[...]
            new = jnp.maximum(old, jnp.max(score, axis=1, keepdims=True))
            weight = jnp.exp2(score - new[:, :1]).astype(BF16)
            both = jnp.concatenate([values[part, :], ones], axis=1)
            product = jnp.dot(weight, both, preferred_element_type=F32)
            factor = jnp.exp2(old - new)
            acc[:, :dim] = acc[:, :dim] * factor + product[:, :dim]
            acc[:, dim:] = acc[:, dim:] * factor + product[:, dim:]
            best[...] = new

        @pl.loop(0, full)
        def _(chunk):
            step(chunk, False)

        last = (own + (block + 1) * tile + KEY_CHUNK - 1) // KEY_CHUNK

        @pl.loop(full, last)
        def _(chunk):
            step(chunk, True)

        total = acc[:, dim : dim + 1]
        result = acc[:, :dim] / total
        for head in range(heads):
            out_ref[rows, head * dim : (head + 1) * dim] = result[
                head * tile : (head + 1) * tile, :
            ].astype(BF16)


def attend(live, q, kv):
    heads, slots, dim = q.shape
    shards = kv.shape[0]
    length = shards * slots + KEY_CHUNK + 512
    return pl.pallas_call(
        attend_kernel,
        out_shape=jax.ShapeDtypeStruct((slots, heads * dim), BF16),
        in_specs=[smem(), vmem(), hbm()],
        out_specs=vmem(),
        scratch_shapes=[
            pltpu.VMEM((length, 2 * dim), BF16),
            pltpu.VMEM((length, dim), BF16),
            pltpu.VMEM((heads * 128, 128), F32),
            pltpu.VMEM((heads * 128, 2 * dim), F32),
            pltpu.VMEM(kv.shape, BF16),
            pltpu.SemaphoreType.DMA((shards,)),
        ],
        compiler_params=pltpu.CompilerParams(vmem_limit_bytes=VMEM_LIMIT),
        name="attend",
    )(live, q, kv)


def tail_kernel(
    counts_ref, pos_ref, router_ref, attn, wo, weights, hidden, out_ref,
    wv, landing, product, zout, zin, acc, place, own, local_sem, send, recv, zsend, zrecv,
):
    x, zl = lax.axis_index("x"), lax.axis_index("zl")
    x_next, x_prev, x_far = lax.rem(x + 1, 4), lax.rem(x + 3, 4), lax.rem(x + 2, 4)
    right, left, beside = {"x": x_next}, {"x": x_prev}, {"zl": 1 - zl}
    slots, feats = attn.shape
    seq, width = own.shape
    wide = weights.shape[2]
    rows = 128
    count = slots // rows
    half = feats // 2
    own_columns = pl.ds(pl.multiple_of(zl * width, width), width)
    other_columns = pl.ds(pl.multiple_of((1 - zl) * width, width), width)
    column = pl.ds(pl.multiple_of((x * 2 + zl) * width, width), width)
    loads = [
        pltpu.make_async_copy(
            wo.at[:, pl.ds(pl.multiple_of(x * wide, wide), wide)], wv.at[3], local_sem.at[3]
        ),
        pltpu.make_async_copy(weights.at[x_prev], wv.at[0], local_sem.at[0]),
        pltpu.make_async_copy(weights.at[x_next], wv.at[1], local_sem.at[1]),
        pltpu.make_async_copy(weights.at[x_far], wv.at[2], local_sem.at[2]),
        pltpu.make_async_copy(hidden.at[:, column], own, local_sem.at[4]),
    ]
    greeted = greet([right, left, beside])
    for load in loads:
        load.start()
    sends = []

    def push(src, dst, send_at, recv_at, peer):
        copy = pltpu.make_async_remote_copy(
            src_ref=src, dst_ref=dst, send_sem=send_at, recv_sem=recv_at,
            device_id=peer, device_id_type=MESH,
        )
        copy.start()
        sends.append(copy)

    def landed(dst, recv_at):
        pltpu.make_async_remote_copy(
            src_ref=dst, dst_ref=dst, send_sem=send.at[0, 0], recv_sem=recv_at,
            device_id=right, device_id_type=MESH,
        ).wait_recv()

    def part_of(index):
        return slice(index * rows, (index + 1) * rows)

    def send_own(index):
        part = part_of(index)
        push(attn.at[part], landing.at[0, part], send.at[index, 0], recv.at[index, 0], right)
        push(attn.at[part], landing.at[1, part], send.at[index, 1], recv.at[index, 1], left)

    greeted()
    send_own(0)
    send_own(1)

    compact = compact_positions(counts_ref, pos_ref, lax.axis_index(CTX) * seq, slots)
    compact = jnp.transpose(jnp.broadcast_to(compact.astype(F32), (slots, 128)))[:1, :]
    at = lax.broadcasted_iota(jnp.int32, (seq, slots), 0)
    place[...] = jnp.where(at == compact.astype(jnp.int32), 1.0, 0.0).astype(BF16)
    acc[...] = jnp.zeros_like(acc)
    for load in loads:
        load.wait()

    def near(index):
        part = part_of(index)
        product[part, :] = jnp.dot(attn[part, :], wv[3], preferred_element_type=F32)
        landed(landing.at[0, part], recv.at[index, 0])
        first = landing.at[0, part, :half]
        push(first, landing.at[2, part, :half], send.at[index, 2], recv.at[index, 2], right)
        landed(landing.at[1, part], recv.at[index, 1])
        second = landing.at[1, part, half:]
        push(second, landing.at[2, part, half:], send.at[index, 3], recv.at[index, 3], left)
        if index + 2 < count:
            send_own(index + 2)
        product[part, :] += jnp.dot(landing[0, part, :], wv[0], preferred_element_type=F32)
        product[part, :] += jnp.dot(landing[1, part, :], wv[1], preferred_element_type=F32)

    def far(index):
        part = part_of(index)
        landed(landing.at[2, part, :half], recv.at[index, 2])
        landed(landing.at[2, part, half:], recv.at[index, 3])
        value = landing[2, part, :]
        other = product[part, other_columns] + jnp.dot(
            value, wv[2, :, other_columns], preferred_element_type=F32
        )
        zout[part, :] = other.astype(BF16)
        push(zout.at[part], zin.at[part], zsend.at[index], zrecv.at[index], beside)
        product[part, own_columns] += jnp.dot(
            value, wv[2, :, own_columns], preferred_element_type=F32
        )

    def put(index):
        part = part_of(index)
        landed(zin.at[part], zrecv.at[index])
        total = product[part, own_columns] + zin[part, :].astype(F32)
        high = total.astype(BF16)
        low = (total - high.astype(F32)).astype(BF16)
        lanes = place[:, part]
        acc[...] += jnp.dot(
            jnp.concatenate([lanes, lanes], axis=1), jnp.concatenate([high, low], axis=0),
            preferred_element_type=F32,
        )

    for index in range(count + 2):
        if index < count:
            near(index)
        if 1 <= index <= count:
            far(index - 1)
        if index >= 2:
            put(index - 2)
    router = jnp.transpose(jnp.broadcast_to(router_ref[...], (128, seq)))[:, :1]
    out_ref[...] = (own[...].astype(F32) + router * acc[...]).astype(BF16)
    for copy in sends:
        copy.wait_send()


def tail(counts, pos, router, attn, wo, weights, hidden):
    seq = hidden.shape[0]
    slots, feats = attn.shape
    wide = weights.shape[2]
    width = wide // 2
    count = slots // 128
    return pl.pallas_call(
        tail_kernel,
        out_shape=jax.ShapeDtypeStruct((seq, width), BF16),
        in_specs=[smem(), vmem(), vmem(), vmem(), hbm(), hbm(), hbm()],
        out_specs=vmem(),
        scratch_shapes=[
            pltpu.VMEM(weights.shape, BF16),
            pltpu.VMEM((3, slots, feats), BF16),
            pltpu.VMEM((slots, wide), F32),
            pltpu.VMEM((slots, width), BF16),
            pltpu.VMEM((slots, width), BF16),
            pltpu.VMEM((seq, width), F32),
            pltpu.VMEM((seq, slots), BF16),
            pltpu.VMEM((seq, width), BF16),
            pltpu.SemaphoreType.DMA((5,)),
            pltpu.SemaphoreType.DMA((count, 4)),
            pltpu.SemaphoreType.DMA((count, 4)),
            pltpu.SemaphoreType.DMA((count,)),
            pltpu.SemaphoreType.DMA((count,)),
        ],
        compiler_params=pltpu.CompilerParams(
            vmem_limit_bytes=VMEM_LIMIT, collective_id=1, has_side_effects=True
        ),
        name="tail",
    )(counts, pos, router, attn, wo, weights, hidden)


def per_device(
    hidden, norm_gain, w_query, w_key, w_value, w_output, positions, counts, router_weight
):
    seq = hidden.shape[0]
    slots = positions.shape[0]
    shards = lax.axis_size(CTX)
    big, small = angle_tables(seq, shards)
    pos = positions.reshape(1, slots)
    q, live, gathered, weights = front(
        counts, pos, norm_gain.reshape(1, -1), jnp.asarray(small), jnp.asarray(big),
        hidden, w_query, w_key, w_value, w_output,
    )
    attn = attend(live, q, gathered)
    router = router_weight.reshape(1, seq)
    return tail(counts, pos, router, attn, w_output, weights, hidden)


def solution(mesh):
    finer = Mesh(mesh.devices.reshape(2, 4, 2, 4, 2), CTX + TP)
    return jax.shard_map(
        per_device,
        mesh=finer,
        in_specs=(
            P(CTX, None), P(), P(None, TP), P(None, TP), P(None, TP), P(TP, None),
            P(CTX), P(CTX), P(CTX),
        ),
        out_specs=P(CTX, TP),
        check_vma=False,
    )
```

```python
import jax
import jax.numpy as jnp
import numpy as np
from jax import lax
from jax.experimental import pallas as pl
from jax.experimental.pallas import tpu as pltpu
from jax.sharding import Mesh
from jax.sharding import PartitionSpec as P

HEAD_DIM = 128
BLOCK = 128
CTX = ("zh", "y", "core")
TP = ("x", "zl")
CHUNK = 512
KEY_CHUNK = 512
SIZES = (2048, 1024, 512)
STEP = 32
F32 = jnp.float32
BF16 = jnp.bfloat16
VMEM_LIMIT = 60 * 1024 * 1024
MESH = pl.DeviceIdType.MESH


def freq_table():
    half = HEAD_DIM // 2
    one = 500000.0 ** (-2.0 * np.arange(half, dtype=np.float64) / HEAD_DIM)
    return np.concatenate([one, one])


def angle_tables(seq, shards):
    freq = freq_table()
    sign = np.concatenate([-np.ones(HEAD_DIM // 2), np.ones(HEAD_DIM // 2)])
    coarse = np.arange(0, seq * shards, STEP, dtype=np.float64)[:, None] * freq[None, :]
    fine = np.arange(STEP, dtype=np.float64)[:, None] * freq[None, :]
    big = np.stack([np.cos(coarse), np.sin(coarse)]).astype(np.float32)
    small = np.stack([np.cos(fine), np.sin(fine), np.tile(sign, (STEP, 1))]).astype(np.float32)
    return big.reshape(2, shards, seq // STEP, HEAD_DIM).transpose(1, 0, 2, 3), small


def live_rows(counts_ref, blocks):
    total = counts_ref[0]
    for block in range(1, blocks):
        total = total + counts_ref[block]
    return total


def compact_positions(counts_ref, pos_ref, base, slots):
    lane = lax.broadcasted_iota(jnp.int32, (1, BLOCK), 1)
    row = lax.broadcasted_iota(jnp.int32, (slots, BLOCK), 0)
    start = jnp.int32(0)
    total = jnp.zeros((slots, BLOCK), F32)
    for block in range(slots // BLOCK):
        count = counts_ref[block]
        place = jnp.where(lane < count, lane + start, -1)
        value = (pos_ref[:, block * BLOCK : (block + 1) * BLOCK] - (base - 1)).astype(F32)
        total = total + jnp.where(place == row, value, 0.0)
        start = start + count
    return jnp.sum(total, axis=1, keepdims=True).astype(jnp.int32) - 1


def select_matrix(counts_ref, pos_ref, base, slots, seq):
    column = compact_positions(counts_ref, pos_ref, base, slots)
    place = lax.broadcasted_iota(jnp.int32, (slots, seq), 1)
    return jnp.where(place == column, 1.0, 0.0).astype(BF16)


def rotated(field, cos, sin):
    return field * cos + pltpu.roll(field, HEAD_DIM // 2, 1) * sin


def greet(peers):
    barrier = pltpu.get_barrier_semaphore()
    for peer in peers:
        pl.semaphore_signal(barrier, inc=1, device_id=peer, device_id_type=MESH)

    def wait():
        pl.semaphore_wait(barrier, len(peers))

    return wait


def front_kernel(
    counts_ref, pos_ref, gain_ref, small_ref, big, hidden, wq, wk, wv, wo,
    q_out, live_out, kv_hbm, w_out,
    hbuf, wkv, wqv, xg, acc_kv, acc_q, ssq, cos, sin, sel, bigv, kvbuf, relay,
    hsem, wsem, kv_send, kv_recv, w_send, w_recv, out_sem,
):
    zh, y, core = lax.axis_index("zh"), lax.axis_index("y"), lax.axis_index("core")
    x = lax.axis_index("x")
    y_next, y_prev, y_far = lax.rem(y + 1, 4), lax.rem(y + 3, 4), lax.rem(y + 2, 4)
    x_next, x_prev, x_far = lax.rem(x + 1, 4), lax.rem(x + 3, 4), lax.rem(x + 2, 4)
    mate, up, down = {"core": 1 - core}, {"y": y_next}, {"y": y_prev}
    across, right, left = {"zh": 1 - zh}, {"x": x_next}, {"x": x_prev}

    def shard_at(plane, row, side):
        return (plane * 4 + row) * 2 + side

    shard = shard_at(zh, y, core)
    seq, width = hidden.shape
    slots = pos_ref.shape[1]
    chunks = width // CHUNK
    rows = 256
    blocks = seq // rows
    copies_w = [
        pltpu.make_async_copy(wk, wkv.at[:, :HEAD_DIM], wsem.at[0]),
        pltpu.make_async_copy(wv, wkv.at[:, HEAD_DIM:], wsem.at[1]),
        pltpu.make_async_copy(wq, wqv, wsem.at[2]),
    ]
    copy_big = pltpu.make_async_copy(big.at[shard], bigv, wsem.at[3])

    def fetch(chunk):
        columns = pl.ds(pl.multiple_of(chunk * CHUNK, CHUNK), CHUNK)
        slot = lax.rem(chunk, 3)
        return pltpu.make_async_copy(hidden.at[:, columns], hbuf.at[slot], hsem.at[slot])

    copy_big.start()
    copies_w[0].start()
    copies_w[1].start()
    fetch(0).start()
    fetch(1).start()
    copies_w[2].start()
    greeted = greet([mate, up, down, across, right, left])

    base = shard * seq
    sel[...] = select_matrix(counts_ref, pos_ref, base, slots, seq)
    copy_big.wait()
    for step in range(seq // STEP):
        part = slice(step * STEP, (step + 1) * STEP)
        cb, sb = bigv[0, step : step + 1, :], bigv[1, step : step + 1, :]
        cf, sf, sign = small_ref[0], small_ref[1], small_ref[2]
        cos[part, :] = cb * cf - sb * sf
        sin[part, :] = (sb * cf + cb * sf) * sign

    sends = []

    def push(src, dst, send, recv, peer):
        copy = pltpu.make_async_remote_copy(
            src_ref=src, dst_ref=dst, send_sem=send, recv_sem=recv,
            device_id=peer, device_id_type=MESH,
        )
        copy.start()
        sends.append(copy)

    def landed(dst, recv):
        pltpu.make_async_remote_copy(
            src_ref=dst, dst_ref=dst, send_sem=w_send.at[0], recv_sem=recv,
            device_id=mate, device_id_type=MESH,
        ).wait_recv()

    half_rows = wo.shape[0] // 2
    quarter = half_rows // 2
    own_row = core * half_rows
    wide = wo.shape[1] // 4

    def wo_part(row, count, column):
        return wo.at[
            pl.ds(pl.multiple_of(row, quarter), count),
            pl.ds(pl.multiple_of(column * wide, wide), wide),
        ]

    def slot_part(source, row, count):
        return w_out.at[source, pl.ds(pl.multiple_of(row, quarter), count), :]

    greeted()
    push(wo_part(own_row, quarter, x_far), relay.at[0], w_send.at[0], w_recv.at[2], right)
    push(
        wo_part(own_row + quarter, quarter, x_far), relay.at[1], w_send.at[1], w_recv.at[3], left
    )
    push(
        wo_part(own_row, half_rows, x_next), slot_part(x, own_row, half_rows),
        w_send.at[2], w_recv.at[0], right,
    )
    push(
        wo_part(own_row, half_rows, x_prev), slot_part(x, own_row, half_rows),
        w_send.at[3], w_recv.at[1], left,
    )

    acc_kv[...] = jnp.zeros_like(acc_kv)
    ssq[...] = jnp.zeros_like(ssq)
    copies_w[0].wait()
    copies_w[1].wait()

    @pl.loop(0, chunks)
    def _(chunk):
        fetch(chunk).wait()

        @pl.when(chunk + 2 < chunks)
        def _():
            fetch(chunk + 2).start()

        slot = lax.rem(chunk, 3)
        columns = pl.ds(pl.multiple_of(chunk * CHUNK, CHUNK), CHUNK)
        gain = gain_ref[:, columns]
        weight = wkv[columns, :]
        for block in range(blocks):
            part = slice(block * rows, (block + 1) * rows)
            value = hbuf[slot, part, :].astype(F32)
            square = value * value
            partial = square[:, :128]
            for lane in range(1, CHUNK // 128):
                partial = partial + square[:, lane * 128 : (lane + 1) * 128]
            ssq[part, :] += partial
            scaled = (value * gain).astype(BF16)
            xg[part, columns] = scaled
            acc_kv[part, :] += jnp.dot(scaled, weight, preferred_element_type=F32)

    def scale_of(part):
        mean = jnp.sum(ssq[part, :], axis=1, keepdims=True) * (1.0 / width)
        return lax.rsqrt(mean + 1e-05)

    pieces = []
    for block in range(blocks):
        part = slice(block * rows, (block + 1) * rows)
        scale = scale_of(part)
        keys = rotated(acc_kv[part, :HEAD_DIM] * scale, cos[part, :], sin[part, :])
        values = acc_kv[part, HEAD_DIM:] * scale
        pieces.append(jnp.concatenate([keys.astype(BF16), values.astype(BF16)], axis=1))
    both = jnp.dot(sel[...], jnp.concatenate(pieces, axis=0), preferred_element_type=F32)
    live = live_rows(counts_ref, slots // BLOCK)
    low = jnp.minimum(live, 256)
    lane = lax.broadcasted_iota(jnp.int32, (16, HEAD_DIM), 1)
    first = lax.broadcasted_iota(jnp.int32, (16, HEAD_DIM), 0) == 0
    tag = jnp.where(lane == 0, low, jnp.where(lane == 1, live - low, 0))
    kvbuf[shard, 0, :slots] = both[:, :HEAD_DIM].astype(BF16)
    kvbuf[shard, 0, slots:] = jnp.where(first, tag, 0).astype(F32).astype(BF16)
    kvbuf[shard, 1, :slots] = both[:, HEAD_DIM:].astype(BF16)

    def kv_part(source, part):
        return kvbuf.at[source, 0] if part == 0 else kvbuf.at[source, 1, :slots]

    outs = []

    def send_kv(source, part, peer):
        ref = kv_part(source, part)
        push(ref, ref, kv_send.at[len(sends)], kv_recv.at[source, part], peer)

    def keep(source, part):
        ref = kv_part(source, part)
        to = kv_hbm.at[source, part]
        copy = pltpu.make_async_copy(ref.at[:slots] if part == 0 else ref, to, out_sem.at[source, part])
        copy.start()
        outs.append(copy)

    def receive_kv(source, part, peers):
        landed(kv_part(source, part), kv_recv.at[source, part])
        for peer in peers:
            send_kv(source, part, peer)
        keep(source, part)

    for part in range(2):
        send_kv(shard, part, across)
        send_kv(shard, part, up)
        send_kv(shard, part, down)
        send_kv(shard, part, mate)
        keep(shard, part)

    copies_w[2].wait()
    heads = wq.shape[1] // HEAD_DIM
    factor = HEAD_DIM ** (-0.5) * 1.4426950408889634

    @pl.loop(0, blocks)
    def _(block):
        part = pl.ds(pl.multiple_of(block * rows, rows), rows)
        product = jnp.dot(xg[part, :], wqv[...], preferred_element_type=F32)
        scale = scale_of(part) * factor
        for head in range(heads):
            lanes = slice(head * HEAD_DIM, (head + 1) * HEAD_DIM)
            turned = rotated(product[:, lanes] * scale, cos[part, :], sin[part, :])
            acc_q[part, lanes] = turned.astype(BF16)

    picked = jnp.dot(sel[...], acc_q[...], preferred_element_type=F32)
    for head in range(heads):
        q_out[head] = picked[:, head * HEAD_DIM : (head + 1) * HEAD_DIM].astype(BF16)

    landed(relay.at[0], w_recv.at[2])
    push(relay.at[0], slot_part(x_prev, own_row, quarter), w_send.at[4], w_recv.at[4], right)
    landed(relay.at[1], w_recv.at[3])
    push(
        relay.at[1], slot_part(x_next, own_row + quarter, quarter), w_send.at[5], w_recv.at[5], left
    )

    def ring(plane):
        prev, following = shard_at(plane, y_prev, core), shard_at(plane, y_next, core)
        receive_kv(prev, 0, [up, mate])
        receive_kv(following, 0, [mate])
        receive_kv(following, 1, [down, mate])
        receive_kv(prev, 1, [mate])

    ring(zh)
    other = 1 - zh
    for part in range(2):
        receive_kv(shard_at(other, y, core), part, [up, down, mate])
    for part in range(2):
        receive_kv(shard_at(zh, y_far, core), part, [mate])
    ring(other)

    def pass_on(source, row, count, received, index):
        ref = slot_part(source, row, count)
        landed(ref, w_recv.at[received])
        push(ref, ref, w_send.at[index], w_recv.at[index], mate)

    pass_on(x_prev, own_row, half_rows, 0, 6)
    pass_on(x_next, own_row, half_rows, 1, 7)
    for part in range(2):
        receive_kv(shard_at(other, y_far, core), part, [mate])
    pass_on(x_far, own_row, quarter, 4, 8)
    pass_on(x_far, own_row + quarter, quarter, 5, 9)

    for plane in range(2):
        for row in range(4):
            for part in range(2):
                receive_kv(shard_at(plane, row, 1 - core), part, [])
    mate_row = (1 - core) * half_rows
    landed(slot_part(x_prev, mate_row, half_rows), w_recv.at[6])
    landed(slot_part(x_next, mate_row, half_rows), w_recv.at[7])
    landed(slot_part(x_far, mate_row, quarter), w_recv.at[8])
    landed(slot_part(x_far, mate_row + quarter, quarter), w_recv.at[9])
    for source in range(kvbuf.shape[0]):
        tag = jnp.sum(kvbuf[source, 0, slots:].astype(F32))
        live_out[source] = tag.astype(jnp.int32)
    for copy in sends:
        copy.wait_send()
    for copy in outs:
        copy.wait()


def smem():
    return pl.BlockSpec(memory_space=pltpu.SMEM)


def vmem():
    return pl.BlockSpec(memory_space=pltpu.VMEM)


def hbm():
    return pl.BlockSpec(memory_space=pl.ANY)


def front(counts, pos, gain, small, big, hidden, wq, wk, wv, wo):
    seq, width = hidden.shape
    slots = pos.shape[1]
    heads = wq.shape[1] // HEAD_DIM
    shards = big.shape[0]
    wide = wo.shape[1] // 4
    return pl.pallas_call(
        front_kernel,
        out_shape=(
            jax.ShapeDtypeStruct((heads, slots, HEAD_DIM), BF16),
            jax.ShapeDtypeStruct((shards,), jnp.int32),
            jax.ShapeDtypeStruct((shards, 2, slots, HEAD_DIM), BF16),
            jax.ShapeDtypeStruct((4, wo.shape[0], wide), BF16),
        ),
        in_specs=[smem(), vmem(), vmem(), vmem(), hbm(), hbm(), hbm(), hbm(), hbm(), hbm()],
        out_specs=(vmem(), smem(), hbm(), hbm()),
        scratch_shapes=[
            pltpu.VMEM((3, seq, CHUNK), BF16),
            pltpu.VMEM((width, 2 * HEAD_DIM), BF16),
            pltpu.VMEM(wq.shape, BF16),
            pltpu.VMEM((seq, width), BF16),
            pltpu.VMEM((seq, 2 * HEAD_DIM), F32),
            pltpu.VMEM((seq, heads * HEAD_DIM), BF16),
            pltpu.VMEM((seq, 128), F32),
            pltpu.VMEM((seq, HEAD_DIM), F32),
            pltpu.VMEM((seq, HEAD_DIM), F32),
            pltpu.VMEM((slots, seq), BF16),
            pltpu.VMEM(big.shape[1:], F32),
            pltpu.VMEM((shards, 2, slots + 16, HEAD_DIM), BF16),
            pltpu.VMEM((2, wo.shape[0] // 4, wide), BF16),
            pltpu.SemaphoreType.DMA((3,)),
            pltpu.SemaphoreType.DMA((4,)),
            pltpu.SemaphoreType.DMA((48,)),
            pltpu.SemaphoreType.DMA((shards, 2)),
            pltpu.SemaphoreType.DMA((10,)),
            pltpu.SemaphoreType.DMA((10,)),
            pltpu.SemaphoreType.DMA((shards, 2)),
        ],
        compiler_params=pltpu.CompilerParams(
            vmem_limit_bytes=VMEM_LIMIT, collective_id=0, has_side_effects=True
        ),
        name="front",
    )(counts, pos, gain, small, big, hidden, wq, wk, wv, wo)


def attend_kernel(live_ref, q_ref, kv, out_ref, keys, values, best, acc, score, sem):
    shards, _, slots, dim = kv.shape
    heads = q_ref.shape[0]
    me = lax.axis_index(CTX)
    tile = 128
    lane = lax.broadcasted_iota(jnp.int32, (KEY_CHUNK, dim), 1)
    ones = jnp.where(lane == 0, 1.0, 0.0).astype(BF16)

    lane_q = lax.broadcasted_iota(jnp.int32, (heads * tile, dim), 1)
    ones_q = jnp.where(lane_q == 0, 1.0, 0.0).astype(BF16)
    lane_t = lax.broadcasted_iota(jnp.int32, (16, dim), 1)
    row_t = lax.broadcasted_iota(jnp.int32, (16, dim), 0)

    def each_piece(shard, start, act):
        units = jnp.right_shift(live_ref[shard] + 15, 4)
        size = slots
        while size >= 16:
            part = size // 16

            @pl.when(jnp.bitwise_and(units, part) != 0)
            def _(size=size, part=part):
                done = jnp.bitwise_and(units, -2 * part) * 16
                source = pl.ds(pl.multiple_of(done, 16), size)
                target = pl.ds(pl.multiple_of(start + done, 16), size)
                act(pltpu.make_async_copy(
                    kv.at[shard, 0, source, :], keys.at[target, :dim], sem.at[0, shard]
                ))
                act(pltpu.make_async_copy(
                    kv.at[shard, 1, source, :], values.at[target, :], sem.at[1, shard]
                ))

            size //= 2
        return start + units * 16

    def begin(shard, start):
        return each_piece(shard, start, lambda copy: copy.start())

    own = lax.fori_loop(0, me, begin, jnp.int32(0))
    end = begin(me, own)
    rest = pl.ds(pl.multiple_of(end, 16), KEY_CHUNK + tile)
    keys[rest, :dim] = jnp.zeros((KEY_CHUNK + tile, dim), BF16)
    values[rest, :] = jnp.zeros((KEY_CHUNK + tile, dim), BF16)

    @pl.loop(0, end // KEY_CHUNK + 2)
    def _(chunk):
        part = pl.ds(pl.multiple_of(chunk * KEY_CHUNK, KEY_CHUNK), KEY_CHUNK)
        keys[part, dim:] = jnp.zeros((KEY_CHUNK, dim), BF16)

    def close(shard, start):
        live = live_ref[shard]
        after = start + jnp.bitwise_and(live + 15, -16)
        dead = (lane_t == 0) & (row_t + (after - start - 16) >= live)
        keys[pl.ds(pl.multiple_of(after - 16, 16), 16), dim:] = jnp.where(
            dead, -1e30, 0.0
        ).astype(BF16)
        return after

    lax.fori_loop(0, me + 1, close, jnp.int32(0))

    used = (live_ref[me] + tile - 1) // tile

    @pl.loop(used, slots // tile)
    def _(block):
        rows = pl.ds(pl.multiple_of(block * tile, tile), tile)
        out_ref[rows, :] = jnp.zeros((tile, heads * dim), BF16)

    @pl.loop(0, me + 1)
    def _(shard):
        each_piece(shard, jnp.int32(0), lambda copy: copy.wait())

    full = own // KEY_CHUNK

    @pl.loop(0, used)
    def _(block):
        rows = pl.ds(pl.multiple_of(block * tile, tile), tile)
        query = jnp.concatenate([q_ref[head, rows, :] for head in range(heads)], axis=0)
        query = jnp.concatenate([query, ones_q], axis=1)
        best[...] = jnp.full_like(best, -3e38)
        acc[...] = jnp.zeros_like(acc)

        def look(chunk, size, masked):
            part = pl.ds(pl.multiple_of(chunk * size, size), size)
            found = lax.dot_general(
                query, keys[part, :], (((1,), (1,)), ((), ())), preferred_element_type=F32
            )
            if masked:
                key_at = lax.broadcasted_iota(jnp.int32, found.shape, 1) + chunk * size
                query_at = lax.broadcasted_iota(jnp.int32, found.shape, 0)
                limit = jnp.bitwise_and(query_at, tile - 1) + (own + block * tile)
                found = jnp.where(key_at <= limit, found, -1e30)
            score[:, part] = found
            most = found[:, :128]
            for at in range(128, size, 128):
                most = jnp.maximum(most, found[:, at : at + 128])
            best[...] = jnp.maximum(best[...], most)

        def use(chunk, size):
            part = pl.ds(pl.multiple_of(chunk * size, size), size)
            most = best[...]
            weight = jnp.concatenate(
                [
                    jnp.exp2(
                        score[:, pl.ds(pl.multiple_of(chunk * size + at, 128), 128)] - most
                    ).astype(BF16)
                    for at in range(0, size, 128)
                ],
                axis=1,
            )
            right = jnp.concatenate(
                [values[part, :], jnp.concatenate([ones] * (size // KEY_CHUNK), axis=0)], axis=1
            )
            acc[...] += jnp.dot(weight, right, preferred_element_type=F32)

        def cascade(amount, act):
            done = jnp.int32(0)
            for size in SIZES:
                ratio = size // KEY_CHUNK
                first, last = done // ratio, amount // ratio

                @pl.loop(first, last)
                def _(chunk, size=size):
                    act(chunk, size)

                done = last * ratio

        last = (own + (block + 1) * tile + KEY_CHUNK - 1) // KEY_CHUNK
        cascade(full, lambda chunk, size: look(chunk, size, False))

        @pl.loop(full, last)
        def _(chunk):
            look(chunk, KEY_CHUNK, True)

        best[...] = jnp.broadcast_to(jnp.max(best[...], axis=1, keepdims=True), best.shape)
        cascade(last, use)
        result = acc[:, :dim] / acc[:, dim : dim + 1]
        for head in range(heads):
            out_ref[rows, head * dim : (head + 1) * dim] = result[
                head * tile : (head + 1) * tile, :
            ].astype(BF16)


def attend(live, q, kv):
    heads, slots, dim = q.shape
    shards = kv.shape[0]
    length = shards * slots + 2 * KEY_CHUNK
    return pl.pallas_call(
        attend_kernel,
        out_shape=jax.ShapeDtypeStruct((slots, heads * dim), BF16),
        in_specs=[smem(), vmem(), hbm()],
        out_specs=vmem(),
        scratch_shapes=[
            pltpu.VMEM((length, 2 * dim), BF16),
            pltpu.VMEM((length, dim), BF16),
            pltpu.VMEM((heads * 128, 128), F32),
            pltpu.VMEM((heads * 128, 2 * dim), F32),
            pltpu.VMEM((heads * 128, length), F32),
            pltpu.SemaphoreType.DMA((2, shards)),
        ],
        compiler_params=pltpu.CompilerParams(vmem_limit_bytes=VMEM_LIMIT),
        name="attend",
    )(live, q, kv)


def tail_kernel(
    counts_ref, pos_ref, router_ref, attn, wo, weights, hidden, out_ref,
    wv, landing, product, zout, zin, acc, place, own, local_sem, send, recv, zsend, zrecv,
):
    x, zl = lax.axis_index("x"), lax.axis_index("zl")
    x_next, x_prev, x_far = lax.rem(x + 1, 4), lax.rem(x + 3, 4), lax.rem(x + 2, 4)
    right, left, beside = {"x": x_next}, {"x": x_prev}, {"zl": 1 - zl}
    slots, feats = attn.shape
    seq, width = own.shape
    wide = weights.shape[2]
    rows = 128
    count = slots // rows
    half = feats // 2
    own_columns = pl.ds(pl.multiple_of(zl * width, width), width)
    other_columns = pl.ds(pl.multiple_of((1 - zl) * width, width), width)
    column = pl.ds(pl.multiple_of((x * 2 + zl) * width, width), width)
    loads = [
        pltpu.make_async_copy(
            wo.at[:, pl.ds(pl.multiple_of(x * wide, wide), wide)], wv.at[3], local_sem.at[3]
        ),
        pltpu.make_async_copy(weights.at[x_prev], wv.at[0], local_sem.at[0]),
        pltpu.make_async_copy(weights.at[x_next], wv.at[1], local_sem.at[1]),
        pltpu.make_async_copy(weights.at[x_far], wv.at[2], local_sem.at[2]),
        pltpu.make_async_copy(hidden.at[:, column], own, local_sem.at[4]),
    ]
    greeted = greet([right, left, beside])
    for load in loads:
        load.start()
    sends = []

    def push(src, dst, send_at, recv_at, peer):
        copy = pltpu.make_async_remote_copy(
            src_ref=src, dst_ref=dst, send_sem=send_at, recv_sem=recv_at,
            device_id=peer, device_id_type=MESH,
        )
        copy.start()
        sends.append(copy)

    def landed(dst, recv_at):
        pltpu.make_async_remote_copy(
            src_ref=dst, dst_ref=dst, send_sem=send.at[0, 0], recv_sem=recv_at,
            device_id=right, device_id_type=MESH,
        ).wait_recv()

    def part_of(index):
        return slice(index * rows, (index + 1) * rows)

    def send_own(index):
        part = part_of(index)
        push(attn.at[part], landing.at[0, part], send.at[index, 0], recv.at[index, 0], right)
        push(attn.at[part], landing.at[1, part], send.at[index, 1], recv.at[index, 1], left)

    greeted()
    send_own(0)
    send_own(1)

    compact = compact_positions(counts_ref, pos_ref, lax.axis_index(CTX) * seq, slots)
    compact = jnp.transpose(jnp.broadcast_to(compact.astype(F32), (slots, 128)))[:1, :]
    at = lax.broadcasted_iota(jnp.int32, (seq, slots), 0)
    place[...] = jnp.where(at == compact.astype(jnp.int32), 1.0, 0.0).astype(BF16)
    acc[...] = jnp.zeros_like(acc)
    for load in loads:
        load.wait()

    def near(index):
        part = part_of(index)
        product[part, :] = jnp.dot(attn[part, :], wv[3], preferred_element_type=F32)
        landed(landing.at[0, part], recv.at[index, 0])
        first = landing.at[0, part, :half]
        push(first, landing.at[2, part, :half], send.at[index, 2], recv.at[index, 2], right)
        landed(landing.at[1, part], recv.at[index, 1])
        second = landing.at[1, part, half:]
        push(second, landing.at[2, part, half:], send.at[index, 3], recv.at[index, 3], left)
        if index + 2 < count:
            send_own(index + 2)
        product[part, :] += jnp.dot(landing[0, part, :], wv[0], preferred_element_type=F32)
        product[part, :] += jnp.dot(landing[1, part, :], wv[1], preferred_element_type=F32)

    def far(index):
        part = part_of(index)
        landed(landing.at[2, part, :half], recv.at[index, 2])
        landed(landing.at[2, part, half:], recv.at[index, 3])
        value = landing[2, part, :]
        other = product[part, other_columns] + jnp.dot(
            value, wv[2, :, other_columns], preferred_element_type=F32
        )
        zout[part, :] = other.astype(BF16)
        push(zout.at[part], zin.at[part], zsend.at[index], zrecv.at[index], beside)
        product[part, own_columns] += jnp.dot(
            value, wv[2, :, own_columns], preferred_element_type=F32
        )

    def put(index):
        part = part_of(index)
        landed(zin.at[part], zrecv.at[index])
        total = product[part, own_columns] + zin[part, :].astype(F32)
        high = total.astype(BF16)
        low = (total - high.astype(F32)).astype(BF16)
        lanes = place[:, part]
        acc[...] += jnp.dot(
            jnp.concatenate([lanes, lanes], axis=1), jnp.concatenate([high, low], axis=0),
            preferred_element_type=F32,
        )

    for index in range(count + 2):
        if index < count:
            near(index)
        if 1 <= index <= count:
            far(index - 1)
        if index >= 2:
            put(index - 2)
    router = jnp.transpose(jnp.broadcast_to(router_ref[...], (128, seq)))[:, :1]
    out_ref[...] = (own[...].astype(F32) + router * acc[...]).astype(BF16)
    for copy in sends:
        copy.wait_send()


def tail(counts, pos, router, attn, wo, weights, hidden):
    seq = hidden.shape[0]
    slots, feats = attn.shape
    wide = weights.shape[2]
    width = wide // 2
    count = slots // 128
    return pl.pallas_call(
        tail_kernel,
        out_shape=jax.ShapeDtypeStruct((seq, width), BF16),
        in_specs=[smem(), vmem(), vmem(), vmem(), hbm(), hbm(), hbm()],
        out_specs=vmem(),
        scratch_shapes=[
            pltpu.VMEM(weights.shape, BF16),
            pltpu.VMEM((3, slots, feats), BF16),
            pltpu.VMEM((slots, wide), F32),
            pltpu.VMEM((slots, width), BF16),
            pltpu.VMEM((slots, width), BF16),
            pltpu.VMEM((seq, width), F32),
            pltpu.VMEM((seq, slots), BF16),
            pltpu.VMEM((seq, width), BF16),
            pltpu.SemaphoreType.DMA((5,)),
            pltpu.SemaphoreType.DMA((count, 4)),
            pltpu.SemaphoreType.DMA((count, 4)),
            pltpu.SemaphoreType.DMA((count,)),
            pltpu.SemaphoreType.DMA((count,)),
        ],
        compiler_params=pltpu.CompilerParams(
            vmem_limit_bytes=VMEM_LIMIT, collective_id=1, has_side_effects=True
        ),
        name="tail",
    )(counts, pos, router, attn, wo, weights, hidden)


def per_device(
    hidden, norm_gain, w_query, w_key, w_value, w_output, positions, counts, router_weight
):
    seq = hidden.shape[0]
    slots = positions.shape[0]
    shards = lax.axis_size(CTX)
    big, small = angle_tables(seq, shards)
    pos = positions.reshape(1, slots)
    q, live, gathered, weights = front(
        counts, pos, norm_gain.reshape(1, -1), jnp.asarray(small), jnp.asarray(big),
        hidden, w_query, w_key, w_value, w_output,
    )
    attn = attend(live, q, gathered)
    router = router_weight.reshape(1, seq)
    return tail(counts, pos, router, attn, w_output, weights, hidden)


def solution(mesh):
    finer = Mesh(mesh.devices.reshape(2, 4, 2, 4, 2), CTX + TP)
    return jax.shard_map(
        per_device,
        mesh=finer,
        in_specs=(
            P(CTX, None), P(), P(None, TP), P(None, TP), P(None, TP), P(TP, None),
            P(CTX), P(CTX), P(CTX),
        ),
        out_specs=P(CTX, TP),
        check_vma=False,
    )
```

```python
import jax
import jax.numpy as jnp
import numpy as np
from jax import lax
from jax.experimental import pallas as pl
from jax.experimental.pallas import tpu as pltpu
from jax.sharding import Mesh
from jax.sharding import PartitionSpec as P

HEAD_DIM = 128
BLOCK = 128
CTX = ("zh", "y", "core")
TP = ("x", "zl")
CHUNK = 1024
KEY_CHUNK = 512
SIZES = (2048, 1024, 512)
STEP = 32
F32 = jnp.float32
BF16 = jnp.bfloat16
VMEM_LIMIT = 60 * 1024 * 1024
MESH = pl.DeviceIdType.MESH


def freq_table():
    half = HEAD_DIM // 2
    one = 500000.0 ** (-2.0 * np.arange(half, dtype=np.float64) / HEAD_DIM)
    return np.concatenate([one, one])


def angle_tables(seq, shards):
    freq = freq_table()
    sign = np.concatenate([-np.ones(HEAD_DIM // 2), np.ones(HEAD_DIM // 2)])
    coarse = np.arange(0, seq * shards, STEP, dtype=np.float64)[:, None] * freq[None, :]
    fine = np.arange(STEP, dtype=np.float64)[:, None] * freq[None, :]
    big = np.stack([np.cos(coarse), np.sin(coarse)]).astype(np.float32)
    small = np.stack([np.cos(fine), np.sin(fine), np.tile(sign, (STEP, 1))]).astype(np.float32)
    return big.reshape(2, shards, seq // STEP, HEAD_DIM).transpose(1, 0, 2, 3), small


def live_rows(counts_ref, blocks):
    total = counts_ref[0]
    for block in range(1, blocks):
        total = total + counts_ref[block]
    return total


def compact_positions(counts_ref, pos_ref, base, slots):
    lane = lax.broadcasted_iota(jnp.int32, (1, BLOCK), 1)
    row = lax.broadcasted_iota(jnp.int32, (slots, BLOCK), 0)
    start = jnp.int32(0)
    total = jnp.zeros((slots, BLOCK), F32)
    for block in range(slots // BLOCK):
        count = counts_ref[block]
        place = jnp.where(lane < count, lane + start, -1)
        value = (pos_ref[:, block * BLOCK : (block + 1) * BLOCK] - (base - 1)).astype(F32)
        total = total + jnp.where(place == row, value, 0.0)
        start = start + count
    return jnp.sum(total, axis=1, keepdims=True).astype(jnp.int32) - 1


def select_matrix(counts_ref, pos_ref, base, slots, seq):
    column = compact_positions(counts_ref, pos_ref, base, slots)
    place = lax.broadcasted_iota(jnp.int32, (slots, seq), 1)
    return jnp.where(place == column, 1.0, 0.0).astype(BF16)


def rotated(field, cos, sin):
    return field * cos + pltpu.roll(field, HEAD_DIM // 2, 1) * sin


def greet(peers):
    barrier = pltpu.get_barrier_semaphore()
    for peer in peers:
        pl.semaphore_signal(barrier, inc=1, device_id=peer, device_id_type=MESH)

    def wait():
        pl.semaphore_wait(barrier, len(peers))

    return wait


def front_kernel(
    counts, positions, gains, small, big, hidden, wq, wk, wv, wo,
    q_out, live_out, kv_hbm, w_out,
    hbuf, wkv, wqv, gain, acc_kv, acc_q, ssq, cos, sin, sel, bigv, kvbuf, relay,
    counts_ref, pos_ref, gain_row, small_ref,
    hsem, wsem, kv_send, kv_recv, w_send, w_recv, out_sem,
):
    zh, y, core = lax.axis_index("zh"), lax.axis_index("y"), lax.axis_index("core")
    x = lax.axis_index("x")
    y_next, y_prev, y_far = lax.rem(y + 1, 4), lax.rem(y + 3, 4), lax.rem(y + 2, 4)
    x_next, x_prev, x_far = lax.rem(x + 1, 4), lax.rem(x + 3, 4), lax.rem(x + 2, 4)
    mate, up, down = {"core": 1 - core}, {"y": y_next}, {"y": y_prev}
    across, right, left = {"zh": 1 - zh}, {"x": x_next}, {"x": x_prev}

    def shard_at(plane, row, side):
        return (plane * 4 + row) * 2 + side

    shard = shard_at(zh, y, core)
    seq, width = hidden.shape
    slots = positions.shape[1]
    chunks = width // CHUNK
    rows = 256
    blocks = seq // rows
    loads = [
        pltpu.make_async_copy(gains, gain_row, wsem.at[0]),
        pltpu.make_async_copy(wk, wkv.at[:, :HEAD_DIM], wsem.at[1]),
        pltpu.make_async_copy(wv, wkv.at[:, HEAD_DIM:], wsem.at[2]),
        pltpu.make_async_copy(counts, counts_ref, wsem.at[3]),
        pltpu.make_async_copy(positions, pos_ref, wsem.at[4]),
        pltpu.make_async_copy(big.at[shard], bigv, wsem.at[5]),
        pltpu.make_async_copy(small, small_ref, wsem.at[6]),
    ]
    load_q = pltpu.make_async_copy(wq, wqv, wsem.at[7])

    def fetch(chunk):
        columns = slice(chunk * CHUNK, (chunk + 1) * CHUNK)
        return pltpu.make_async_copy(hidden.at[:, columns], hbuf.at[:, columns], hsem.at[chunk])

    for load in loads:
        load.start()
    for chunk in range(chunks):
        fetch(chunk).start()
    load_q.start()
    greeted = greet([mate, up, down, across, right, left])

    loads[0].wait()
    for lanes in range(0, width, 128):
        column = jnp.broadcast_to(gain_row[:, lanes : lanes + 128], (128, 128))
        gain[lanes : lanes + 128, :] = jnp.transpose(column)
    for load in loads[1:]:
        load.wait()
    base = shard * seq
    sel[...] = select_matrix(counts_ref, pos_ref, base, slots, seq)
    for step in range(seq // STEP):
        part = slice(step * STEP, (step + 1) * STEP)
        cb, sb = bigv[0, step : step + 1, :], bigv[1, step : step + 1, :]
        cf, sf, sign = small_ref[0], small_ref[1], small_ref[2]
        cos[part, :] = cb * cf - sb * sf
        sin[part, :] = (sb * cf + cb * sf) * sign

    sends = []

    def push(src, dst, send, recv, peer):
        copy = pltpu.make_async_remote_copy(
            src_ref=src, dst_ref=dst, send_sem=send, recv_sem=recv,
            device_id=peer, device_id_type=MESH,
        )
        copy.start()
        sends.append(copy)

    def landed(dst, recv):
        pltpu.make_async_remote_copy(
            src_ref=dst, dst_ref=dst, send_sem=w_send.at[0], recv_sem=recv,
            device_id=mate, device_id_type=MESH,
        ).wait_recv()

    half_rows = wo.shape[0] // 2
    quarter = half_rows // 2
    own_row = core * half_rows
    wide = wo.shape[1] // 4

    def wo_part(row, count, column):
        return wo.at[
            pl.ds(pl.multiple_of(row, quarter), count),
            pl.ds(pl.multiple_of(column * wide, wide), wide),
        ]

    def slot_part(source, row, count):
        return w_out.at[source, pl.ds(pl.multiple_of(row, quarter), count), :]

    def start_weights():
        greeted()
        push(wo_part(own_row, quarter, x_far), relay.at[0], w_send.at[0], w_recv.at[2], right)
        push(
            wo_part(own_row + quarter, quarter, x_far), relay.at[1],
            w_send.at[1], w_recv.at[3], left,
        )
        push(
            wo_part(own_row, half_rows, x_next), slot_part(x, own_row, half_rows),
            w_send.at[2], w_recv.at[0], right,
        )
        push(
            wo_part(own_row, half_rows, x_prev), slot_part(x, own_row, half_rows),
            w_send.at[3], w_recv.at[1], left,
        )

    def scaled(ref, part):
        lanes = ref.shape[1] // 128
        factor = gain[part, :]
        for lane in range(lanes):
            column = slice(lane * 128, (lane + 1) * 128)
            ref[part, column] = (ref[part, column].astype(F32) * factor).astype(BF16)

    for chunk in range(chunks):
        columns = slice(chunk * CHUNK, (chunk + 1) * CHUNK)
        scaled(wkv, columns)
        weight = wkv[columns, :]
        fetch(chunk).wait()

        @pl.loop(0, blocks)
        def _(block, chunk=chunk, columns=columns, weight=weight):
            part = pl.ds(pl.multiple_of(block * rows, rows), rows)
            block_rows = hbuf[part, columns]
            value = block_rows.astype(F32)
            square = value * value
            partial = square[:, :128]
            for lane in range(1, CHUNK // 128):
                partial = partial + square[:, lane * 128 : (lane + 1) * 128]
            product = jnp.dot(block_rows, weight, preferred_element_type=F32)
            if chunk == 0:
                ssq[part, :] = partial
                acc_kv[part, :] = product
            else:
                ssq[part, :] += partial
                acc_kv[part, :] += product

        if chunk == 1:
            start_weights()

    def scale_of(part):
        mean = jnp.sum(ssq[part, :], axis=1, keepdims=True) * (1.0 / width)
        return lax.rsqrt(mean + 1e-05)

    pieces = []
    for block in range(blocks):
        part = slice(block * rows, (block + 1) * rows)
        scale = scale_of(part)
        keys = rotated(acc_kv[part, :HEAD_DIM] * scale, cos[part, :], sin[part, :])
        values = acc_kv[part, HEAD_DIM:] * scale
        pieces.append(jnp.concatenate([keys.astype(BF16), values.astype(BF16)], axis=1))
    both = jnp.dot(sel[...], jnp.concatenate(pieces, axis=0), preferred_element_type=F32)
    live = live_rows(counts_ref, slots // BLOCK)
    low = jnp.minimum(live, 256)
    lane = lax.broadcasted_iota(jnp.int32, (16, HEAD_DIM), 1)
    first = lax.broadcasted_iota(jnp.int32, (16, HEAD_DIM), 0) == 0
    tag = jnp.where(lane == 0, low, jnp.where(lane == 1, live - low, 0))
    kvbuf[shard, 0, :slots] = both[:, :HEAD_DIM].astype(BF16)
    kvbuf[shard, 0, slots:] = jnp.where(first, tag, 0).astype(F32).astype(BF16)
    kvbuf[shard, 1, :slots] = both[:, HEAD_DIM:].astype(BF16)

    def kv_part(source, part):
        return kvbuf.at[source, 0] if part == 0 else kvbuf.at[source, 1, :slots]

    outs = []

    def send_kv(source, part, peer):
        ref = kv_part(source, part)
        push(ref, ref, kv_send.at[len(sends)], kv_recv.at[source, part], peer)

    def keep(source, part):
        ref = kv_part(source, part)
        to = kv_hbm.at[source, part]
        copy = pltpu.make_async_copy(ref.at[:slots] if part == 0 else ref, to, out_sem.at[source, part])
        copy.start()
        outs.append(copy)

    def receive_kv(source, part, peers):
        landed(kv_part(source, part), kv_recv.at[source, part])
        for peer in peers:
            send_kv(source, part, peer)
        keep(source, part)

    for part in range(2):
        send_kv(shard, part, across)
        send_kv(shard, part, up)
        send_kv(shard, part, down)
        send_kv(shard, part, mate)
        keep(shard, part)

    load_q.wait()
    heads = wq.shape[1] // HEAD_DIM
    factor = HEAD_DIM ** (-0.5) * 1.4426950408889634

    @pl.loop(0, width // 512)
    def _(step):
        scaled(wqv, pl.ds(pl.multiple_of(step * 512, 512), 512))

    @pl.loop(0, blocks)
    def _(block):
        part = pl.ds(pl.multiple_of(block * rows, rows), rows)
        product = jnp.dot(hbuf[part, :], wqv[...], preferred_element_type=F32)
        scale = scale_of(part) * factor
        for head in range(heads):
            lanes = slice(head * HEAD_DIM, (head + 1) * HEAD_DIM)
            turned = rotated(product[:, lanes] * scale, cos[part, :], sin[part, :])
            acc_q[part, lanes] = turned.astype(BF16)

    picked = jnp.dot(sel[...], acc_q[...], preferred_element_type=F32)
    for head in range(heads):
        q_out[head] = picked[:, head * HEAD_DIM : (head + 1) * HEAD_DIM].astype(BF16)

    landed(relay.at[0], w_recv.at[2])
    push(relay.at[0], slot_part(x_prev, own_row, quarter), w_send.at[4], w_recv.at[4], right)
    landed(relay.at[1], w_recv.at[3])
    push(
        relay.at[1], slot_part(x_next, own_row + quarter, quarter), w_send.at[5], w_recv.at[5], left
    )

    other = 1 - zh
    prev, following = shard_at(zh, y_prev, core), shard_at(zh, y_next, core)
    opposite, far = shard_at(other, y, core), shard_at(zh, y_far, core)
    receive_kv(prev, 0, [up, mate])
    receive_kv(opposite, 0, [up, down, mate])
    receive_kv(following, 0, [mate])
    receive_kv(following, 1, [down, mate])
    receive_kv(opposite, 1, [up, down, mate])
    receive_kv(prev, 1, [mate])
    receive_kv(far, 0, [across, mate])
    receive_kv(far, 1, [across, mate])

    def pass_on(source, row, count, received, index):
        ref = slot_part(source, row, count)
        landed(ref, w_recv.at[received])
        push(ref, ref, w_send.at[index], w_recv.at[index], mate)

    for part in range(2):
        receive_kv(shard_at(other, y_prev, core), part, [mate])
        receive_kv(shard_at(other, y_next, core), part, [mate])
        receive_kv(shard_at(other, y_far, core), part, [mate])
    pass_on(x_prev, own_row, half_rows, 0, 6)
    pass_on(x_next, own_row, half_rows, 1, 7)
    pass_on(x_far, own_row, quarter, 4, 8)
    pass_on(x_far, own_row + quarter, quarter, 5, 9)

    for plane in range(2):
        for row in range(4):
            for part in range(2):
                receive_kv(shard_at(plane, row, 1 - core), part, [])
    tags = [kvbuf[source, 0, slots : slots + 1, :] for source in range(kvbuf.shape[0])]
    total = jnp.sum(jnp.concatenate(tags, axis=0).astype(F32), axis=1, keepdims=True)
    live_out[...] = jnp.broadcast_to(total, live_out.shape).astype(jnp.int32)
    mate_row = (1 - core) * half_rows
    landed(slot_part(x_prev, mate_row, half_rows), w_recv.at[6])
    landed(slot_part(x_next, mate_row, half_rows), w_recv.at[7])
    landed(slot_part(x_far, mate_row, quarter), w_recv.at[8])
    landed(slot_part(x_far, mate_row + quarter, quarter), w_recv.at[9])
    for copy in sends:
        copy.wait_send()
    for copy in outs:
        copy.wait()


def smem():
    return pl.BlockSpec(memory_space=pltpu.SMEM)


def vmem():
    return pl.BlockSpec(memory_space=pltpu.VMEM)


def hbm():
    return pl.BlockSpec(memory_space=pl.ANY)


def front(counts, pos, gain, small, big, hidden, wq, wk, wv, wo):
    seq, width = hidden.shape
    slots = pos.shape[1]
    heads = wq.shape[1] // HEAD_DIM
    shards = big.shape[0]
    wide = wo.shape[1] // 4
    return pl.pallas_call(
        front_kernel,
        out_shape=(
            jax.ShapeDtypeStruct((heads, slots, HEAD_DIM), BF16),
            jax.ShapeDtypeStruct((shards, 128), jnp.int32),
            jax.ShapeDtypeStruct((shards, 2, slots, HEAD_DIM), BF16),
            jax.ShapeDtypeStruct((4, wo.shape[0], wide), BF16),
        ),
        in_specs=[hbm()] * 10,
        out_specs=(vmem(), vmem(), hbm(), hbm()),
        scratch_shapes=[
            pltpu.VMEM((seq, width), BF16),
            pltpu.VMEM((width, 2 * HEAD_DIM), BF16),
            pltpu.VMEM(wq.shape, BF16),
            pltpu.VMEM((width, 128), F32),
            pltpu.VMEM((seq, 2 * HEAD_DIM), F32),
            pltpu.VMEM((seq, heads * HEAD_DIM), BF16),
            pltpu.VMEM((seq, 128), F32),
            pltpu.VMEM((seq, HEAD_DIM), F32),
            pltpu.VMEM((seq, HEAD_DIM), F32),
            pltpu.VMEM((slots, seq), BF16),
            pltpu.VMEM(big.shape[1:], F32),
            pltpu.VMEM((shards, 2, slots + 16, HEAD_DIM), BF16),
            pltpu.VMEM((2, wo.shape[0] // 4, wide), BF16),
            pltpu.SMEM(counts.shape, jnp.int32),
            pltpu.VMEM(pos.shape, jnp.int32),
            pltpu.VMEM(gain.shape, F32),
            pltpu.VMEM(small.shape, F32),
            pltpu.SemaphoreType.DMA((width // CHUNK,)),
            pltpu.SemaphoreType.DMA((8,)),
            pltpu.SemaphoreType.DMA((48,)),
            pltpu.SemaphoreType.DMA((shards, 2)),
            pltpu.SemaphoreType.DMA((10,)),
            pltpu.SemaphoreType.DMA((10,)),
            pltpu.SemaphoreType.DMA((shards, 2)),
        ],
        compiler_params=pltpu.CompilerParams(
            vmem_limit_bytes=VMEM_LIMIT, collective_id=0, has_side_effects=True
        ),
        name="front",
    )(counts, pos, gain, small, big, hidden, wq, wk, wv, wo)


def attend_kernel(live_ref, q_ref, kv, out_ref, keys, values, best, acc, score, sem):
    shards, _, slots, dim = kv.shape
    heads = q_ref.shape[0]
    me = lax.axis_index(CTX)
    tile = 128
    lane = lax.broadcasted_iota(jnp.int32, (KEY_CHUNK, dim), 1)
    ones = jnp.where(lane == 0, 1.0, 0.0).astype(BF16)

    lane_q = lax.broadcasted_iota(jnp.int32, (heads * tile, dim), 1)
    ones_q = jnp.where(lane_q == 0, 1.0, 0.0).astype(BF16)
    lane_t = lax.broadcasted_iota(jnp.int32, (16, dim), 1)
    row_t = lax.broadcasted_iota(jnp.int32, (16, dim), 0)

    def each_piece(shard, start, act):
        units = jnp.right_shift(live_ref[shard, 0] + 15, 4)
        size = slots
        while size >= 16:
            part = size // 16

            @pl.when(jnp.bitwise_and(units, part) != 0)
            def _(size=size, part=part):
                done = jnp.bitwise_and(units, -2 * part) * 16
                source = pl.ds(pl.multiple_of(done, 16), size)
                target = pl.ds(pl.multiple_of(start + done, 16), size)
                act(pltpu.make_async_copy(
                    kv.at[shard, 0, source, :], keys.at[target, :dim], sem.at[0, shard]
                ))
                act(pltpu.make_async_copy(
                    kv.at[shard, 1, source, :], values.at[target, :], sem.at[1, shard]
                ))

            size //= 2
        return start + units * 16

    def begin(shard, start):
        return each_piece(shard, start, lambda copy: copy.start())

    own = lax.fori_loop(0, me, begin, jnp.int32(0))
    end = begin(me, own)
    rest = pl.ds(pl.multiple_of(end, 16), KEY_CHUNK + tile)
    keys[rest, :dim] = jnp.zeros((KEY_CHUNK + tile, dim), BF16)
    values[rest, :] = jnp.zeros((KEY_CHUNK + tile, dim), BF16)

    @pl.loop(0, end // KEY_CHUNK + 2)
    def _(chunk):
        part = pl.ds(pl.multiple_of(chunk * KEY_CHUNK, KEY_CHUNK), KEY_CHUNK)
        keys[part, dim:] = jnp.zeros((KEY_CHUNK, dim), BF16)

    def close(shard, start):
        live = live_ref[shard, 0]
        after = start + jnp.bitwise_and(live + 15, -16)
        dead = (lane_t == 0) & (row_t + (after - start - 16) >= live)
        keys[pl.ds(pl.multiple_of(after - 16, 16), 16), dim:] = jnp.where(
            dead, -1e30, 0.0
        ).astype(BF16)
        return after

    lax.fori_loop(0, me + 1, close, jnp.int32(0))

    used = (live_ref[me, 0] + tile - 1) // tile

    @pl.loop(used, slots // tile)
    def _(block):
        rows = pl.ds(pl.multiple_of(block * tile, tile), tile)
        out_ref[rows, :] = jnp.zeros((tile, heads * dim), BF16)

    @pl.loop(0, me + 1)
    def _(shard):
        each_piece(shard, jnp.int32(0), lambda copy: copy.wait())

    full = own // KEY_CHUNK

    @pl.loop(0, used)
    def _(block):
        rows = pl.ds(pl.multiple_of(block * tile, tile), tile)
        query = jnp.concatenate([q_ref[head, rows, :] for head in range(heads)], axis=0)
        query = jnp.concatenate([query, ones_q], axis=1)
        best[...] = jnp.full_like(best, -3e38)
        acc[...] = jnp.zeros_like(acc)

        def look(chunk, size, masked):
            part = pl.ds(pl.multiple_of(chunk * size, size), size)
            found = lax.dot_general(
                query, keys[part, :], (((1,), (1,)), ((), ())), preferred_element_type=F32
            )
            if masked:
                key_at = lax.broadcasted_iota(jnp.int32, found.shape, 1) + chunk * size
                query_at = lax.broadcasted_iota(jnp.int32, found.shape, 0)
                limit = jnp.bitwise_and(query_at, tile - 1) + (own + block * tile)
                found = jnp.where(key_at <= limit, found, -1e30)
            score[:, part] = found
            most = found[:, :128]
            for at in range(128, size, 128):
                most = jnp.maximum(most, found[:, at : at + 128])
            best[...] = jnp.maximum(best[...], most)

        def use(chunk, size):
            part = pl.ds(pl.multiple_of(chunk * size, size), size)
            most = best[...]
            weight = jnp.concatenate(
                [
                    jnp.exp2(
                        score[:, pl.ds(pl.multiple_of(chunk * size + at, 128), 128)] - most
                    ).astype(BF16)
                    for at in range(0, size, 128)
                ],
                axis=1,
            )
            right = jnp.concatenate(
                [values[part, :], jnp.concatenate([ones] * (size // KEY_CHUNK), axis=0)], axis=1
            )
            acc[...] += jnp.dot(weight, right, preferred_element_type=F32)

        def cascade(amount, act):
            done = jnp.int32(0)
            for size in SIZES:
                ratio = size // KEY_CHUNK
                first, last = done // ratio, amount // ratio

                @pl.loop(first, last)
                def _(chunk, size=size):
                    act(chunk, size)

                done = last * ratio

        last = (own + (block + 1) * tile + KEY_CHUNK - 1) // KEY_CHUNK
        cascade(full, lambda chunk, size: look(chunk, size, False))

        @pl.loop(full, last)
        def _(chunk):
            look(chunk, KEY_CHUNK, True)

        best[...] = jnp.broadcast_to(jnp.max(best[...], axis=1, keepdims=True), best.shape)
        cascade(last, use)
        result = acc[:, :dim] / acc[:, dim : dim + 1]
        for head in range(heads):
            out_ref[rows, head * dim : (head + 1) * dim] = result[
                head * tile : (head + 1) * tile, :
            ].astype(BF16)


def attend(live, q, kv):
    heads, slots, dim = q.shape
    shards = kv.shape[0]
    length = shards * slots + 2 * KEY_CHUNK
    return pl.pallas_call(
        attend_kernel,
        out_shape=jax.ShapeDtypeStruct((slots, heads * dim), BF16),
        in_specs=[smem(), vmem(), hbm()],
        out_specs=vmem(),
        scratch_shapes=[
            pltpu.VMEM((length, 2 * dim), BF16),
            pltpu.VMEM((length, dim), BF16),
            pltpu.VMEM((heads * 128, 128), F32),
            pltpu.VMEM((heads * 128, 2 * dim), F32),
            pltpu.VMEM((heads * 128, length), F32),
            pltpu.SemaphoreType.DMA((2, shards)),
        ],
        compiler_params=pltpu.CompilerParams(vmem_limit_bytes=VMEM_LIMIT),
        name="attend",
    )(live, q, kv)


def tail_kernel(
    counts_ref, pos_ref, router_ref, attn, wo, weights, hidden, out_ref,
    wv, landing, product, zout, zin, acc, place, own, local_sem, send, recv, zsend, zrecv,
):
    x, zl = lax.axis_index("x"), lax.axis_index("zl")
    x_next, x_prev, x_far = lax.rem(x + 1, 4), lax.rem(x + 3, 4), lax.rem(x + 2, 4)
    right, left, beside = {"x": x_next}, {"x": x_prev}, {"zl": 1 - zl}
    slots, feats = attn.shape
    seq, width = own.shape
    wide = weights.shape[2]
    rows = 128
    count = slots // rows
    half = feats // 2
    own_columns = pl.ds(pl.multiple_of(zl * width, width), width)
    other_columns = pl.ds(pl.multiple_of((1 - zl) * width, width), width)
    column = pl.ds(pl.multiple_of((x * 2 + zl) * width, width), width)
    loads = [
        pltpu.make_async_copy(
            wo.at[:, pl.ds(pl.multiple_of(x * wide, wide), wide)], wv.at[3], local_sem.at[3]
        ),
        pltpu.make_async_copy(weights.at[x_prev], wv.at[0], local_sem.at[0]),
        pltpu.make_async_copy(weights.at[x_next], wv.at[1], local_sem.at[1]),
        pltpu.make_async_copy(weights.at[x_far], wv.at[2], local_sem.at[2]),
        pltpu.make_async_copy(hidden.at[:, column], own, local_sem.at[4]),
    ]
    greeted = greet([right, left, beside])
    for load in loads:
        load.start()
    sends = []

    def push(src, dst, send_at, recv_at, peer):
        copy = pltpu.make_async_remote_copy(
            src_ref=src, dst_ref=dst, send_sem=send_at, recv_sem=recv_at,
            device_id=peer, device_id_type=MESH,
        )
        copy.start()
        sends.append(copy)

    def landed(dst, recv_at):
        pltpu.make_async_remote_copy(
            src_ref=dst, dst_ref=dst, send_sem=send.at[0, 0], recv_sem=recv_at,
            device_id=right, device_id_type=MESH,
        ).wait_recv()

    def part_of(index):
        return slice(index * rows, (index + 1) * rows)

    def send_own(index):
        part = part_of(index)
        push(attn.at[part], landing.at[0, part], send.at[index, 0], recv.at[index, 0], right)
        push(attn.at[part], landing.at[1, part], send.at[index, 1], recv.at[index, 1], left)

    greeted()
    send_own(0)
    send_own(1)

    compact = compact_positions(counts_ref, pos_ref, lax.axis_index(CTX) * seq, slots)
    compact = jnp.transpose(jnp.broadcast_to(compact.astype(F32), (slots, 128)))[:1, :]
    at = lax.broadcasted_iota(jnp.int32, (seq, slots), 0)
    place[...] = jnp.where(at == compact.astype(jnp.int32), 1.0, 0.0).astype(BF16)
    acc[...] = jnp.zeros_like(acc)
    for load in loads:
        load.wait()

    def near(index):
        part = part_of(index)
        product[part, :] = jnp.dot(attn[part, :], wv[3], preferred_element_type=F32)
        landed(landing.at[0, part], recv.at[index, 0])
        first = landing.at[0, part, :half]
        push(first, landing.at[2, part, :half], send.at[index, 2], recv.at[index, 2], right)
        landed(landing.at[1, part], recv.at[index, 1])
        second = landing.at[1, part, half:]
        push(second, landing.at[2, part, half:], send.at[index, 3], recv.at[index, 3], left)
        if index + 2 < count:
            send_own(index + 2)
        product[part, :] += jnp.dot(landing[0, part, :], wv[0], preferred_element_type=F32)
        product[part, :] += jnp.dot(landing[1, part, :], wv[1], preferred_element_type=F32)

    def far(index):
        part = part_of(index)
        landed(landing.at[2, part, :half], recv.at[index, 2])
        landed(landing.at[2, part, half:], recv.at[index, 3])
        value = landing[2, part, :]
        other = product[part, other_columns] + jnp.dot(
            value, wv[2, :, other_columns], preferred_element_type=F32
        )
        zout[part, :] = other.astype(BF16)
        push(zout.at[part], zin.at[part], zsend.at[index], zrecv.at[index], beside)
        product[part, own_columns] += jnp.dot(
            value, wv[2, :, own_columns], preferred_element_type=F32
        )

    def put(index):
        part = part_of(index)
        landed(zin.at[part], zrecv.at[index])
        total = product[part, own_columns] + zin[part, :].astype(F32)
        high = total.astype(BF16)
        low = (total - high.astype(F32)).astype(BF16)
        lanes = place[:, part]
        acc[...] += jnp.dot(
            jnp.concatenate([lanes, lanes], axis=1), jnp.concatenate([high, low], axis=0),
            preferred_element_type=F32,
        )

    for index in range(count + 2):
        if index < count:
            near(index)
        if 1 <= index <= count:
            far(index - 1)
        if index >= 2:
            put(index - 2)
    router = jnp.transpose(jnp.broadcast_to(router_ref[...], (128, seq)))[:, :1]
    out_ref[...] = (own[...].astype(F32) + router * acc[...]).astype(BF16)
    for copy in sends:
        copy.wait_send()


def tail(counts, pos, router, attn, wo, weights, hidden):
    seq = hidden.shape[0]
    slots, feats = attn.shape
    wide = weights.shape[2]
    width = wide // 2
    count = slots // 128
    return pl.pallas_call(
        tail_kernel,
        out_shape=jax.ShapeDtypeStruct((seq, width), BF16),
        in_specs=[smem(), vmem(), vmem(), vmem(), hbm(), hbm(), hbm()],
        out_specs=vmem(),
        scratch_shapes=[
            pltpu.VMEM(weights.shape, BF16),
            pltpu.VMEM((3, slots, feats), BF16),
            pltpu.VMEM((slots, wide), F32),
            pltpu.VMEM((slots, width), BF16),
            pltpu.VMEM((slots, width), BF16),
            pltpu.VMEM((seq, width), F32),
            pltpu.VMEM((seq, slots), BF16),
            pltpu.VMEM((seq, width), BF16),
            pltpu.SemaphoreType.DMA((5,)),
            pltpu.SemaphoreType.DMA((count, 4)),
            pltpu.SemaphoreType.DMA((count, 4)),
            pltpu.SemaphoreType.DMA((count,)),
            pltpu.SemaphoreType.DMA((count,)),
        ],
        compiler_params=pltpu.CompilerParams(
            vmem_limit_bytes=VMEM_LIMIT, collective_id=1, has_side_effects=True
        ),
        name="tail",
    )(counts, pos, router, attn, wo, weights, hidden)


def per_device(
    hidden, norm_gain, w_query, w_key, w_value, w_output, positions, counts, router_weight
):
    seq = hidden.shape[0]
    slots = positions.shape[0]
    shards = lax.axis_size(CTX)
    big, small = angle_tables(seq, shards)
    pos = positions.reshape(1, slots)
    q, live, gathered, weights = front(
        counts, pos, norm_gain.reshape(1, -1), jnp.asarray(small), jnp.asarray(big),
        hidden, w_query, w_key, w_value, w_output,
    )
    attn = attend(live, q, gathered)
    router = router_weight.reshape(1, seq)
    return tail(counts, pos, router, attn, w_output, weights, hidden)


def solution(mesh):
    finer = Mesh(mesh.devices.reshape(2, 4, 2, 4, 2), CTX + TP)
    return jax.shard_map(
        per_device,
        mesh=finer,
        in_specs=(
            P(CTX, None), P(), P(None, TP), P(None, TP), P(None, TP), P(TP, None),
            P(CTX), P(CTX), P(CTX),
        ),
        out_specs=P(CTX, TP),
        check_vma=False,
    )
```

```python
import jax
import jax.numpy as jnp
import numpy as np
from jax import lax
from jax.experimental import pallas as pl
from jax.experimental.pallas import tpu as pltpu
from jax.sharding import Mesh
from jax.sharding import PartitionSpec as P

HEAD_DIM = 128
BLOCK = 128
CTX = ("zh", "y", "core")
TP = ("x", "zl")
CHUNK = 1024
KEY_CHUNK = 512
PARTS = (0, 4, 8, 12, 14, 16)
SIZES = (2048, 1024, 512)
STEP = 32
F32 = jnp.float32
BF16 = jnp.bfloat16
VMEM_LIMIT = 60 * 1024 * 1024
MESH = pl.DeviceIdType.MESH


def freq_table():
    half = HEAD_DIM // 2
    one = 500000.0 ** (-2.0 * np.arange(half, dtype=np.float64) / HEAD_DIM)
    return np.concatenate([one, one])


def angle_tables(seq, shards):
    freq = freq_table()
    sign = np.concatenate([-np.ones(HEAD_DIM // 2), np.ones(HEAD_DIM // 2)])
    coarse = np.arange(0, seq * shards, STEP, dtype=np.float64)[:, None] * freq[None, :]
    fine = np.arange(STEP, dtype=np.float64)[:, None] * freq[None, :]
    big = np.stack([np.cos(coarse), np.sin(coarse)]).astype(np.float32)
    small = np.stack([np.cos(fine), np.sin(fine), np.tile(sign, (STEP, 1))]).astype(np.float32)
    return big.reshape(2, shards, seq // STEP, HEAD_DIM).transpose(1, 0, 2, 3), small


def live_rows(counts_ref, blocks):
    total = counts_ref[0]
    for block in range(1, blocks):
        total = total + counts_ref[block]
    return total


def compact_positions(counts_ref, pos_ref, base, slots):
    lane = lax.broadcasted_iota(jnp.int32, (1, BLOCK), 1)
    row = lax.broadcasted_iota(jnp.int32, (slots, BLOCK), 0)
    start = jnp.int32(0)
    total = jnp.zeros((slots, BLOCK), F32)
    for block in range(slots // BLOCK):
        count = counts_ref[block]
        place = jnp.where(lane < count, lane + start, -1)
        value = (pos_ref[:, block * BLOCK : (block + 1) * BLOCK] - (base - 1)).astype(F32)
        total = total + jnp.where(place == row, value, 0.0)
        start = start + count
    return jnp.sum(total, axis=1, keepdims=True).astype(jnp.int32) - 1


def select_matrix(counts_ref, pos_ref, base, slots, seq):
    column = compact_positions(counts_ref, pos_ref, base, slots)
    place = lax.broadcasted_iota(jnp.int32, (slots, seq), 1)
    return jnp.where(place == column, 1.0, 0.0).astype(BF16)


def rotated(field, cos, sin):
    return field * cos + pltpu.roll(field, HEAD_DIM // 2, 1) * sin


def greet(peers):
    barrier = pltpu.get_barrier_semaphore()
    for peer in peers:
        pl.semaphore_signal(barrier, inc=1, device_id=peer, device_id_type=MESH)

    def wait():
        pl.semaphore_wait(barrier, len(peers))

    return wait


def front_kernel(
    counts, positions, gains, small, big, hidden, wq, wk, wv, wo,
    q_out, live_out, kv_hbm, w_out,
    hbuf, wkv, wqv, gain, acc_kv, acc_q, ssq, cos, sin, sel, bigv, kvbuf, picked_ref,
    counts_ref, pos_ref, gain_row, small_ref,
    hsem, wsem, kv_send, kv_recv, w_send, w_recv, out_sem,
):
    zh, y, core = lax.axis_index("zh"), lax.axis_index("y"), lax.axis_index("core")
    x = lax.axis_index("x")
    y_next, y_prev, y_far = lax.rem(y + 1, 4), lax.rem(y + 3, 4), lax.rem(y + 2, 4)
    x_next, x_prev, x_far = lax.rem(x + 1, 4), lax.rem(x + 3, 4), lax.rem(x + 2, 4)
    mate, up, down = {"core": 1 - core}, {"y": y_next}, {"y": y_prev}
    across, right, left, beyond = {"zh": 1 - zh}, {"x": x_next}, {"x": x_prev}, {"x": x_far}

    def shard_at(plane, row, side):
        return (plane * 4 + row) * 2 + side

    shard = shard_at(zh, y, core)
    seq, width = hidden.shape
    slots = positions.shape[1]
    chunks = width // CHUNK
    rows = 256
    blocks = seq // rows
    loads = [
        pltpu.make_async_copy(counts, counts_ref, wsem.at[3]),
        pltpu.make_async_copy(positions, pos_ref, wsem.at[4]),
        pltpu.make_async_copy(gains, gain_row, wsem.at[0]),
        pltpu.make_async_copy(big.at[shard], bigv, wsem.at[5]),
        pltpu.make_async_copy(small, small_ref, wsem.at[6]),
        pltpu.make_async_copy(wk, wkv.at[:, :HEAD_DIM], wsem.at[1]),
        pltpu.make_async_copy(wv, wkv.at[:, HEAD_DIM:], wsem.at[2]),
    ]
    load_q = pltpu.make_async_copy(wq, wqv, wsem.at[7])

    def fetch(chunk):
        columns = slice(chunk * CHUNK, (chunk + 1) * CHUNK)
        return pltpu.make_async_copy(hidden.at[:, columns], hbuf.at[:, columns], hsem.at[chunk])

    greeted = greet([mate, up, down, across, right, left, beyond])
    for load in loads:
        load.start()
    for chunk in range(chunks):
        fetch(chunk).start()
    load_q.start()

    sends = []

    def push(src, dst, send, recv, peer):
        copy = pltpu.make_async_remote_copy(
            src_ref=src, dst_ref=dst, send_sem=send, recv_sem=recv,
            device_id=peer, device_id_type=MESH,
        )
        copy.start()
        sends.append(copy)

    def landed(dst, recv):
        pltpu.make_async_remote_copy(
            src_ref=dst, dst_ref=dst, send_sem=w_send.at[0], recv_sem=recv,
            device_id=mate, device_id_type=MESH,
        ).wait_recv()

    half_rows = wo.shape[0] // 2
    quarter = half_rows // 2
    own_row = core * half_rows
    wide = wo.shape[1] // 4

    def wo_part(row, count, column):
        return wo.at[
            pl.ds(pl.multiple_of(row, quarter), count),
            pl.ds(pl.multiple_of(column * wide, wide), wide),
        ]

    def slot_part(source, row, count):
        return w_out.at[source, pl.ds(pl.multiple_of(row, quarter), count), :]

    def start_weights():
        greeted()
        for index, (column, peer) in enumerate(((x_far, beyond), (x_next, right), (x_prev, left))):
            for piece in range(2):
                row = own_row + piece * quarter
                push(
                    wo_part(row, quarter, column), slot_part(x, row, quarter),
                    w_send.at[2 * index + piece], w_recv.at[2 * index + piece], peer,
                )

    def scaled(ref, part):
        lanes = ref.shape[1] // 128
        factor = gain[part, :]
        for lane in range(lanes):
            column = slice(lane * 128, (lane + 1) * 128)
            ref[part, column] = (ref[part, column].astype(F32) * factor).astype(BF16)

    loads[0].wait()
    loads[1].wait()
    base = shard * seq
    sel[...] = select_matrix(counts_ref, pos_ref, base, slots, seq)
    loads[2].wait()
    for lanes in range(0, width, 128):
        column = jnp.broadcast_to(gain_row[:, lanes : lanes + 128], (128, 128))
        gain[lanes : lanes + 128, :] = jnp.transpose(column)
    start_weights()
    loads[3].wait()
    loads[4].wait()
    for step in range(seq // STEP):
        part = slice(step * STEP, (step + 1) * STEP)
        cb, sb = bigv[0, step : step + 1, :], bigv[1, step : step + 1, :]
        cf, sf, sign = small_ref[0], small_ref[1], small_ref[2]
        cos[part, :] = cb * cf - sb * sf
        sin[part, :] = (sb * cf + cb * sf) * sign
    loads[5].wait()
    loads[6].wait()
    scaled(wkv, slice(0, width))
    for chunk in range(chunks):
        columns = slice(chunk * CHUNK, (chunk + 1) * CHUNK)
        fetch(chunk).wait()

        @pl.loop(0, seq // 512)
        def _(block, chunk=chunk, columns=columns):
            part = pl.ds(pl.multiple_of(block * 512, 512), 512)
            block_rows = hbuf[part, columns]
            weight = wkv[columns, :]
            value = block_rows.astype(F32)
            square = value * value
            partial = square[:, :128]
            for lane in range(1, CHUNK // 128):
                partial = partial + square[:, lane * 128 : (lane + 1) * 128]
            product = jnp.dot(block_rows, weight, preferred_element_type=F32)
            if chunk == 0:
                ssq[part, :] = partial
                acc_kv[part, :] = product
            else:
                ssq[part, :] += partial
                acc_kv[part, :] += product


    def scale_of(part):
        mean = jnp.sum(ssq[part, :], axis=1, keepdims=True) * (1.0 / width)
        return lax.rsqrt(mean + 1e-05)

    pieces = []
    for block in range(blocks):
        part = slice(block * rows, (block + 1) * rows)
        scale = scale_of(part)
        keys = rotated(acc_kv[part, :HEAD_DIM] * scale, cos[part, :], sin[part, :])
        values = acc_kv[part, HEAD_DIM:] * scale
        pieces.append(jnp.concatenate([keys.astype(BF16), values.astype(BF16)], axis=1))
    both = jnp.dot(sel[...], jnp.concatenate(pieces, axis=0), preferred_element_type=F32)
    live = live_rows(counts_ref, slots // BLOCK)
    low = jnp.minimum(live, 256)
    lane = lax.broadcasted_iota(jnp.int32, (16, HEAD_DIM), 1)
    first = lax.broadcasted_iota(jnp.int32, (16, HEAD_DIM), 0) == 0
    tag = jnp.where(lane == 0, low, jnp.where(lane == 1, live - low, 0))
    kvbuf[shard, 0, :slots] = both[:, :HEAD_DIM].astype(BF16)
    kvbuf[shard, 0, slots:] = jnp.where(first, tag, 0).astype(F32).astype(BF16)
    kvbuf[shard, 1, :slots] = both[:, HEAD_DIM:].astype(BF16)

    def kv_part(source, part):
        return kvbuf.at[source, 0] if part == 0 else kvbuf.at[source, 1, :slots]

    outs = []

    def send_kv(source, part, peer):
        ref = kv_part(source, part)
        push(ref, ref, kv_send.at[len(sends)], kv_recv.at[source, part], peer)

    def keep(source, part):
        ref = kv_part(source, part)
        to = kv_hbm.at[source, part]
        copy = pltpu.make_async_copy(ref.at[:slots] if part == 0 else ref, to, out_sem.at[source, part])
        copy.start()
        outs.append(copy)

    def receive_kv(source, part, peers):
        landed(kv_part(source, part), kv_recv.at[source, part])
        for peer in peers:
            send_kv(source, part, peer)
        keep(source, part)

    for part in range(2):
        send_kv(shard, part, across)
        send_kv(shard, part, up)
        send_kv(shard, part, down)
        send_kv(shard, part, mate)
        keep(shard, part)

    heads = wq.shape[1] // HEAD_DIM
    factor = HEAD_DIM ** (-0.5) * 1.4426950408889634

    def project(block):
        part = slice(block * rows, (block + 1) * rows)
        product = jnp.dot(hbuf[part, :], wqv[...], preferred_element_type=F32)
        scale = scale_of(part) * factor
        for head in range(heads):
            lanes = slice(head * HEAD_DIM, (head + 1) * HEAD_DIM)
            turned = rotated(product[:, lanes] * scale, cos[part, :], sin[part, :])
            acc_q[part, lanes] = turned.astype(BF16)

    load_q.wait()

    @pl.loop(0, width // 512)
    def _(step):
        scaled(wqv, pl.ds(pl.multiple_of(step * 512, 512), 512))

    project(0)
    project(1)
    other = 1 - zh
    prev, following = shard_at(zh, y_prev, core), shard_at(zh, y_next, core)
    opposite, far = shard_at(other, y, core), shard_at(zh, y_far, core)
    receive_kv(prev, 0, [up, mate])
    receive_kv(opposite, 0, [up, down, mate])
    receive_kv(following, 0, [mate])
    project(2)
    receive_kv(following, 1, [down, mate])
    receive_kv(opposite, 1, [up, down, mate])
    receive_kv(prev, 1, [mate])
    project(3)
    receive_kv(far, 0, [across, mate])
    receive_kv(far, 1, [across, mate])
    picked = jnp.dot(sel[...], acc_q[...], preferred_element_type=F32)
    for head in range(heads):
        picked_ref[head] = picked[:, head * HEAD_DIM : (head + 1) * HEAD_DIM].astype(BF16)
    copy_q = pltpu.make_async_copy(picked_ref, q_out, wsem.at[0])
    copy_q.start()
    outs.append(copy_q)

    def pass_on(source, row, count, received, index):
        ref = slot_part(source, row, count)
        landed(ref, w_recv.at[received])
        push(ref, ref, w_send.at[index], w_recv.at[index], mate)

    def pass_piece(index, piece):
        source = (x_far, x_prev, x_next)[index]
        slot = 2 * index + piece
        pass_on(source, own_row + piece * quarter, quarter, slot, slot + 6)

    pass_piece(0, 0)
    pass_piece(0, 1)
    for part in range(2):
        receive_kv(shard_at(other, y_prev, core), part, [mate])
        receive_kv(shard_at(other, y_next, core), part, [mate])
        if part == 0:
            pass_piece(1, 0)
            pass_piece(2, 0)
        receive_kv(shard_at(other, y_far, core), part, [mate])
    pass_piece(1, 1)
    pass_piece(2, 1)

    for plane in range(2):
        for row in range(4):
            for part in range(2):
                receive_kv(shard_at(plane, row, 1 - core), part, [])
    tags = [kvbuf[source, 0, slots : slots + 1, :] for source in range(kvbuf.shape[0])]
    total = jnp.sum(jnp.concatenate(tags, axis=0).astype(F32), axis=1, keepdims=True)
    live_out[...] = jnp.broadcast_to(total, live_out.shape).astype(jnp.int32)
    mate_row = (1 - core) * half_rows
    for index, source in enumerate((x_far, x_prev, x_next)):
        for piece in range(2):
            slot = 2 * index + piece
            landed(slot_part(source, mate_row + piece * quarter, quarter), w_recv.at[slot + 6])
    for copy in sends:
        copy.wait_send()
    for copy in outs:
        copy.wait()


def smem():
    return pl.BlockSpec(memory_space=pltpu.SMEM)


def vmem():
    return pl.BlockSpec(memory_space=pltpu.VMEM)


def hbm():
    return pl.BlockSpec(memory_space=pl.ANY)


def front(counts, pos, gain, small, big, hidden, wq, wk, wv, wo):
    seq, width = hidden.shape
    slots = pos.shape[1]
    heads = wq.shape[1] // HEAD_DIM
    shards = big.shape[0]
    wide = wo.shape[1] // 4
    return pl.pallas_call(
        front_kernel,
        out_shape=(
            jax.ShapeDtypeStruct((heads, slots, HEAD_DIM), BF16),
            jax.ShapeDtypeStruct((shards, 128), jnp.int32),
            jax.ShapeDtypeStruct((shards, 2, slots, HEAD_DIM), BF16),
            jax.ShapeDtypeStruct((4, wo.shape[0], wide), BF16),
        ),
        in_specs=[hbm()] * 10,
        out_specs=(hbm(), vmem(), hbm(), hbm()),
        scratch_shapes=[
            pltpu.VMEM((seq, width), BF16),
            pltpu.VMEM((width, 2 * HEAD_DIM), BF16),
            pltpu.VMEM(wq.shape, BF16),
            pltpu.VMEM((width, 128), F32),
            pltpu.VMEM((seq, 2 * HEAD_DIM), F32),
            pltpu.VMEM((seq, heads * HEAD_DIM), BF16),
            pltpu.VMEM((seq, 128), F32),
            pltpu.VMEM((seq, HEAD_DIM), F32),
            pltpu.VMEM((seq, HEAD_DIM), F32),
            pltpu.VMEM((slots, seq), BF16),
            pltpu.VMEM(big.shape[1:], F32),
            pltpu.VMEM((shards, 2, slots + 16, HEAD_DIM), BF16),
            pltpu.VMEM((heads, slots, HEAD_DIM), BF16),
            pltpu.SMEM(counts.shape, jnp.int32),
            pltpu.VMEM(pos.shape, jnp.int32),
            pltpu.VMEM(gain.shape, F32),
            pltpu.VMEM(small.shape, F32),
            pltpu.SemaphoreType.DMA((width // CHUNK,)),
            pltpu.SemaphoreType.DMA((8,)),
            pltpu.SemaphoreType.DMA((64,)),
            pltpu.SemaphoreType.DMA((shards, 2)),
            pltpu.SemaphoreType.DMA((12,)),
            pltpu.SemaphoreType.DMA((12,)),
            pltpu.SemaphoreType.DMA((shards, 2)),
        ],
        compiler_params=pltpu.CompilerParams(
            vmem_limit_bytes=VMEM_LIMIT, collective_id=0, has_side_effects=True
        ),
        name="front",
    )(counts, pos, gain, small, big, hidden, wq, wk, wv, wo)


def attend_kernel(live_ref, q, kv, out, keys, values, best, acc, score, q_ref, out_ref, sem, io_sem):
    shards, _, slots, dim = kv.shape
    heads = q.shape[0]
    me = lax.axis_index(CTX)
    load_q = pltpu.make_async_copy(q, q_ref, io_sem.at[slots // 128])
    load_q.start()
    tile = 128
    lane = lax.broadcasted_iota(jnp.int32, (KEY_CHUNK, dim), 1)
    ones = jnp.where(lane == 0, 1.0, 0.0).astype(BF16)

    lane_q = lax.broadcasted_iota(jnp.int32, (heads * tile, dim), 1)
    ones_q = jnp.where(lane_q == 0, 1.0, 0.0).astype(BF16)
    lane_t = lax.broadcasted_iota(jnp.int32, (16, dim), 1)
    row_t = lax.broadcasted_iota(jnp.int32, (16, dim), 0)

    def each_piece(shard, start, act):
        units = jnp.right_shift(live_ref[shard, 0] + 15, 4)
        size = slots
        while size >= 16:
            part = size // 16

            @pl.when(jnp.bitwise_and(units, part) != 0)
            def _(size=size, part=part):
                done = jnp.bitwise_and(units, -2 * part) * 16
                source = pl.ds(pl.multiple_of(done, 16), size)
                target = pl.ds(pl.multiple_of(start + done, 16), size)
                act(pltpu.make_async_copy(
                    kv.at[shard, 0, source, :], keys.at[target, :dim], sem.at[0]
                ))
                act(pltpu.make_async_copy(
                    kv.at[shard, 1, source, :], values.at[target, :], sem.at[1]
                ))

            size //= 2
        return start + units * 16

    def begin(shard, start):
        return each_piece(shard, start, lambda copy: copy.start())

    own = lax.fori_loop(0, me, begin, jnp.int32(0))
    end = begin(me, own)
    rest = pl.ds(pl.multiple_of(end, 16), KEY_CHUNK + tile)
    keys[rest, :dim] = jnp.zeros((KEY_CHUNK + tile, dim), BF16)
    values[rest, :] = jnp.zeros((KEY_CHUNK + tile, dim), BF16)

    @pl.loop(0, end // KEY_CHUNK + 2)
    def _(chunk):
        part = pl.ds(pl.multiple_of(chunk * KEY_CHUNK, KEY_CHUNK), KEY_CHUNK)
        keys[part, dim:] = jnp.zeros((KEY_CHUNK, dim), BF16)

    def close(shard, start):
        live = live_ref[shard, 0]
        after = start + jnp.bitwise_and(live + 15, -16)
        dead = (lane_t == 0) & (row_t + (after - start - 16) >= live)
        keys[pl.ds(pl.multiple_of(after - 16, 16), 16), dim:] = jnp.where(
            dead, -1e30, 0.0
        ).astype(BF16)
        return after

    lax.fori_loop(0, me + 1, close, jnp.int32(0))

    used = (live_ref[me, 0] + tile - 1) // tile

    def write(block):
        rows = pl.ds(pl.multiple_of(block * tile, tile), tile)
        return pltpu.make_async_copy(out_ref.at[rows, :], out.at[rows, :], io_sem.at[block])

    @pl.loop(used, slots // tile)
    def _(block):
        rows = pl.ds(pl.multiple_of(block * tile, tile), tile)
        out_ref[rows, :] = jnp.zeros((tile, heads * dim), BF16)
        write(block).start()

    def settle(size):
        source = pl.ds(0, size)
        pltpu.make_async_copy(kv.at[0, 0, source, :], keys.at[source, :dim], sem.at[0]).wait()
        pltpu.make_async_copy(kv.at[0, 1, source, :], values.at[source, :], sem.at[1]).wait()

    @pl.loop(0, end // slots)
    def _(_):
        settle(slots)

    size = slots // 2
    while size >= 16:

        @pl.when(jnp.bitwise_and(end, size) != 0)
        def _(size=size):
            settle(size)

        size //= 2

    load_q.wait()
    full = own // KEY_CHUNK

    @pl.loop(0, used)
    def _(block):
        rows = pl.ds(pl.multiple_of(block * tile, tile), tile)
        query = jnp.concatenate([q_ref[head, rows, :] for head in range(heads)], axis=0)
        query = jnp.concatenate([query, ones_q], axis=1)
        best[...] = jnp.full_like(best, -3e38)
        acc[...] = jnp.zeros_like(acc)

        def look(chunk, size, masked):
            part = pl.ds(pl.multiple_of(chunk * size, size), size)
            found = lax.dot_general(
                query, keys[part, :], (((1,), (1,)), ((), ())), preferred_element_type=F32
            )
            if masked:
                key_at = lax.broadcasted_iota(jnp.int32, found.shape, 1) + chunk * size
                query_at = lax.broadcasted_iota(jnp.int32, found.shape, 0)
                limit = jnp.bitwise_and(query_at, tile - 1) + (own + block * tile)
                found = jnp.where(key_at <= limit, found, -1e30)
            score[:, part] = found
            most = found[:, :128]
            for at in range(128, size, 128):
                most = jnp.maximum(most, found[:, at : at + 128])
            best[...] = jnp.maximum(best[...], most)

        def use(chunk, size):
            part = pl.ds(pl.multiple_of(chunk * size, size), size)
            most = best[...]
            weight = jnp.concatenate(
                [
                    jnp.exp2(
                        score[:, pl.ds(pl.multiple_of(chunk * size + at, 128), 128)] - most
                    ).astype(BF16)
                    for at in range(0, size, 128)
                ],
                axis=1,
            )
            right = jnp.concatenate(
                [values[part, :], jnp.concatenate([ones] * (size // KEY_CHUNK), axis=0)], axis=1
            )
            acc[...] += jnp.dot(weight, right, preferred_element_type=F32)

        def cascade(amount, act):
            done = jnp.int32(0)
            for size in SIZES:
                ratio = size // KEY_CHUNK
                first, last = done // ratio, amount // ratio

                @pl.loop(first, last)
                def _(chunk, size=size):
                    act(chunk, size)

                done = last * ratio

        last = (own + (block + 1) * tile + KEY_CHUNK - 1) // KEY_CHUNK
        cascade(full, lambda chunk, size: look(chunk, size, False))

        @pl.loop(full, last)
        def _(chunk):
            look(chunk, KEY_CHUNK, True)

        best[...] = jnp.broadcast_to(jnp.max(best[...], axis=1, keepdims=True), best.shape)
        cascade(last, use)
        result = acc[:, :dim] / acc[:, dim : dim + 1]
        for head in range(heads):
            out_ref[rows, head * dim : (head + 1) * dim] = result[
                head * tile : (head + 1) * tile, :
            ].astype(BF16)
        write(block).start()

    @pl.loop(0, slots // tile)
    def _(block):
        write(block).wait()


def attend(live, q, kv):
    heads, slots, dim = q.shape
    shards = kv.shape[0]
    length = shards * slots + 2 * KEY_CHUNK
    return pl.pallas_call(
        attend_kernel,
        out_shape=jax.ShapeDtypeStruct((slots, heads * dim), BF16),
        in_specs=[smem(), hbm(), hbm()],
        out_specs=hbm(),
        scratch_shapes=[
            pltpu.VMEM((length, 2 * dim), BF16),
            pltpu.VMEM((length, dim), BF16),
            pltpu.VMEM((heads * 128, 128), F32),
            pltpu.VMEM((heads * 128, 2 * dim), F32),
            pltpu.VMEM((heads * 128, length), F32),
            pltpu.VMEM(q.shape, BF16),
            pltpu.VMEM((slots, heads * dim), BF16),
            pltpu.SemaphoreType.DMA((2,)),
            pltpu.SemaphoreType.DMA((slots // 128 + 1,)),
        ],
        compiler_params=pltpu.CompilerParams(vmem_limit_bytes=VMEM_LIMIT),
        name="attend",
    )(live, q, kv)


def tail_bounds(slots):
    return [slots * part // 16 for part in PARTS]


def tail_kernel(
    counts, positions, routers, attn_hbm, wo, weights, hidden, out_ref,
    counts_ref, pos_ref, router_ref, attn, wv, landing, product, zout, zin, acc, place, own, local_sem, send, recv, zsend, zrecv,
):
    x, zl = lax.axis_index("x"), lax.axis_index("zl")
    x_next, x_prev, x_far = lax.rem(x + 1, 4), lax.rem(x + 3, 4), lax.rem(x + 2, 4)
    right, left, beside = {"x": x_next}, {"x": x_prev}, {"zl": 1 - zl}
    slots, feats = attn.shape
    seq, width = own.shape
    wide = weights.shape[2]
    bounds = tail_bounds(slots)
    count = len(bounds) - 1
    half = feats // 2
    own_columns = pl.ds(pl.multiple_of(zl * width, width), width)
    other_columns = pl.ds(pl.multiple_of((1 - zl) * width, width), width)
    column = pl.ds(pl.multiple_of((x * 2 + zl) * width, width), width)
    loads = [
        pltpu.make_async_copy(
            wo.at[:, pl.ds(pl.multiple_of(x * wide, wide), wide)], wv.at[3], local_sem.at[3]
        ),
        pltpu.make_async_copy(weights.at[x_prev], wv.at[0], local_sem.at[0]),
        pltpu.make_async_copy(weights.at[x_next], wv.at[1], local_sem.at[1]),
        pltpu.make_async_copy(weights.at[x_far], wv.at[2], local_sem.at[2]),
        pltpu.make_async_copy(hidden.at[:, column], own, local_sem.at[4]),
    ]
    greeted = greet([right, left, beside])
    load_attn = pltpu.make_async_copy(attn_hbm, attn, local_sem.at[5])
    smalls = [
        pltpu.make_async_copy(counts, counts_ref, local_sem.at[6]),
        pltpu.make_async_copy(positions, pos_ref, local_sem.at[7]),
        pltpu.make_async_copy(routers, router_ref, local_sem.at[8]),
    ]
    load_attn.start()
    for load in smalls + loads:
        load.start()
    sends = []

    def push(src, dst, send_at, recv_at, peer):
        copy = pltpu.make_async_remote_copy(
            src_ref=src, dst_ref=dst, send_sem=send_at, recv_sem=recv_at,
            device_id=peer, device_id_type=MESH,
        )
        copy.start()
        sends.append(copy)

    def landed(dst, recv_at):
        pltpu.make_async_remote_copy(
            src_ref=dst, dst_ref=dst, send_sem=send.at[0, 0], recv_sem=recv_at,
            device_id=right, device_id_type=MESH,
        ).wait_recv()

    def part_of(index):
        return slice(bounds[index], bounds[index + 1])

    def send_own(index):
        part = part_of(index)
        push(attn.at[part], landing.at[0, part], send.at[index, 0], recv.at[index, 0], right)
        push(attn.at[part], landing.at[1, part], send.at[index, 1], recv.at[index, 1], left)

    load_attn.wait()
    greeted()
    send_own(0)
    send_own(1)

    for load in smalls:
        load.wait()
    compact = compact_positions(counts_ref, pos_ref, lax.axis_index(CTX) * seq, slots)
    compact = jnp.transpose(jnp.broadcast_to(compact.astype(F32), (slots, 128)))[:1, :]
    at = lax.broadcasted_iota(jnp.int32, (seq, slots), 0)
    place[...] = jnp.where(at == compact.astype(jnp.int32), 1.0, 0.0).astype(BF16)
    acc[...] = jnp.zeros_like(acc)
    for load in loads:
        load.wait()

    def near(index):
        part = part_of(index)
        product[part, :] = jnp.dot(attn[part, :], wv[3], preferred_element_type=F32)
        landed(landing.at[0, part], recv.at[index, 0])
        first = landing.at[0, part, :half]
        push(first, landing.at[2, part, :half], send.at[index, 2], recv.at[index, 2], right)
        landed(landing.at[1, part], recv.at[index, 1])
        second = landing.at[1, part, half:]
        push(second, landing.at[2, part, half:], send.at[index, 3], recv.at[index, 3], left)
        if index + 2 < count:
            send_own(index + 2)
        product[part, :] += jnp.dot(landing[0, part, :], wv[0], preferred_element_type=F32)
        product[part, :] += jnp.dot(landing[1, part, :], wv[1], preferred_element_type=F32)

    def far(index):
        part = part_of(index)
        landed(landing.at[2, part, :half], recv.at[index, 2])
        landed(landing.at[2, part, half:], recv.at[index, 3])
        value = landing[2, part, :]
        other = product[part, other_columns] + jnp.dot(
            value, wv[2, :, other_columns], preferred_element_type=F32
        )
        zout[part, :] = other.astype(BF16)
        push(zout.at[part], zin.at[part], zsend.at[index], zrecv.at[index], beside)
        product[part, own_columns] += jnp.dot(
            value, wv[2, :, own_columns], preferred_element_type=F32
        )

    def put(first, last):
        part = slice(bounds[first], bounds[last + 1])
        for index in range(first, last + 1):
            landed(zin.at[part_of(index)], zrecv.at[index])
        total = product[part, own_columns] + zin[part, :].astype(F32)
        high = total.astype(BF16)
        low = (total - high.astype(F32)).astype(BF16)
        lanes = place[:, part]
        acc[...] += jnp.dot(
            jnp.concatenate([lanes, lanes], axis=1), jnp.concatenate([high, low], axis=0),
            preferred_element_type=F32,
        )

    for index in range(count + 1):
        if index < count:
            near(index)
        if 1 <= index <= count:
            far(index - 1)
        if 2 <= index < count:
            put(index - 2, index - 2)
    put(count - 2, count - 1)
    router = jnp.transpose(jnp.broadcast_to(router_ref[...], (128, seq)))[:, :1]
    out_ref[...] = (own[...].astype(F32) + router * acc[...]).astype(BF16)
    for copy in sends:
        copy.wait_send()


def tail(counts, pos, router, attn, wo, weights, hidden):
    seq = hidden.shape[0]
    slots, feats = attn.shape
    wide = weights.shape[2]
    width = wide // 2
    count = len(tail_bounds(slots)) - 1
    return pl.pallas_call(
        tail_kernel,
        out_shape=jax.ShapeDtypeStruct((seq, width), BF16),
        in_specs=[hbm()] * 7,
        out_specs=vmem(),
        scratch_shapes=[
            pltpu.SMEM(counts.shape, jnp.int32),
            pltpu.VMEM(pos.shape, jnp.int32),
            pltpu.VMEM(router.shape, F32),
            pltpu.VMEM(attn.shape, BF16),
            pltpu.VMEM(weights.shape, BF16),
            pltpu.VMEM((3, slots, feats), BF16),
            pltpu.VMEM((slots, wide), F32),
            pltpu.VMEM((slots, width), BF16),
            pltpu.VMEM((slots, width), BF16),
            pltpu.VMEM((seq, width), F32),
            pltpu.VMEM((seq, slots), BF16),
            pltpu.VMEM((seq, width), BF16),
            pltpu.SemaphoreType.DMA((9,)),
            pltpu.SemaphoreType.DMA((count, 4)),
            pltpu.SemaphoreType.DMA((count, 4)),
            pltpu.SemaphoreType.DMA((count,)),
            pltpu.SemaphoreType.DMA((count,)),
        ],
        compiler_params=pltpu.CompilerParams(
            vmem_limit_bytes=VMEM_LIMIT, collective_id=1, has_side_effects=True
        ),
        name="tail",
    )(counts, pos, router, attn, wo, weights, hidden)


def per_device(
    hidden, norm_gain, w_query, w_key, w_value, w_output, positions, counts, router_weight
):
    seq = hidden.shape[0]
    slots = positions.shape[0]
    shards = lax.axis_size(CTX)
    big, small = angle_tables(seq, shards)
    pos = positions.reshape(1, slots)
    q, live, gathered, weights = front(
        counts, pos, norm_gain.reshape(1, -1), jnp.asarray(small), jnp.asarray(big),
        hidden, w_query, w_key, w_value, w_output,
    )
    attn = attend(live, q, gathered)
    router = router_weight.reshape(1, seq)
    return tail(counts, pos, router, attn, w_output, weights, hidden)


def solution(mesh):
    finer = Mesh(mesh.devices.reshape(2, 4, 2, 4, 2), CTX + TP)
    return jax.shard_map(
        per_device,
        mesh=finer,
        in_specs=(
            P(CTX, None), P(), P(None, TP), P(None, TP), P(None, TP), P(TP, None),
            P(CTX), P(CTX), P(CTX),
        ),
        out_specs=P(CTX, TP),
        check_vma=False,
    )
```

```python
import jax
import jax.numpy as jnp
import numpy as np
from jax import lax
from jax.experimental import pallas as pl
from jax.experimental.pallas import tpu as pltpu
from jax.sharding import Mesh
from jax.sharding import PartitionSpec as P

HEAD_DIM = 128
BLOCK = 128
CTX = ("zh", "y", "core")
TP = ("x", "zl")
CHUNK = 1024
KEY_CHUNK = 512
PARTS = (0, 4, 8, 12, 14, 16)
SIZES = (2048, 1024, 512)
STEP = 32
F32 = jnp.float32
BF16 = jnp.bfloat16
VMEM_LIMIT = 60 * 1024 * 1024
MESH = pl.DeviceIdType.MESH


def freq_table():
    half = HEAD_DIM // 2
    one = 500000.0 ** (-2.0 * np.arange(half, dtype=np.float64) / HEAD_DIM)
    return np.concatenate([one, one])


def angle_tables(seq, shards):
    freq = freq_table()
    sign = np.concatenate([-np.ones(HEAD_DIM // 2), np.ones(HEAD_DIM // 2)])
    coarse = np.arange(0, seq * shards, STEP, dtype=np.float64)[:, None] * freq[None, :]
    fine = np.arange(STEP, dtype=np.float64)[:, None] * freq[None, :]
    big = np.stack([np.cos(coarse), np.sin(coarse)]).astype(np.float32)
    small = np.stack([np.cos(fine), np.sin(fine), np.tile(sign, (STEP, 1))]).astype(np.float32)
    return big.reshape(2, shards, seq // STEP, HEAD_DIM).transpose(1, 0, 2, 3), small


def live_rows(counts_ref, blocks):
    total = counts_ref[0]
    for block in range(1, blocks):
        total = total + counts_ref[block]
    return total


def compact_positions(counts_ref, pos_ref, base, slots):
    lane = lax.broadcasted_iota(jnp.int32, (1, BLOCK), 1)
    row = lax.broadcasted_iota(jnp.int32, (slots, BLOCK), 0)
    start = jnp.int32(0)
    total = jnp.zeros((slots, BLOCK), F32)
    for block in range(slots // BLOCK):
        count = counts_ref[block]
        place = jnp.where(lane < count, lane + start, -1)
        value = (pos_ref[:, block * BLOCK : (block + 1) * BLOCK] - (base - 1)).astype(F32)
        total = total + jnp.where(place == row, value, 0.0)
        start = start + count
    return jnp.sum(total, axis=1, keepdims=True).astype(jnp.int32) - 1


def select_matrix(counts_ref, pos_ref, base, slots, seq):
    column = compact_positions(counts_ref, pos_ref, base, slots)
    place = lax.broadcasted_iota(jnp.int32, (slots, seq), 1)
    return jnp.where(place == column, 1.0, 0.0).astype(BF16)


def rotated(field, cos, sin):
    return field * cos + pltpu.roll(field, HEAD_DIM // 2, 1) * sin


def greet(peers):
    barrier = pltpu.get_barrier_semaphore()
    for peer in peers:
        pl.semaphore_signal(barrier, inc=1, device_id=peer, device_id_type=MESH)

    def wait():
        pl.semaphore_wait(barrier, len(peers))

    return wait


def front_kernel(
    counts, positions, gains, small, big, hidden, wq, wk, wv, wo,
    q_out, live_out, kv_hbm, w_out,
    hbuf, wkv, wqv, gain, acc_kv, acc_q, ssq, cos, sin, sel, bigv, kvbuf, picked_ref,
    counts_ref, pos_ref, gain_row, small_ref,
    hsem, wsem, kv_send, kv_recv, w_send, w_recv, out_sem,
):
    zh, y, core = lax.axis_index("zh"), lax.axis_index("y"), lax.axis_index("core")
    x = lax.axis_index("x")
    y_next, y_prev, y_far = lax.rem(y + 1, 4), lax.rem(y + 3, 4), lax.rem(y + 2, 4)
    x_next, x_prev, x_far = lax.rem(x + 1, 4), lax.rem(x + 3, 4), lax.rem(x + 2, 4)
    mate, up, down = {"core": 1 - core}, {"y": y_next}, {"y": y_prev}
    across, right, left, beyond = {"zh": 1 - zh}, {"x": x_next}, {"x": x_prev}, {"x": x_far}

    def shard_at(plane, row, side):
        return (plane * 4 + row) * 2 + side

    shard = shard_at(zh, y, core)
    seq, width = hidden.shape
    slots = positions.shape[1]
    chunks = width // CHUNK
    rows = 256
    blocks = seq // rows
    loads = [
        pltpu.make_async_copy(counts, counts_ref, wsem.at[3]),
        pltpu.make_async_copy(positions, pos_ref, wsem.at[4]),
        pltpu.make_async_copy(gains, gain_row, wsem.at[0]),
        pltpu.make_async_copy(big.at[shard], bigv, wsem.at[5]),
        pltpu.make_async_copy(small, small_ref, wsem.at[6]),
        pltpu.make_async_copy(wk, wkv.at[:, :HEAD_DIM], wsem.at[1]),
        pltpu.make_async_copy(wv, wkv.at[:, HEAD_DIM:], wsem.at[2]),
    ]
    load_q = pltpu.make_async_copy(wq, wqv, wsem.at[7])

    def fetch(chunk):
        columns = slice(chunk * CHUNK, (chunk + 1) * CHUNK)
        return pltpu.make_async_copy(hidden.at[:, columns], hbuf.at[:, columns], hsem.at[chunk])

    greeted = greet([mate, up, down, across, right, left, beyond])
    for load in loads:
        load.start()
    for chunk in range(chunks):
        fetch(chunk).start()
    load_q.start()

    sends = []

    def push(src, dst, send, recv, peer):
        copy = pltpu.make_async_remote_copy(
            src_ref=src, dst_ref=dst, send_sem=send, recv_sem=recv,
            device_id=peer, device_id_type=MESH,
        )
        copy.start()
        sends.append(copy)

    def landed(dst, recv):
        pltpu.make_async_remote_copy(
            src_ref=dst, dst_ref=dst, send_sem=w_send.at[0], recv_sem=recv,
            device_id=mate, device_id_type=MESH,
        ).wait_recv()

    half_rows = wo.shape[0] // 2
    quarter = half_rows // 2
    own_row = core * half_rows
    wide = wo.shape[1] // 4

    def wo_part(row, count, column):
        return wo.at[
            pl.ds(pl.multiple_of(row, quarter), count),
            pl.ds(pl.multiple_of(column * wide, wide), wide),
        ]

    def slot_part(source, row, count):
        return w_out.at[source, pl.ds(pl.multiple_of(row, quarter), count), :]

    def start_weights():
        greeted()
        for index, (column, peer) in enumerate(((x_far, beyond), (x_next, right), (x_prev, left))):
            for piece in range(2):
                row = own_row + piece * quarter
                push(
                    wo_part(row, quarter, column), slot_part(x, row, quarter),
                    w_send.at[2 * index + piece], w_recv.at[2 * index + piece], peer,
                )

    def scaled(ref, part):
        lanes = ref.shape[1] // 128
        factor = gain[part, :]
        for lane in range(lanes):
            column = slice(lane * 128, (lane + 1) * 128)
            ref[part, column] = (ref[part, column].astype(F32) * factor).astype(BF16)

    loads[0].wait()
    loads[1].wait()
    base = shard * seq
    sel[...] = select_matrix(counts_ref, pos_ref, base, slots, seq)
    loads[2].wait()
    for lanes in range(0, width, 128):
        column = jnp.broadcast_to(gain_row[:, lanes : lanes + 128], (128, 128))
        gain[lanes : lanes + 128, :] = jnp.transpose(column)
    start_weights()
    loads[3].wait()
    loads[4].wait()
    for step in range(seq // STEP):
        part = slice(step * STEP, (step + 1) * STEP)
        cb, sb = bigv[0, step : step + 1, :], bigv[1, step : step + 1, :]
        cf, sf, sign = small_ref[0], small_ref[1], small_ref[2]
        cos[part, :] = cb * cf - sb * sf
        sin[part, :] = (sb * cf + cb * sf) * sign
    loads[5].wait()
    loads[6].wait()
    scaled(wkv, slice(0, width))
    for chunk in range(chunks):
        columns = slice(chunk * CHUNK, (chunk + 1) * CHUNK)
        fetch(chunk).wait()

        @pl.loop(0, seq // 512)
        def _(block, chunk=chunk, columns=columns):
            part = pl.ds(pl.multiple_of(block * 512, 512), 512)
            block_rows = hbuf[part, columns]
            weight = wkv[columns, :]
            value = block_rows.astype(F32)
            square = value * value
            partial = square[:, :128]
            for lane in range(1, CHUNK // 128):
                partial = partial + square[:, lane * 128 : (lane + 1) * 128]
            product = jnp.dot(block_rows, weight, preferred_element_type=F32)
            if chunk == 0:
                ssq[part, :] = partial
                acc_kv[part, :] = product
            else:
                ssq[part, :] += partial
                acc_kv[part, :] += product


    def scale_of(part):
        mean = jnp.sum(ssq[part, :], axis=1, keepdims=True) * (1.0 / width)
        return lax.rsqrt(mean + 1e-05)

    pieces = []
    for block in range(blocks):
        part = slice(block * rows, (block + 1) * rows)
        scale = scale_of(part)
        keys = rotated(acc_kv[part, :HEAD_DIM] * scale, cos[part, :], sin[part, :])
        values = acc_kv[part, HEAD_DIM:] * scale
        pieces.append(jnp.concatenate([keys.astype(BF16), values.astype(BF16)], axis=1))
    both = jnp.dot(sel[...], jnp.concatenate(pieces, axis=0), preferred_element_type=F32)
    live = live_rows(counts_ref, slots // BLOCK)
    low = jnp.minimum(live, 256)
    lane = lax.broadcasted_iota(jnp.int32, (16, HEAD_DIM), 1)
    first = lax.broadcasted_iota(jnp.int32, (16, HEAD_DIM), 0) == 0
    tag = jnp.where(lane == 0, low, jnp.where(lane == 1, live - low, 0))
    kvbuf[shard, 0, :slots] = both[:, :HEAD_DIM].astype(BF16)
    kvbuf[shard, 0, slots:] = jnp.where(first, tag, 0).astype(F32).astype(BF16)
    kvbuf[shard, 1, :slots] = both[:, HEAD_DIM:].astype(BF16)

    def kv_part(source, part):
        return kvbuf.at[source, 0] if part == 0 else kvbuf.at[source, 1, :slots]

    outs = []

    def send_kv(source, part, peer):
        ref = kv_part(source, part)
        push(ref, ref, kv_send.at[len(sends)], kv_recv.at[source, part], peer)

    def keep(source, part):
        ref = kv_part(source, part)
        to = kv_hbm.at[source, part]
        copy = pltpu.make_async_copy(ref.at[:slots] if part == 0 else ref, to, out_sem.at[source, part])
        copy.start()
        outs.append(copy)

    def receive_kv(source, part, peers):
        landed(kv_part(source, part), kv_recv.at[source, part])
        for peer in peers:
            send_kv(source, part, peer)
        keep(source, part)

    for part in range(2):
        send_kv(shard, part, across)
        send_kv(shard, part, up)
        send_kv(shard, part, down)
        send_kv(shard, part, mate)
        keep(shard, part)

    heads = wq.shape[1] // HEAD_DIM
    factor = HEAD_DIM ** (-0.5) * 1.4426950408889634

    def project(block):
        part = slice(block * rows, (block + 1) * rows)
        product = jnp.dot(hbuf[part, :], wqv[...], preferred_element_type=F32)
        scale = scale_of(part) * factor
        for head in range(heads):
            lanes = slice(head * HEAD_DIM, (head + 1) * HEAD_DIM)
            turned = rotated(product[:, lanes] * scale, cos[part, :], sin[part, :])
            acc_q[part, lanes] = turned.astype(BF16)

    load_q.wait()

    @pl.loop(0, width // 512)
    def _(step):
        scaled(wqv, pl.ds(pl.multiple_of(step * 512, 512), 512))

    project(0)
    project(1)
    other = 1 - zh
    prev, following = shard_at(zh, y_prev, core), shard_at(zh, y_next, core)
    opposite, far = shard_at(other, y, core), shard_at(zh, y_far, core)
    receive_kv(prev, 0, [up, mate])
    receive_kv(opposite, 0, [up, down, mate])
    receive_kv(following, 0, [mate])
    project(2)
    receive_kv(following, 1, [down, mate])
    receive_kv(opposite, 1, [up, down, mate])
    receive_kv(prev, 1, [mate])
    project(3)
    receive_kv(far, 0, [across, mate])
    receive_kv(far, 1, [across, mate])
    picked = jnp.dot(sel[...], acc_q[...], preferred_element_type=F32)
    for head in range(heads):
        picked_ref[head] = picked[:, head * HEAD_DIM : (head + 1) * HEAD_DIM].astype(BF16)
    copy_q = pltpu.make_async_copy(picked_ref, q_out, wsem.at[0])
    copy_q.start()
    outs.append(copy_q)

    def pass_on(source, row, count, received, index):
        ref = slot_part(source, row, count)
        landed(ref, w_recv.at[received])
        push(ref, ref, w_send.at[index], w_recv.at[index], mate)

    def pass_piece(index, piece):
        source = (x_far, x_prev, x_next)[index]
        slot = 2 * index + piece
        pass_on(source, own_row + piece * quarter, quarter, slot, slot + 6)

    pass_piece(0, 0)
    pass_piece(0, 1)
    for part in range(2):
        receive_kv(shard_at(other, y_prev, core), part, [mate])
        receive_kv(shard_at(other, y_next, core), part, [mate])
        if part == 0:
            pass_piece(1, 0)
            pass_piece(2, 0)
        receive_kv(shard_at(other, y_far, core), part, [mate])
    pass_piece(1, 1)
    pass_piece(2, 1)

    for plane in range(2):
        for row in range(4):
            for part in range(2):
                receive_kv(shard_at(plane, row, 1 - core), part, [])
    tags = [kvbuf[source, 0, slots : slots + 1, :] for source in range(kvbuf.shape[0])]
    total = jnp.sum(jnp.concatenate(tags, axis=0).astype(F32), axis=1, keepdims=True)
    live_out[...] = jnp.broadcast_to(total, live_out.shape).astype(jnp.int32)
    mate_row = (1 - core) * half_rows
    for index, source in enumerate((x_far, x_prev, x_next)):
        for piece in range(2):
            slot = 2 * index + piece
            landed(slot_part(source, mate_row + piece * quarter, quarter), w_recv.at[slot + 6])
    for copy in sends:
        copy.wait_send()
    for copy in outs:
        copy.wait()


def smem():
    return pl.BlockSpec(memory_space=pltpu.SMEM)


def vmem():
    return pl.BlockSpec(memory_space=pltpu.VMEM)


def hbm():
    return pl.BlockSpec(memory_space=pl.ANY)


def front(counts, pos, gain, small, big, hidden, wq, wk, wv, wo):
    seq, width = hidden.shape
    slots = pos.shape[1]
    heads = wq.shape[1] // HEAD_DIM
    shards = big.shape[0]
    wide = wo.shape[1] // 4
    return pl.pallas_call(
        front_kernel,
        out_shape=(
            jax.ShapeDtypeStruct((heads, slots, HEAD_DIM), BF16),
            jax.ShapeDtypeStruct((shards, 128), jnp.int32),
            jax.ShapeDtypeStruct((shards, 2, slots, HEAD_DIM), BF16),
            jax.ShapeDtypeStruct((4, wo.shape[0], wide), BF16),
        ),
        in_specs=[hbm()] * 10,
        out_specs=(hbm(), vmem(), hbm(), hbm()),
        scratch_shapes=[
            pltpu.VMEM((seq, width), BF16),
            pltpu.VMEM((width, 2 * HEAD_DIM), BF16),
            pltpu.VMEM(wq.shape, BF16),
            pltpu.VMEM((width, 128), F32),
            pltpu.VMEM((seq, 2 * HEAD_DIM), F32),
            pltpu.VMEM((seq, heads * HEAD_DIM), BF16),
            pltpu.VMEM((seq, 128), F32),
            pltpu.VMEM((seq, HEAD_DIM), F32),
            pltpu.VMEM((seq, HEAD_DIM), F32),
            pltpu.VMEM((slots, seq), BF16),
            pltpu.VMEM(big.shape[1:], F32),
            pltpu.VMEM((shards, 2, slots + 16, HEAD_DIM), BF16),
            pltpu.VMEM((heads, slots, HEAD_DIM), BF16),
            pltpu.SMEM(counts.shape, jnp.int32),
            pltpu.VMEM(pos.shape, jnp.int32),
            pltpu.VMEM(gain.shape, F32),
            pltpu.VMEM(small.shape, F32),
            pltpu.SemaphoreType.DMA((width // CHUNK,)),
            pltpu.SemaphoreType.DMA((8,)),
            pltpu.SemaphoreType.DMA((64,)),
            pltpu.SemaphoreType.DMA((shards, 2)),
            pltpu.SemaphoreType.DMA((12,)),
            pltpu.SemaphoreType.DMA((12,)),
            pltpu.SemaphoreType.DMA((shards, 2)),
        ],
        compiler_params=pltpu.CompilerParams(
            vmem_limit_bytes=VMEM_LIMIT, collective_id=0, has_side_effects=True
        ),
        name="front",
    )(counts, pos, gain, small, big, hidden, wq, wk, wv, wo)


def attend_kernel(live_ref, q, kv, out, keys, values, best, acc, score, q_ref, out_ref, sem, io_sem):
    shards, _, slots, dim = kv.shape
    heads = q.shape[0]
    me = lax.axis_index(CTX)
    load_q = pltpu.make_async_copy(q, q_ref, io_sem.at[slots // 128])
    load_q.start()
    tile = 128
    lane = lax.broadcasted_iota(jnp.int32, (KEY_CHUNK, dim), 1)
    ones = jnp.where(lane == 0, 1.0, 0.0).astype(BF16)

    lane_q = lax.broadcasted_iota(jnp.int32, (heads * tile, dim), 1)
    ones_q = jnp.where(lane_q == 0, 1.0, 0.0).astype(BF16)
    lane_t = lax.broadcasted_iota(jnp.int32, (16, dim), 1)
    row_t = lax.broadcasted_iota(jnp.int32, (16, dim), 0)

    def each_piece(shard, start, act):
        units = jnp.right_shift(live_ref[shard, 0] + 15, 4)
        size = slots
        while size >= 16:
            part = size // 16

            @pl.when(jnp.bitwise_and(units, part) != 0)
            def _(size=size, part=part):
                done = jnp.bitwise_and(units, -2 * part) * 16
                source = pl.ds(pl.multiple_of(done, 16), size)
                target = pl.ds(pl.multiple_of(start + done, 16), size)
                act(pltpu.make_async_copy(
                    kv.at[shard, 0, source, :], keys.at[target, :dim], sem.at[0]
                ))
                act(pltpu.make_async_copy(
                    kv.at[shard, 1, source, :], values.at[target, :], sem.at[1]
                ))

            size //= 2
        return start + units * 16

    def begin(shard, start):
        return each_piece(shard, start, lambda copy: copy.start())

    own = lax.fori_loop(0, me, begin, jnp.int32(0))
    end = begin(me, own)
    rest = pl.ds(pl.multiple_of(end, 16), KEY_CHUNK + tile)
    keys[rest, :dim] = jnp.zeros((KEY_CHUNK + tile, dim), BF16)
    values[rest, :] = jnp.zeros((KEY_CHUNK + tile, dim), BF16)

    @pl.loop(0, end // KEY_CHUNK + 2)
    def _(chunk):
        part = pl.ds(pl.multiple_of(chunk * KEY_CHUNK, KEY_CHUNK), KEY_CHUNK)
        keys[part, dim:] = jnp.zeros((KEY_CHUNK, dim), BF16)

    def close(shard, start):
        live = live_ref[shard, 0]
        after = start + jnp.bitwise_and(live + 15, -16)
        dead = (lane_t == 0) & (row_t + (after - start - 16) >= live)
        keys[pl.ds(pl.multiple_of(after - 16, 16), 16), dim:] = jnp.where(
            dead, -1e30, 0.0
        ).astype(BF16)
        return after

    lax.fori_loop(0, me + 1, close, jnp.int32(0))

    used = (live_ref[me, 0] + tile - 1) // tile

    def write(block):
        rows = pl.ds(pl.multiple_of(block * tile, tile), tile)
        return pltpu.make_async_copy(out_ref.at[rows, :], out.at[rows, :], io_sem.at[block])

    @pl.loop(used, slots // tile)
    def _(block):
        rows = pl.ds(pl.multiple_of(block * tile, tile), tile)
        out_ref[rows, :] = jnp.zeros((tile, heads * dim), BF16)
        write(block).start()

    def settle(size):
        source = pl.ds(0, size)
        pltpu.make_async_copy(kv.at[0, 0, source, :], keys.at[source, :dim], sem.at[0]).wait()
        pltpu.make_async_copy(kv.at[0, 1, source, :], values.at[source, :], sem.at[1]).wait()

    @pl.loop(0, end // slots)
    def _(_):
        settle(slots)

    size = slots // 2
    while size >= 16:

        @pl.when(jnp.bitwise_and(end, size) != 0)
        def _(size=size):
            settle(size)

        size //= 2

    load_q.wait()
    full = own // KEY_CHUNK

    @pl.loop(0, used)
    def _(block):
        rows = pl.ds(pl.multiple_of(block * tile, tile), tile)
        query = jnp.concatenate([q_ref[head, rows, :] for head in range(heads)], axis=0)
        query = jnp.concatenate([query, ones_q], axis=1)
        best[...] = jnp.full_like(best, -3e38)
        acc[...] = jnp.zeros_like(acc)

        def look(chunk, size, masked):
            part = pl.ds(pl.multiple_of(chunk * size, size), size)
            found = lax.dot_general(
                query, keys[part, :], (((1,), (1,)), ((), ())), preferred_element_type=F32
            )
            if masked:
                key_at = lax.broadcasted_iota(jnp.int32, found.shape, 1) + chunk * size
                query_at = lax.broadcasted_iota(jnp.int32, found.shape, 0)
                limit = jnp.bitwise_and(query_at, tile - 1) + (own + block * tile)
                found = jnp.where(key_at <= limit, found, -1e30)
            score[:, part] = found
            most = found[:, :128]
            for at in range(128, size, 128):
                most = jnp.maximum(most, found[:, at : at + 128])
            best[...] = jnp.maximum(best[...], most)

        def use(chunk, size):
            part = pl.ds(pl.multiple_of(chunk * size, size), size)
            most = best[...]
            weight = jnp.concatenate(
                [
                    jnp.exp2(
                        score[:, pl.ds(pl.multiple_of(chunk * size + at, 128), 128)] - most
                    ).astype(BF16)
                    for at in range(0, size, 128)
                ],
                axis=1,
            )
            right = jnp.concatenate(
                [values[part, :], jnp.concatenate([ones] * (size // KEY_CHUNK), axis=0)], axis=1
            )
            acc[...] += jnp.dot(weight, right, preferred_element_type=F32)

        def cascade(amount, act):
            done = jnp.int32(0)
            for size in SIZES:
                ratio = size // KEY_CHUNK
                first, last = done // ratio, amount // ratio

                @pl.loop(first, last)
                def _(chunk, size=size):
                    act(chunk, size)

                done = last * ratio

        last = (own + (block + 1) * tile + KEY_CHUNK - 1) // KEY_CHUNK
        cascade(full, lambda chunk, size: look(chunk, size, False))

        @pl.loop(full, last)
        def _(chunk):
            look(chunk, KEY_CHUNK, True)

        best[...] = jnp.broadcast_to(jnp.max(best[...], axis=1, keepdims=True), best.shape)
        cascade(last, use)
        result = acc[:, :dim] / acc[:, dim : dim + 1]
        for head in range(heads):
            out_ref[rows, head * dim : (head + 1) * dim] = result[
                head * tile : (head + 1) * tile, :
            ].astype(BF16)
        write(block).start()

    @pl.loop(0, slots // tile)
    def _(block):
        write(block).wait()


def attend(live, q, kv):
    heads, slots, dim = q.shape
    shards = kv.shape[0]
    length = shards * slots + 2 * KEY_CHUNK
    return pl.pallas_call(
        attend_kernel,
        out_shape=jax.ShapeDtypeStruct((slots, heads * dim), BF16),
        in_specs=[smem(), hbm(), hbm()],
        out_specs=hbm(),
        scratch_shapes=[
            pltpu.VMEM((length, 2 * dim), BF16),
            pltpu.VMEM((length, dim), BF16),
            pltpu.VMEM((heads * 128, 128), F32),
            pltpu.VMEM((heads * 128, 2 * dim), F32),
            pltpu.VMEM((heads * 128, length), F32),
            pltpu.VMEM(q.shape, BF16),
            pltpu.VMEM((slots, heads * dim), BF16),
            pltpu.SemaphoreType.DMA((2,)),
            pltpu.SemaphoreType.DMA((slots // 128 + 1,)),
        ],
        compiler_params=pltpu.CompilerParams(vmem_limit_bytes=VMEM_LIMIT),
        name="attend",
    )(live, q, kv)


def tail_bounds(slots):
    return [slots * part // 16 for part in PARTS]


def tail_kernel(
    counts, positions, routers, attn_hbm, wo, weights, hidden, out,
    out_ref, counts_ref, pos_ref, router_ref, attn, wv, landing, product, zout, zin, acc, place, own, local_sem, send, recv, zsend, zrecv,
):
    x, zl = lax.axis_index("x"), lax.axis_index("zl")
    x_next, x_prev, x_far = lax.rem(x + 1, 4), lax.rem(x + 3, 4), lax.rem(x + 2, 4)
    right, left, beside = {"x": x_next}, {"x": x_prev}, {"zl": 1 - zl}
    slots, feats = attn.shape
    seq, width = own.shape
    wide = weights.shape[2]
    bounds = tail_bounds(slots)
    count = len(bounds) - 1
    half = feats // 2
    own_columns = pl.ds(pl.multiple_of(zl * width, width), width)
    other_columns = pl.ds(pl.multiple_of((1 - zl) * width, width), width)
    column = pl.ds(pl.multiple_of((x * 2 + zl) * width, width), width)
    loads = [
        pltpu.make_async_copy(
            wo.at[:, pl.ds(pl.multiple_of(x * wide, wide), wide)], wv.at[3], local_sem.at[3]
        ),
        pltpu.make_async_copy(weights.at[x_prev], wv.at[0], local_sem.at[0]),
        pltpu.make_async_copy(weights.at[x_next], wv.at[1], local_sem.at[1]),
        pltpu.make_async_copy(weights.at[x_far], wv.at[2], local_sem.at[2]),
        pltpu.make_async_copy(hidden.at[:, column], own, local_sem.at[4]),
    ]
    greeted = greet([right, left, beside])
    load_attn = pltpu.make_async_copy(attn_hbm, attn, local_sem.at[5])
    smalls = [
        pltpu.make_async_copy(counts, counts_ref, local_sem.at[6]),
        pltpu.make_async_copy(positions, pos_ref, local_sem.at[7]),
        pltpu.make_async_copy(routers, router_ref, local_sem.at[8]),
    ]
    load_attn.start()
    for load in smalls + loads:
        load.start()
    sends = []

    def push(src, dst, send_at, recv_at, peer):
        copy = pltpu.make_async_remote_copy(
            src_ref=src, dst_ref=dst, send_sem=send_at, recv_sem=recv_at,
            device_id=peer, device_id_type=MESH,
        )
        copy.start()
        sends.append(copy)

    def landed(dst, recv_at):
        pltpu.make_async_remote_copy(
            src_ref=dst, dst_ref=dst, send_sem=send.at[0, 0], recv_sem=recv_at,
            device_id=right, device_id_type=MESH,
        ).wait_recv()

    def part_of(index):
        return slice(bounds[index], bounds[index + 1])

    def send_own(index):
        part = part_of(index)
        push(attn.at[part], landing.at[0, part], send.at[index, 0], recv.at[index, 0], right)
        push(attn.at[part], landing.at[1, part], send.at[index, 1], recv.at[index, 1], left)

    load_attn.wait()
    greeted()
    send_own(0)
    send_own(1)

    for load in smalls:
        load.wait()
    compact = compact_positions(counts_ref, pos_ref, lax.axis_index(CTX) * seq, slots)
    compact = jnp.transpose(jnp.broadcast_to(compact.astype(F32), (slots, 128)))[:1, :]
    at = lax.broadcasted_iota(jnp.int32, (seq, slots), 0)
    place[...] = jnp.where(at == compact.astype(jnp.int32), 1.0, 0.0).astype(BF16)
    acc[...] = jnp.zeros_like(acc)
    router = jnp.transpose(jnp.broadcast_to(router_ref[...], (128, seq)))[:, :1]
    for load in loads:
        load.wait()

    def near(index):
        part = part_of(index)
        product[part, :] = jnp.dot(attn[part, :], wv[3], preferred_element_type=F32)
        landed(landing.at[0, part], recv.at[index, 0])
        first = landing.at[0, part, :half]
        push(first, landing.at[2, part, :half], send.at[index, 2], recv.at[index, 2], right)
        landed(landing.at[1, part], recv.at[index, 1])
        second = landing.at[1, part, half:]
        push(second, landing.at[2, part, half:], send.at[index, 3], recv.at[index, 3], left)
        if index + 2 < count:
            send_own(index + 2)
        product[part, :] += jnp.dot(landing[0, part, :], wv[0], preferred_element_type=F32)
        product[part, :] += jnp.dot(landing[1, part, :], wv[1], preferred_element_type=F32)

    def far(index):
        part = part_of(index)
        landed(landing.at[2, part, :half], recv.at[index, 2])
        landed(landing.at[2, part, half:], recv.at[index, 3])
        value = landing[2, part, :]
        other = product[part, other_columns] + jnp.dot(
            value, wv[2, :, other_columns], preferred_element_type=F32
        )
        zout[part, :] = other.astype(BF16)
        push(zout.at[part], zin.at[part], zsend.at[index], zrecv.at[index], beside)
        product[part, own_columns] += jnp.dot(
            value, wv[2, :, own_columns], preferred_element_type=F32
        )

    def put(first, last):
        part = slice(bounds[first], bounds[last + 1])
        for index in range(first, last + 1):
            landed(zin.at[part_of(index)], zrecv.at[index])
        total = product[part, own_columns] + zin[part, :].astype(F32)
        high = total.astype(BF16)
        low = (total - high.astype(F32)).astype(BF16)
        lanes = place[:, part]
        acc[...] += jnp.dot(
            jnp.concatenate([lanes, lanes], axis=1), jnp.concatenate([high, low], axis=0),
            preferred_element_type=F32,
        )

    for index in range(count + 1):
        if index < count:
            near(index)
        if 1 <= index <= count:
            far(index - 1)
        if 2 <= index < count:
            put(index - 2, index - 2)
    put(count - 2, count - 1)
    writes = []
    for block in range(4):
        part = slice(block * (seq // 4), (block + 1) * (seq // 4))
        value = own[part, :].astype(F32) + router[part, :] * acc[part, :]
        out_ref[part, :] = value.astype(BF16)
        write = pltpu.make_async_copy(out_ref.at[part], out.at[part], local_sem.at[block])
        write.start()
        writes.append(write)
    for write in writes:
        write.wait()
    for copy in sends:
        copy.wait_send()


def tail(counts, pos, router, attn, wo, weights, hidden):
    seq = hidden.shape[0]
    slots, feats = attn.shape
    wide = weights.shape[2]
    width = wide // 2
    count = len(tail_bounds(slots)) - 1
    return pl.pallas_call(
        tail_kernel,
        out_shape=jax.ShapeDtypeStruct((seq, width), BF16),
        in_specs=[hbm()] * 7,
        out_specs=hbm(),
        scratch_shapes=[
            pltpu.VMEM((seq, width), BF16),
            pltpu.SMEM(counts.shape, jnp.int32),
            pltpu.VMEM(pos.shape, jnp.int32),
            pltpu.VMEM(router.shape, F32),
            pltpu.VMEM(attn.shape, BF16),
            pltpu.VMEM(weights.shape, BF16),
            pltpu.VMEM((3, slots, feats), BF16),
            pltpu.VMEM((slots, wide), F32),
            pltpu.VMEM((slots, width), BF16),
            pltpu.VMEM((slots, width), BF16),
            pltpu.VMEM((seq, width), F32),
            pltpu.VMEM((seq, slots), BF16),
            pltpu.VMEM((seq, width), BF16),
            pltpu.SemaphoreType.DMA((9,)),
            pltpu.SemaphoreType.DMA((count, 4)),
            pltpu.SemaphoreType.DMA((count, 4)),
            pltpu.SemaphoreType.DMA((count,)),
            pltpu.SemaphoreType.DMA((count,)),
        ],
        compiler_params=pltpu.CompilerParams(
            vmem_limit_bytes=VMEM_LIMIT, collective_id=1, has_side_effects=True
        ),
        name="tail",
    )(counts, pos, router, attn, wo, weights, hidden)


def per_device(
    hidden, norm_gain, w_query, w_key, w_value, w_output, positions, counts, router_weight
):
    seq = hidden.shape[0]
    slots = positions.shape[0]
    shards = lax.axis_size(CTX)
    big, small = angle_tables(seq, shards)
    pos = positions.reshape(1, slots)
    q, live, gathered, weights = front(
        counts, pos, norm_gain.reshape(1, -1), jnp.asarray(small), jnp.asarray(big),
        hidden, w_query, w_key, w_value, w_output,
    )
    attn = attend(live, q, gathered)
    router = router_weight.reshape(1, seq)
    return tail(counts, pos, router, attn, w_output, weights, hidden)


def solution(mesh):
    finer = Mesh(mesh.devices.reshape(2, 4, 2, 4, 2), CTX + TP)
    return jax.shard_map(
        per_device,
        mesh=finer,
        in_specs=(
            P(CTX, None), P(), P(None, TP), P(None, TP), P(None, TP), P(TP, None),
            P(CTX), P(CTX), P(CTX),
        ),
        out_specs=P(CTX, TP),
        check_vma=False,
    )
```

```python
import jax
import jax.numpy as jnp
import numpy as np
from jax import lax
from jax.experimental import pallas as pl
from jax.experimental.pallas import tpu as pltpu
from jax.sharding import Mesh
from jax.sharding import PartitionSpec as P

HEAD_DIM = 128
BLOCK = 128
CTX = ("zh", "y", "core")
TP = ("x", "zl")
CHUNK = 2048
KEY_CHUNK = 512
PARTS = (0, 4, 8, 12, 14, 16)
SIZES = (2048, 1024, 512)
STEP = 32
F32 = jnp.float32
BF16 = jnp.bfloat16
VMEM_LIMIT = 60 * 1024 * 1024
MESH = pl.DeviceIdType.MESH


def freq_table():
    half = HEAD_DIM // 2
    one = 500000.0 ** (-2.0 * np.arange(half, dtype=np.float64) / HEAD_DIM)
    return np.concatenate([one, one])


def angle_tables(seq, shards):
    freq = freq_table()
    sign = np.concatenate([-np.ones(HEAD_DIM // 2), np.ones(HEAD_DIM // 2)])
    coarse = np.arange(0, seq * shards, STEP, dtype=np.float64)[:, None] * freq[None, :]
    fine = np.arange(STEP, dtype=np.float64)[:, None] * freq[None, :]
    big = np.stack([np.cos(coarse), np.sin(coarse)]).astype(np.float32)
    small = np.stack([np.cos(fine), np.sin(fine), np.tile(sign, (STEP, 1))]).astype(np.float32)
    return big.reshape(2, shards, seq // STEP, HEAD_DIM).transpose(1, 0, 2, 3), small


def live_rows(counts_ref, blocks):
    total = counts_ref[0]
    for block in range(1, blocks):
        total = total + counts_ref[block]
    return total


def compact_positions(counts_ref, pos_ref, base, slots):
    lane = lax.broadcasted_iota(jnp.int32, (1, BLOCK), 1)
    row = lax.broadcasted_iota(jnp.int32, (slots, BLOCK), 0)
    start = jnp.int32(0)
    total = jnp.zeros((slots, BLOCK), F32)
    for block in range(slots // BLOCK):
        count = counts_ref[block]
        place = jnp.where(lane < count, lane + start, -1)
        value = (pos_ref[:, block * BLOCK : (block + 1) * BLOCK] - (base - 1)).astype(F32)
        total = total + jnp.where(place == row, value, 0.0)
        start = start + count
    return jnp.sum(total, axis=1, keepdims=True).astype(jnp.int32) - 1


def select_matrix(counts_ref, pos_ref, base, slots, seq):
    column = compact_positions(counts_ref, pos_ref, base, slots)
    place = lax.broadcasted_iota(jnp.int32, (slots, seq), 1)
    return jnp.where(place == column, 1.0, 0.0).astype(BF16)


def rotated(field, cos, sin):
    return field * cos + pltpu.roll(field, HEAD_DIM // 2, 1) * sin


def greet(peers):
    barrier = pltpu.get_barrier_semaphore()
    for peer in peers:
        pl.semaphore_signal(barrier, inc=1, device_id=peer, device_id_type=MESH)

    def wait():
        pl.semaphore_wait(barrier, len(peers))

    return wait


def front_kernel(
    counts, positions, gains, small, big, hidden, wq, wk, wv, wo,
    q_out, live_out, kv_hbm, w_out,
    hbuf, wkv, wqv, gain, acc_kv, acc_q, ssq, cos, sin, sel, bigv, kvbuf, picked_ref,
    counts_ref, pos_ref, gain_row, small_ref,
    hsem, wsem, kv_send, kv_recv, w_send, w_recv, out_sem,
):
    zh, y, core = lax.axis_index("zh"), lax.axis_index("y"), lax.axis_index("core")
    x = lax.axis_index("x")
    y_next, y_prev, y_far = lax.rem(y + 1, 4), lax.rem(y + 3, 4), lax.rem(y + 2, 4)
    x_next, x_prev, x_far = lax.rem(x + 1, 4), lax.rem(x + 3, 4), lax.rem(x + 2, 4)
    mate, up, down = {"core": 1 - core}, {"y": y_next}, {"y": y_prev}
    across, right, left, beyond = {"zh": 1 - zh}, {"x": x_next}, {"x": x_prev}, {"x": x_far}

    def shard_at(plane, row, side):
        return (plane * 4 + row) * 2 + side

    shard = shard_at(zh, y, core)
    seq, width = hidden.shape
    slots = positions.shape[1]
    chunks = width // CHUNK
    rows = 256
    blocks = seq // rows
    loads = [
        pltpu.make_async_copy(counts, counts_ref, wsem.at[3]),
        pltpu.make_async_copy(positions, pos_ref, wsem.at[4]),
        pltpu.make_async_copy(gains, gain_row, wsem.at[0]),
        pltpu.make_async_copy(big.at[shard], bigv, wsem.at[5]),
        pltpu.make_async_copy(small, small_ref, wsem.at[6]),
        pltpu.make_async_copy(wk, wkv.at[:, :HEAD_DIM], wsem.at[1]),
        pltpu.make_async_copy(wv, wkv.at[:, HEAD_DIM:], wsem.at[2]),
    ]
    load_q = pltpu.make_async_copy(wq, wqv, wsem.at[7])

    def fetch(chunk):
        columns = slice(chunk * CHUNK, (chunk + 1) * CHUNK)
        return pltpu.make_async_copy(hidden.at[:, columns], hbuf.at[:, columns], hsem.at[chunk])

    greeted = greet([mate, up, down, across, right, left, beyond])
    for load in loads:
        load.start()
    for chunk in range(chunks):
        fetch(chunk).start()
    load_q.start()

    sends = []

    def push(src, dst, send, recv, peer):
        copy = pltpu.make_async_remote_copy(
            src_ref=src, dst_ref=dst, send_sem=send, recv_sem=recv,
            device_id=peer, device_id_type=MESH,
        )
        copy.start()
        sends.append(copy)

    def landed(dst, recv):
        pltpu.make_async_remote_copy(
            src_ref=dst, dst_ref=dst, send_sem=w_send.at[0], recv_sem=recv,
            device_id=mate, device_id_type=MESH,
        ).wait_recv()

    half_rows = wo.shape[0] // 2
    quarter = half_rows // 2
    own_row = core * half_rows
    wide = wo.shape[1] // 4

    def wo_part(row, count, column):
        return wo.at[
            pl.ds(pl.multiple_of(row, quarter), count),
            pl.ds(pl.multiple_of(column * wide, wide), wide),
        ]

    def slot_part(source, row, count):
        return w_out.at[source, pl.ds(pl.multiple_of(row, quarter), count), :]

    def start_weights():
        greeted()
        for index, (column, peer) in enumerate(((x_far, beyond), (x_next, right), (x_prev, left))):
            for piece in range(2):
                row = own_row + piece * quarter
                push(
                    wo_part(row, quarter, column), slot_part(x, row, quarter),
                    w_send.at[2 * index + piece], w_recv.at[2 * index + piece], peer,
                )

    def scaled(ref, part):
        lanes = ref.shape[1] // 128
        factor = gain[part, :]
        for lane in range(lanes):
            column = slice(lane * 128, (lane + 1) * 128)
            ref[part, column] = (ref[part, column].astype(F32) * factor).astype(BF16)

    loads[0].wait()
    loads[1].wait()
    base = shard * seq
    sel[...] = select_matrix(counts_ref, pos_ref, base, slots, seq)
    loads[2].wait()
    for lanes in range(0, width, 128):
        column = jnp.broadcast_to(gain_row[:, lanes : lanes + 128], (128, 128))
        gain[lanes : lanes + 128, :] = jnp.transpose(column)
    start_weights()
    loads[3].wait()
    loads[4].wait()
    for step in range(seq // STEP):
        part = slice(step * STEP, (step + 1) * STEP)
        cb, sb = bigv[0, step : step + 1, :], bigv[1, step : step + 1, :]
        cf, sf, sign = small_ref[0], small_ref[1], small_ref[2]
        cos[part, :] = cb * cf - sb * sf
        sin[part, :] = (sb * cf + cb * sf) * sign
    loads[5].wait()
    loads[6].wait()
    scaled(wkv, slice(0, width))
    for chunk in range(chunks):
        columns = slice(chunk * CHUNK, (chunk + 1) * CHUNK)
        fetch(chunk).wait()

        @pl.loop(0, seq // 512)
        def _(block, chunk=chunk, columns=columns):
            part = pl.ds(pl.multiple_of(block * 512, 512), 512)
            block_rows = hbuf[part, columns]
            weight = wkv[columns, :]
            value = block_rows.astype(F32)
            square = value * value
            partial = square[:, :128]
            for lane in range(1, CHUNK // 128):
                partial = partial + square[:, lane * 128 : (lane + 1) * 128]
            product = jnp.dot(block_rows, weight, preferred_element_type=F32)
            if chunk == 0:
                ssq[part, :] = partial
                acc_kv[part, :] = product
            else:
                ssq[part, :] += partial
                acc_kv[part, :] += product


    def scale_of(part):
        mean = jnp.sum(ssq[part, :], axis=1, keepdims=True) * (1.0 / width)
        return lax.rsqrt(mean + 1e-05)

    pieces = []
    for block in range(blocks):
        part = slice(block * rows, (block + 1) * rows)
        scale = scale_of(part)
        keys = rotated(acc_kv[part, :HEAD_DIM] * scale, cos[part, :], sin[part, :])
        values = acc_kv[part, HEAD_DIM:] * scale
        pieces.append(jnp.concatenate([keys.astype(BF16), values.astype(BF16)], axis=1))
    both = jnp.dot(sel[...], jnp.concatenate(pieces, axis=0), preferred_element_type=F32)
    live = live_rows(counts_ref, slots // BLOCK)
    low = jnp.minimum(live, 256)
    lane = lax.broadcasted_iota(jnp.int32, (16, HEAD_DIM), 1)
    first = lax.broadcasted_iota(jnp.int32, (16, HEAD_DIM), 0) == 0
    tag = jnp.where(lane == 0, low, jnp.where(lane == 1, live - low, 0))
    kvbuf[shard, 0, :slots] = both[:, :HEAD_DIM].astype(BF16)
    kvbuf[shard, 0, slots:] = jnp.where(first, tag, 0).astype(F32).astype(BF16)
    kvbuf[shard, 1, :slots] = both[:, HEAD_DIM:].astype(BF16)

    def kv_part(source, part):
        return kvbuf.at[source, 0] if part == 0 else kvbuf.at[source, 1, :slots]

    outs = []

    def send_kv(source, part, peer):
        ref = kv_part(source, part)
        push(ref, ref, kv_send.at[len(sends)], kv_recv.at[source, part], peer)

    def keep(source, part):
        ref = kv_part(source, part)
        to = kv_hbm.at[source, part]
        copy = pltpu.make_async_copy(ref.at[:slots] if part == 0 else ref, to, out_sem.at[source, part])
        copy.start()
        outs.append(copy)

    def receive_kv(source, part, peers):
        landed(kv_part(source, part), kv_recv.at[source, part])
        for peer in peers:
            send_kv(source, part, peer)
        keep(source, part)

    for part in range(2):
        send_kv(shard, part, across)
        send_kv(shard, part, up)
        send_kv(shard, part, down)
        send_kv(shard, part, mate)
        keep(shard, part)

    heads = wq.shape[1] // HEAD_DIM
    factor = HEAD_DIM ** (-0.5) * 1.4426950408889634

    def project(block):
        part = slice(block * rows, (block + 1) * rows)
        product = jnp.dot(hbuf[part, :], wqv[...], preferred_element_type=F32)
        scale = scale_of(part) * factor
        for head in range(heads):
            lanes = slice(head * HEAD_DIM, (head + 1) * HEAD_DIM)
            turned = rotated(product[:, lanes] * scale, cos[part, :], sin[part, :])
            acc_q[part, lanes] = turned.astype(BF16)

    load_q.wait()

    @pl.loop(0, width // 512)
    def _(step):
        scaled(wqv, pl.ds(pl.multiple_of(step * 512, 512), 512))

    project(0)
    project(1)
    other = 1 - zh
    prev, following = shard_at(zh, y_prev, core), shard_at(zh, y_next, core)
    opposite, far = shard_at(other, y, core), shard_at(zh, y_far, core)
    receive_kv(prev, 0, [up, mate])
    receive_kv(opposite, 0, [up, down, mate])
    receive_kv(following, 0, [mate])
    project(2)
    receive_kv(following, 1, [down, mate])
    receive_kv(opposite, 1, [up, down, mate])
    receive_kv(prev, 1, [mate])
    project(3)
    receive_kv(far, 0, [across, mate])
    receive_kv(far, 1, [across, mate])
    picked = jnp.dot(sel[...], acc_q[...], preferred_element_type=F32)
    for head in range(heads):
        picked_ref[head] = picked[:, head * HEAD_DIM : (head + 1) * HEAD_DIM].astype(BF16)
    copy_q = pltpu.make_async_copy(picked_ref, q_out, wsem.at[0])
    copy_q.start()
    outs.append(copy_q)

    def pass_on(source, row, count, received, index):
        ref = slot_part(source, row, count)
        landed(ref, w_recv.at[received])
        push(ref, ref, w_send.at[index], w_recv.at[index], mate)

    def pass_piece(index, piece):
        source = (x_far, x_prev, x_next)[index]
        slot = 2 * index + piece
        pass_on(source, own_row + piece * quarter, quarter, slot, slot + 6)

    pass_piece(0, 0)
    pass_piece(0, 1)
    for part in range(2):
        receive_kv(shard_at(other, y_prev, core), part, [mate])
        receive_kv(shard_at(other, y_next, core), part, [mate])
        if part == 0:
            pass_piece(1, 0)
            pass_piece(2, 0)
        receive_kv(shard_at(other, y_far, core), part, [mate])
    pass_piece(1, 1)
    pass_piece(2, 1)

    for plane in range(2):
        for row in range(4):
            for part in range(2):
                receive_kv(shard_at(plane, row, 1 - core), part, [])
    tags = [kvbuf[source, 0, slots : slots + 1, :] for source in range(kvbuf.shape[0])]
    total = jnp.sum(jnp.concatenate(tags, axis=0).astype(F32), axis=1, keepdims=True)
    live_out[...] = jnp.broadcast_to(total, live_out.shape).astype(jnp.int32)
    mate_row = (1 - core) * half_rows
    for index, source in enumerate((x_far, x_prev, x_next)):
        for piece in range(2):
            slot = 2 * index + piece
            landed(slot_part(source, mate_row + piece * quarter, quarter), w_recv.at[slot + 6])
    for copy in sends:
        copy.wait_send()
    for copy in outs:
        copy.wait()


def smem():
    return pl.BlockSpec(memory_space=pltpu.SMEM)


def vmem():
    return pl.BlockSpec(memory_space=pltpu.VMEM)


def hbm():
    return pl.BlockSpec(memory_space=pl.ANY)


def front(counts, pos, gain, small, big, hidden, wq, wk, wv, wo):
    seq, width = hidden.shape
    slots = pos.shape[1]
    heads = wq.shape[1] // HEAD_DIM
    shards = big.shape[0]
    wide = wo.shape[1] // 4
    return pl.pallas_call(
        front_kernel,
        out_shape=(
            jax.ShapeDtypeStruct((heads, slots, HEAD_DIM), BF16),
            jax.ShapeDtypeStruct((shards, 128), jnp.int32),
            jax.ShapeDtypeStruct((shards, 2, slots, HEAD_DIM), BF16),
            jax.ShapeDtypeStruct((4, wo.shape[0], wide), BF16),
        ),
        in_specs=[hbm()] * 10,
        out_specs=(hbm(), vmem(), hbm(), hbm()),
        scratch_shapes=[
            pltpu.VMEM((seq, width), BF16),
            pltpu.VMEM((width, 2 * HEAD_DIM), BF16),
            pltpu.VMEM(wq.shape, BF16),
            pltpu.VMEM((width, 128), F32),
            pltpu.VMEM((seq, 2 * HEAD_DIM), F32),
            pltpu.VMEM((seq, heads * HEAD_DIM), BF16),
            pltpu.VMEM((seq, 128), F32),
            pltpu.VMEM((seq, HEAD_DIM), F32),
            pltpu.VMEM((seq, HEAD_DIM), F32),
            pltpu.VMEM((slots, seq), BF16),
            pltpu.VMEM(big.shape[1:], F32),
            pltpu.VMEM((shards, 2, slots + 16, HEAD_DIM), BF16),
            pltpu.VMEM((heads, slots, HEAD_DIM), BF16),
            pltpu.SMEM(counts.shape, jnp.int32),
            pltpu.VMEM(pos.shape, jnp.int32),
            pltpu.VMEM(gain.shape, F32),
            pltpu.VMEM(small.shape, F32),
            pltpu.SemaphoreType.DMA((width // CHUNK,)),
            pltpu.SemaphoreType.DMA((8,)),
            pltpu.SemaphoreType.DMA((64,)),
            pltpu.SemaphoreType.DMA((shards, 2)),
            pltpu.SemaphoreType.DMA((12,)),
            pltpu.SemaphoreType.DMA((12,)),
            pltpu.SemaphoreType.DMA((shards, 2)),
        ],
        compiler_params=pltpu.CompilerParams(
            vmem_limit_bytes=VMEM_LIMIT, collective_id=0, has_side_effects=True
        ),
        name="front",
    )(counts, pos, gain, small, big, hidden, wq, wk, wv, wo)


def attend_kernel(live_ref, q, kv, out, keys, values, best, acc, score, q_ref, out_ref, sem, io_sem):
    shards, _, slots, dim = kv.shape
    heads = q.shape[0]
    me = lax.axis_index(CTX)
    load_q = pltpu.make_async_copy(q, q_ref, io_sem.at[slots // 128])
    load_q.start()
    tile = 128
    lane = lax.broadcasted_iota(jnp.int32, (KEY_CHUNK, dim), 1)
    ones = jnp.where(lane == 0, 1.0, 0.0).astype(BF16)

    lane_q = lax.broadcasted_iota(jnp.int32, (heads * tile, dim), 1)
    ones_q = jnp.where(lane_q == 0, 1.0, 0.0).astype(BF16)
    lane_t = lax.broadcasted_iota(jnp.int32, (16, dim), 1)
    row_t = lax.broadcasted_iota(jnp.int32, (16, dim), 0)

    def each_piece(shard, start, act):
        units = jnp.right_shift(live_ref[shard, 0] + 15, 4)
        size = slots
        while size >= 16:
            part = size // 16

            @pl.when(jnp.bitwise_and(units, part) != 0)
            def _(size=size, part=part):
                done = jnp.bitwise_and(units, -2 * part) * 16
                source = pl.ds(pl.multiple_of(done, 16), size)
                target = pl.ds(pl.multiple_of(start + done, 16), size)
                act(pltpu.make_async_copy(
                    kv.at[shard, 0, source, :], keys.at[target, :dim], sem.at[0]
                ))
                act(pltpu.make_async_copy(
                    kv.at[shard, 1, source, :], values.at[target, :], sem.at[1]
                ))

            size //= 2
        return start + units * 16

    def begin(shard, start):
        return each_piece(shard, start, lambda copy: copy.start())

    own = lax.fori_loop(0, me, begin, jnp.int32(0))
    end = begin(me, own)
    rest = pl.ds(pl.multiple_of(end, 16), KEY_CHUNK + tile)
    keys[rest, :dim] = jnp.zeros((KEY_CHUNK + tile, dim), BF16)
    values[rest, :] = jnp.zeros((KEY_CHUNK + tile, dim), BF16)

    @pl.loop(0, end // KEY_CHUNK + 2)
    def _(chunk):
        part = pl.ds(pl.multiple_of(chunk * KEY_CHUNK, KEY_CHUNK), KEY_CHUNK)
        keys[part, dim:] = jnp.zeros((KEY_CHUNK, dim), BF16)

    def close(shard, start):
        live = live_ref[shard, 0]
        after = start + jnp.bitwise_and(live + 15, -16)
        dead = (lane_t == 0) & (row_t + (after - start - 16) >= live)
        keys[pl.ds(pl.multiple_of(after - 16, 16), 16), dim:] = jnp.where(
            dead, -1e30, 0.0
        ).astype(BF16)
        return after

    lax.fori_loop(0, me + 1, close, jnp.int32(0))

    used = (live_ref[me, 0] + tile - 1) // tile

    def write(block):
        rows = pl.ds(pl.multiple_of(block * tile, tile), tile)
        return pltpu.make_async_copy(out_ref.at[rows, :], out.at[rows, :], io_sem.at[block])

    @pl.loop(used, slots // tile)
    def _(block):
        rows = pl.ds(pl.multiple_of(block * tile, tile), tile)
        out_ref[rows, :] = jnp.zeros((tile, heads * dim), BF16)
        write(block).start()

    def settle(size):
        source = pl.ds(0, size)
        pltpu.make_async_copy(kv.at[0, 0, source, :], keys.at[source, :dim], sem.at[0]).wait()
        pltpu.make_async_copy(kv.at[0, 1, source, :], values.at[source, :], sem.at[1]).wait()

    @pl.loop(0, end // slots)
    def _(_):
        settle(slots)

    size = slots // 2
    while size >= 16:

        @pl.when(jnp.bitwise_and(end, size) != 0)
        def _(size=size):
            settle(size)

        size //= 2

    load_q.wait()
    full = own // KEY_CHUNK

    @pl.loop(0, used)
    def _(block):
        rows = pl.ds(pl.multiple_of(block * tile, tile), tile)
        query = jnp.concatenate([q_ref[head, rows, :] for head in range(heads)], axis=0)
        query = jnp.concatenate([query, ones_q], axis=1)
        best[...] = jnp.full_like(best, -3e38)
        acc[...] = jnp.zeros_like(acc)

        def look(chunk, size, masked):
            part = pl.ds(pl.multiple_of(chunk * size, size), size)
            found = lax.dot_general(
                query, keys[part, :], (((1,), (1,)), ((), ())), preferred_element_type=F32
            )
            if masked:
                key_at = lax.broadcasted_iota(jnp.int32, found.shape, 1) + chunk * size
                query_at = lax.broadcasted_iota(jnp.int32, found.shape, 0)
                limit = jnp.bitwise_and(query_at, tile - 1) + (own + block * tile)
                found = jnp.where(key_at <= limit, found, -1e30)
            score[:, part] = found
            most = found[:, :128]
            for at in range(128, size, 128):
                most = jnp.maximum(most, found[:, at : at + 128])
            best[...] = jnp.maximum(best[...], most)

        def use(chunk, size):
            part = pl.ds(pl.multiple_of(chunk * size, size), size)
            most = best[...]
            weight = jnp.concatenate(
                [
                    jnp.exp2(
                        score[:, pl.ds(pl.multiple_of(chunk * size + at, 128), 128)] - most
                    ).astype(BF16)
                    for at in range(0, size, 128)
                ],
                axis=1,
            )
            right = jnp.concatenate(
                [values[part, :], jnp.concatenate([ones] * (size // KEY_CHUNK), axis=0)], axis=1
            )
            acc[...] += jnp.dot(weight, right, preferred_element_type=F32)

        def cascade(amount, act):
            done = jnp.int32(0)
            for size in SIZES:
                ratio = size // KEY_CHUNK
                first, last = done // ratio, amount // ratio

                @pl.loop(first, last)
                def _(chunk, size=size):
                    act(chunk, size)

                done = last * ratio

        last = (own + (block + 1) * tile + KEY_CHUNK - 1) // KEY_CHUNK
        cascade(full, lambda chunk, size: look(chunk, size, False))

        @pl.loop(full, last)
        def _(chunk):
            look(chunk, KEY_CHUNK, True)

        best[...] = jnp.broadcast_to(jnp.max(best[...], axis=1, keepdims=True), best.shape)
        cascade(last, use)
        result = acc[:, :dim] / acc[:, dim : dim + 1]
        for head in range(heads):
            out_ref[rows, head * dim : (head + 1) * dim] = result[
                head * tile : (head + 1) * tile, :
            ].astype(BF16)
        write(block).start()

    @pl.loop(0, slots // tile)
    def _(block):
        write(block).wait()


def attend(live, q, kv):
    heads, slots, dim = q.shape
    shards = kv.shape[0]
    length = shards * slots + 2 * KEY_CHUNK
    return pl.pallas_call(
        attend_kernel,
        out_shape=jax.ShapeDtypeStruct((slots, heads * dim), BF16),
        in_specs=[smem(), hbm(), hbm()],
        out_specs=hbm(),
        scratch_shapes=[
            pltpu.VMEM((length, 2 * dim), BF16),
            pltpu.VMEM((length, dim), BF16),
            pltpu.VMEM((heads * 128, 128), F32),
            pltpu.VMEM((heads * 128, 2 * dim), F32),
            pltpu.VMEM((heads * 128, length), F32),
            pltpu.VMEM(q.shape, BF16),
            pltpu.VMEM((slots, heads * dim), BF16),
            pltpu.SemaphoreType.DMA((2,)),
            pltpu.SemaphoreType.DMA((slots // 128 + 1,)),
        ],
        compiler_params=pltpu.CompilerParams(vmem_limit_bytes=VMEM_LIMIT),
        name="attend",
    )(live, q, kv)


def tail_bounds(slots):
    return [slots * part // 16 for part in PARTS]


def tail_kernel(
    counts, positions, routers, attn_hbm, wo, weights, hidden, out,
    out_ref, counts_ref, pos_ref, router_ref, attn, wv, landing, product, zout, zin, acc, place, own, local_sem, send, recv, zsend, zrecv,
):
    x, zl = lax.axis_index("x"), lax.axis_index("zl")
    x_next, x_prev, x_far = lax.rem(x + 1, 4), lax.rem(x + 3, 4), lax.rem(x + 2, 4)
    right, left, beside = {"x": x_next}, {"x": x_prev}, {"zl": 1 - zl}
    slots, feats = attn.shape
    seq, width = own.shape
    wide = weights.shape[2]
    bounds = tail_bounds(slots)
    count = len(bounds) - 1
    half = feats // 2
    own_columns = pl.ds(pl.multiple_of(zl * width, width), width)
    other_columns = pl.ds(pl.multiple_of((1 - zl) * width, width), width)
    column = pl.ds(pl.multiple_of((x * 2 + zl) * width, width), width)
    loads = [
        pltpu.make_async_copy(
            wo.at[:, pl.ds(pl.multiple_of(x * wide, wide), wide)], wv.at[3], local_sem.at[3]
        ),
        pltpu.make_async_copy(weights.at[x_prev], wv.at[0], local_sem.at[0]),
        pltpu.make_async_copy(weights.at[x_next], wv.at[1], local_sem.at[1]),
        pltpu.make_async_copy(weights.at[x_far], wv.at[2], local_sem.at[2]),
        pltpu.make_async_copy(hidden.at[:, column], own, local_sem.at[4]),
    ]
    greeted = greet([right, left, beside])
    load_attn = pltpu.make_async_copy(attn_hbm, attn, local_sem.at[5])
    smalls = [
        pltpu.make_async_copy(counts, counts_ref, local_sem.at[6]),
        pltpu.make_async_copy(positions, pos_ref, local_sem.at[7]),
        pltpu.make_async_copy(routers, router_ref, local_sem.at[8]),
    ]
    load_attn.start()
    for load in smalls + loads:
        load.start()
    sends = []

    def push(src, dst, send_at, recv_at, peer):
        copy = pltpu.make_async_remote_copy(
            src_ref=src, dst_ref=dst, send_sem=send_at, recv_sem=recv_at,
            device_id=peer, device_id_type=MESH,
        )
        copy.start()
        sends.append(copy)

    def landed(dst, recv_at):
        pltpu.make_async_remote_copy(
            src_ref=dst, dst_ref=dst, send_sem=send.at[0, 0], recv_sem=recv_at,
            device_id=right, device_id_type=MESH,
        ).wait_recv()

    def part_of(index):
        return slice(bounds[index], bounds[index + 1])

    def send_own(index):
        part = part_of(index)
        push(attn.at[part], landing.at[0, part], send.at[index, 0], recv.at[index, 0], right)
        push(attn.at[part], landing.at[1, part], send.at[index, 1], recv.at[index, 1], left)

    load_attn.wait()
    greeted()
    send_own(0)
    send_own(1)

    for load in smalls:
        load.wait()
    compact = compact_positions(counts_ref, pos_ref, lax.axis_index(CTX) * seq, slots)
    compact = jnp.transpose(jnp.broadcast_to(compact.astype(F32), (slots, 128)))[:1, :]
    at = lax.broadcasted_iota(jnp.int32, (seq, slots), 0)
    place[...] = jnp.where(at == compact.astype(jnp.int32), 1.0, 0.0).astype(BF16)
    acc[...] = jnp.zeros_like(acc)
    router = jnp.transpose(jnp.broadcast_to(router_ref[...], (128, seq)))[:, :1]
    for load in loads:
        load.wait()

    def near(index):
        part = part_of(index)
        product[part, :] = jnp.dot(attn[part, :], wv[3], preferred_element_type=F32)
        landed(landing.at[0, part], recv.at[index, 0])
        first = landing.at[0, part, :half]
        push(first, landing.at[2, part, :half], send.at[index, 2], recv.at[index, 2], right)
        landed(landing.at[1, part], recv.at[index, 1])
        second = landing.at[1, part, half:]
        push(second, landing.at[2, part, half:], send.at[index, 3], recv.at[index, 3], left)
        if index + 2 < count:
            send_own(index + 2)
        product[part, :] += jnp.dot(landing[0, part, :], wv[0], preferred_element_type=F32)
        product[part, :] += jnp.dot(landing[1, part, :], wv[1], preferred_element_type=F32)

    def far(index):
        part = part_of(index)
        landed(landing.at[2, part, :half], recv.at[index, 2])
        landed(landing.at[2, part, half:], recv.at[index, 3])
        value = landing[2, part, :]
        other = product[part, other_columns] + jnp.dot(
            value, wv[2, :, other_columns], preferred_element_type=F32
        )
        zout[part, :] = other.astype(BF16)
        push(zout.at[part], zin.at[part], zsend.at[index], zrecv.at[index], beside)
        product[part, own_columns] += jnp.dot(
            value, wv[2, :, own_columns], preferred_element_type=F32
        )

    def put(first, last):
        part = slice(bounds[first], bounds[last + 1])
        for index in range(first, last + 1):
            landed(zin.at[part_of(index)], zrecv.at[index])
        total = product[part, own_columns] + zin[part, :].astype(F32)
        high = total.astype(BF16)
        low = (total - high.astype(F32)).astype(BF16)
        lanes = place[:, part]
        acc[...] += jnp.dot(
            jnp.concatenate([lanes, lanes], axis=1), jnp.concatenate([high, low], axis=0),
            preferred_element_type=F32,
        )

    for index in range(count + 1):
        if index < count:
            near(index)
        if 1 <= index <= count:
            far(index - 1)
        if 2 <= index < count:
            put(index - 2, index - 2)
    put(count - 2, count - 1)
    writes = []
    for block in range(4):
        part = slice(block * (seq // 4), (block + 1) * (seq // 4))
        value = own[part, :].astype(F32) + router[part, :] * acc[part, :]
        out_ref[part, :] = value.astype(BF16)
        write = pltpu.make_async_copy(out_ref.at[part], out.at[part], local_sem.at[block])
        write.start()
        writes.append(write)
    for write in writes:
        write.wait()
    for copy in sends:
        copy.wait_send()


def tail(counts, pos, router, attn, wo, weights, hidden):
    seq = hidden.shape[0]
    slots, feats = attn.shape
    wide = weights.shape[2]
    width = wide // 2
    count = len(tail_bounds(slots)) - 1
    return pl.pallas_call(
        tail_kernel,
        out_shape=jax.ShapeDtypeStruct((seq, width), BF16),
        in_specs=[hbm()] * 7,
        out_specs=hbm(),
        scratch_shapes=[
            pltpu.VMEM((seq, width), BF16),
            pltpu.SMEM(counts.shape, jnp.int32),
            pltpu.VMEM(pos.shape, jnp.int32),
            pltpu.VMEM(router.shape, F32),
            pltpu.VMEM(attn.shape, BF16),
            pltpu.VMEM(weights.shape, BF16),
            pltpu.VMEM((3, slots, feats), BF16),
            pltpu.VMEM((slots, wide), F32),
            pltpu.VMEM((slots, width), BF16),
            pltpu.VMEM((slots, width), BF16),
            pltpu.VMEM((seq, width), F32),
            pltpu.VMEM((seq, slots), BF16),
            pltpu.VMEM((seq, width), BF16),
            pltpu.SemaphoreType.DMA((9,)),
            pltpu.SemaphoreType.DMA((count, 4)),
            pltpu.SemaphoreType.DMA((count, 4)),
            pltpu.SemaphoreType.DMA((count,)),
            pltpu.SemaphoreType.DMA((count,)),
        ],
        compiler_params=pltpu.CompilerParams(
            vmem_limit_bytes=VMEM_LIMIT, collective_id=1, has_side_effects=True
        ),
        name="tail",
    )(counts, pos, router, attn, wo, weights, hidden)


def per_device(
    hidden, norm_gain, w_query, w_key, w_value, w_output, positions, counts, router_weight
):
    seq = hidden.shape[0]
    slots = positions.shape[0]
    shards = lax.axis_size(CTX)
    big, small = angle_tables(seq, shards)
    pos = positions.reshape(1, slots)
    q, live, gathered, weights = front(
        counts, pos, norm_gain.reshape(1, -1), jnp.asarray(small), jnp.asarray(big),
        hidden, w_query, w_key, w_value, w_output,
    )
    attn = attend(live, q, gathered)
    router = router_weight.reshape(1, seq)
    return tail(counts, pos, router, attn, w_output, weights, hidden)


def solution(mesh):
    finer = Mesh(mesh.devices.reshape(2, 4, 2, 4, 2), CTX + TP)
    return jax.shard_map(
        per_device,
        mesh=finer,
        in_specs=(
            P(CTX, None), P(), P(None, TP), P(None, TP), P(None, TP), P(TP, None),
            P(CTX), P(CTX), P(CTX),
        ),
        out_specs=P(CTX, TP),
        check_vma=False,
    )
```
